16 devices in a mesh: tp: 2 (over z), dp: 8 (over y, x, core).
Axes of the slice: x: 2, y: 2, z: 2, core: 2. Of those that a mesh axis runs over, the one named last changes fastest.
Arguments:
- x_in: bfloat16 [2, 128, 4096], P(None, ('dp', 'tp'))
- w_gate: bfloat16 [4096, 11008], P('dp', 'tp')
- w_up: bfloat16 [4096, 11008], P('dp', 'tp')
- w_down: bfloat16 [11008, 4096], P('tp', 'dp')
- grad_y: bfloat16 [2, 128, 4096], P(None, ('dp', 'tp'))
Outputs:
- output 1: bfloat16 [2, 128, 4096], P(None, ('dp', 'tp'))
- output 2: bfloat16 [2, 128, 4096], P(None, ('dp', 'tp'))
- output 3: float32 [4096, 11008], P('dp', 'tp')
- output 4: float32 [4096, 11008], P('dp', 'tp')
- output 5: float32 [11008, 4096], P('tp', 'dp')
All inputs are finite; a program needn't handle non-finite values.
Results may differ from the reference program's by a relative error of at most 0.001.
Values are sent between devices in bfloat16 or wider.
A program may use at most 1 GiB of HBM per device.

```python
import jax
import jax.numpy as jnp
from jax import lax

D = 4096
FF = 11008
T_ROWS = 8
DATA_SIZE = 8
MODEL_SIZE = 2
MICRO_STEPS = 2
ALL_ROWS = DATA_SIZE * MODEL_SIZE * T_ROWS


def setup_inputs(seed: int = 0) -> dict:
    keys = jax.random.split(jax.random.key(seed), 5)
    x_in = jax.random.normal(keys[0], (MICRO_STEPS, ALL_ROWS, D), jnp.float32)
    w_gate = jax.random.normal(keys[1], (D, FF), jnp.float32) * D ** -0.5
    w_up = jax.random.normal(keys[2], (D, FF), jnp.float32) * D ** -0.5
    w_down = jax.random.normal(keys[3], (FF, D), jnp.float32) * FF ** -0.5
    grad_y = jax.random.normal(keys[4], (MICRO_STEPS, ALL_ROWS, D), jnp.float32)
    return {"x_in": x_in.astype(jnp.bfloat16), "w_gate": w_gate.astype(jnp.bfloat16), "w_up": w_up.astype(jnp.bfloat16), "w_down": w_down.astype(jnp.bfloat16), "grad_y": grad_y.astype(jnp.bfloat16)}


def mlp_rows(x_blk, dy_blk, w_gate, w_up, w_down):
    gate_pre = jnp.dot(x_blk, w_gate, preferred_element_type=jnp.float32)
    up_pre = jnp.dot(x_blk, w_up, preferred_element_type=jnp.float32)
    sig_gate = jax.nn.sigmoid(gate_pre)
    act_gate = gate_pre * sig_gate
    hidden = (act_gate * up_pre).astype(jnp.bfloat16)
    y_blk = (x_blk.astype(jnp.float32) + jnp.dot(hidden, w_down, preferred_element_type=jnp.float32)).astype(jnp.bfloat16)
    grad_h = jnp.dot(dy_blk, w_down.T, preferred_element_type=jnp.float32)
    grad_gate = (grad_h * up_pre * sig_gate * (1.0 + gate_pre * (1.0 - sig_gate))).astype(jnp.bfloat16)
    grad_up = (grad_h * act_gate).astype(jnp.bfloat16)
    dx_blk = (dy_blk.astype(jnp.float32) + jnp.dot(grad_gate, w_gate.T, preferred_element_type=jnp.float32) + jnp.dot(grad_up, w_up.T, preferred_element_type=jnp.float32)).astype(jnp.bfloat16)
    dw_gate = jnp.dot(x_blk.T, grad_gate, preferred_element_type=jnp.float32)
    dw_up = jnp.dot(x_blk.T, grad_up, preferred_element_type=jnp.float32)
    dw_down = jnp.dot(hidden.T, dy_blk, preferred_element_type=jnp.float32)
    return y_blk, dx_blk, dw_gate, dw_up, dw_down


def reference(x_in, w_gate, w_up, w_down, grad_y):
    blocks = MICRO_STEPS * DATA_SIZE * MODEL_SIZE
    x_blocks = x_in.reshape(blocks, T_ROWS, D)
    dy_blocks = grad_y.reshape(blocks, T_ROWS, D)

    def scan_step(acc_sums, row_pair):
        y_blk, dx_blk, dw_gate, dw_up, dw_down = mlp_rows(row_pair[0], row_pair[1], w_gate, w_up, w_down)
        new_sums = (acc_sums[0] + dw_gate, acc_sums[1] + dw_up, acc_sums[2] + dw_down)
        return new_sums, (y_blk, dx_blk)

    zero_sums = (jnp.zeros((D, FF), jnp.float32), jnp.zeros((D, FF), jnp.float32), jnp.zeros((FF, D), jnp.float32))
    (sum_gate, sum_up, sum_down), (y_blocks, dx_blocks) = lax.scan(scan_step, zero_sums, (x_blocks, dy_blocks))
    return (y_blocks.reshape(x_in.shape), dx_blocks.reshape(x_in.shape), sum_gate, sum_up, sum_down)
```

```python
import functools

import jax
import jax.numpy as jnp
from jax import lax
from jax.experimental import pallas as pl
from jax.experimental.pallas import tpu as pltpu
from jax.sharding import PartitionSpec as P

MESH = pl.DeviceIdType.MESH
LANES = 128
SLOTS = 8
LAGS = (1, 2, 2, 2, 2, 1)
STARTS = tuple(sum(LAGS[:k]) for k in range(len(LAGS) + 1))
TRANS_B = (((1,), (1,)), ((), ()))
TRANS_A = (((0,), (0,)), ((), ()))


def dot_f32(lhs, rhs):
    return jnp.dot(lhs, rhs, preferred_element_type=jnp.float32)


def dot_t(lhs, rhs):
    return lax.dot_general(lhs, rhs, TRANS_B, preferred_element_type=jnp.float32)


def exchange_kernel(tiles, x_hbm, dy_hbm, wg_hbm, wu_hbm, wd_hbm,
                    act_hbm, tok_hbm, out_hbm,
                    loc, tok, rows, wg, wu, wd, part, core_in, first_out, first_in, second_out, second_in, act, acc,
                    load_sem, tok_send, tok_recv, send_sem, recv_sem, store_sem):
    tp = lax.axis_index("tp")
    dp = lax.axis_index("dp")
    core = lax.rem(dp, 2)
    xpos = lax.rem(lax.div(dp, 2), 2)
    ypos = lax.div(dp, 4)
    me = dp * 2 + tp

    def device(fc, fx, fy, fz):
        dc = 1 - core if fc else core
        dx = 1 - xpos if fx else xpos
        dy = 1 - ypos if fy else ypos
        return (1 - tp if fz else tp, dy * 4 + dx * 2 + dc)

    core_peer = device(1, 0, 0, 0)
    x_peer = device(0, 1, 0, 0)
    y_peer = device(0, 0, 1, 0)

    token_loads = [pltpu.make_async_copy(x_hbm, loc.at[0], load_sem.at[0]),
                   pltpu.make_async_copy(dy_hbm, loc.at[1], load_sem.at[1])]
    weight_loads = [pltpu.make_async_copy(wg_hbm, wg, load_sem.at[2]),
                    pltpu.make_async_copy(wu_hbm, wu, load_sem.at[3]),
                    pltpu.make_async_copy(wd_hbm, wd, load_sem.at[4])]
    for cp in token_loads + weight_loads:
        cp.start()

    others = [((k >> 0) & 1, (k >> 1) & 1, (k >> 2) & 1, (k >> 3) & 1) for k in range(1, 16)]
    barrier = pltpu.get_barrier_semaphore()
    for flags in others:
        pl.semaphore_signal(barrier, 1, device_id=device(*flags), device_id_type=MESH)
    for cp in token_loads:
        cp.wait()
    pl.semaphore_wait(barrier, 15)

    for mb in range(2):
        for arr in range(2):
            for flags in others:
                dest = device(*flags)
                pltpu.make_async_remote_copy(
                    src_ref=loc.at[arr, mb, :, pl.ds(pl.multiple_of(dest[1] * 512, 512), 512)],
                    dst_ref=tok.at[arr, mb, me],
                    send_sem=tok_send.at[arr, mb], recv_sem=tok_recv.at[arr, mb],
                    device_id=dest, device_id_type=MESH).start()
    for mb in range(2):
        for arr in range(2):
            tok[arr, mb, me] = loc[arr, mb, :, pl.ds(pl.multiple_of(dp * 512, 512), 512)]

    def tokens_in(arr, mb):
        part15 = tok.at[arr, mb, pl.ds(0, 15)]
        pltpu.make_async_copy(part15, part15, tok_recv.at[arr, mb]).wait()
        for pair in range(8):
            lo = tok[arr, mb, 2 * pair].astype(jnp.float32)
            hi = tok[arr, mb, 2 * pair + 1].astype(jnp.float32)
            rows[arr, pl.ds(mb * 128 + 16 * pair, 16), :] = jnp.concatenate([lo, hi], axis=0).astype(jnp.bfloat16)

    acc[...] = jnp.zeros_like(acc)
    tokens_in(0, 0)
    tokens_in(1, 0)
    for cp in weight_loads:
        cp.wait()

    n_iter = tiles

    def unit(i, h):
        u = 2 * i + h
        mb = lax.div(u, tiles)
        return u, mb, u - tiles * mb

    keep_core = pl.multiple_of(core * 64, 64)
    send_core = pl.multiple_of((1 - core) * 64, 64)
    pos1 = (xpos, ypos)
    pos2 = (ypos, xpos)
    peer1 = (x_peer, y_peer)
    peer2 = (y_peer, x_peer)

    def off(v):
        return pl.multiple_of(v, 16)

    def copies(stage, i, h):
        u, mb, t = unit(i, h)
        slot = lax.rem(i, SLOTS)
        base = mb * 128 + core * 64
        if stage == 0:
            src, dst, dev = part.at[slot, h, :, pl.ds(send_core, 64), :], core_in.at[u], core_peer
        elif stage == 1:
            src, dst, dev = first_out.at[slot, h], first_in.at[u], peer1[h]
        elif stage == 2:
            src, dst, dev = second_out.at[slot, h], second_in.at[u], peer2[h]
        elif stage == 3:
            src = dst = act.at[t, :, pl.ds(off(base + 32 * pos1[h] + 16 * pos2[h]), 16), :]
            dev = peer2[h]
        elif stage == 4:
            src = dst = act.at[t, :, pl.ds(off(base + 32 * pos1[h]), 32), :]
            dev = peer1[h]
        else:
            src = dst = act.at[t, :, pl.ds(off(base), 64), :]
            dev = core_peer
        return pltpu.make_async_remote_copy(
            src_ref=src, dst_ref=dst, send_sem=send_sem.at[stage, h, slot], recv_sem=recv_sem.at[stage, h, slot],
            device_id=dev, device_id_type=MESH)

    def stage_partials(i):
        for h in range(2):
            u, mb, t = unit(i, h)
            slot = lax.rem(i, SLOTS)
            cols = pl.ds(pl.multiple_of(t * LANES, LANES), LANES)
            r = pl.ds(pl.multiple_of(mb * 128, 128), 128)
            pair = jnp.concatenate([wg[:, cols], wu[:, cols]], axis=1)
            ab = dot_f32(rows[0, r, :], pair)
            part[slot, h, 0] = ab[:, :LANES]
            part[slot, h, 1] = ab[:, LANES:]
            part[slot, h, 2] = dot_t(rows[1, r, :], wd[cols, :])
            copies(0, i, h).start()

    def stage_first(i):
        slot = lax.rem(i, SLOTS)
        for h in range(2):
            u, _, _ = unit(i, h)
            copies(0, i, h).wait()
            o = (1 - pos1[h]) * 32
            first_out[slot, h] = (part[slot, h, :, pl.ds(off(core * 64 + o), 32), :] + core_in[u, :, pl.ds(off(o), 32), :])
            copies(1, i, h).start()

    def stage_second(i):
        slot = lax.rem(i, SLOTS)
        for h in range(2):
            u, _, _ = unit(i, h)
            copies(1, i, h).wait()
            o2 = (1 - pos2[h]) * 16
            o = pos1[h] * 32 + o2
            second_out[slot, h] = (part[slot, h, :, pl.ds(off(core * 64 + o), 16), :] + core_in[u, :, pl.ds(off(o), 16), :]
                                   + first_in[u, :, pl.ds(off(o2), 16), :])
            copies(2, i, h).start()

    def stage_act(i):
        slot = lax.rem(i, SLOTS)
        for h in range(2):
            u, mb, t = unit(i, h)
            copies(2, i, h).wait()
            o2 = pos2[h] * 16
            o = pos1[h] * 32 + o2
            tot = (part[slot, h, :, pl.ds(off(core * 64 + o), 16), :] + core_in[u, :, pl.ds(off(o), 16), :]
                   + first_in[u, :, pl.ds(off(o2), 16), :] + second_in[u])
            a, b, g = tot[0], tot[1], tot[2]
            s = jax.nn.sigmoid(a)
            silu = a * s
            r = pl.ds(off(mb * 128 + core * 64 + o), 16)
            act[t, 0, r, :] = (silu * b).astype(jnp.bfloat16)
            act[t, 1, r, :] = (g * b * s * (1.0 + a * (1.0 - s))).astype(jnp.bfloat16)
            act[t, 2, r, :] = (g * silu).astype(jnp.bfloat16)
            copies(3, i, h).start()

    def stage_forward(stage, i):
        for h in range(2):
            copies(stage - 1, i, h).wait()
            copies(stage, i, h).start()

    def stage_outputs(i):
        for h in range(2):
            u, mb, t = unit(i, h)
            copies(5, i, h).wait()
            cols = pl.ds(pl.multiple_of(t * LANES, LANES), LANES)
            r = pl.ds(pl.multiple_of(mb * 128, 128), 128)
            acc[0, r, :] += dot_f32(act[t, 0, r, :], wd[cols, :])
            grads = jnp.concatenate([act[t, 1, r, :], act[t, 2, r, :]], axis=1)
            pair = jnp.concatenate([wg[:, cols], wu[:, cols]], axis=1)
            acc[1, r, :] += dot_t(grads, pair)

            pltpu.make_async_copy(act.at[t, :, r, :], act_hbm.at[t, :, r, :], store_sem.at[0]).start()

    def body(j, carry):
        def run(stage, fn):
            i = j - STARTS[stage]
            pl.when(jnp.logical_and(i >= 0, i < n_iter))(functools.partial(fn, i))

        run(5, functools.partial(stage_forward, 5))
        run(4, functools.partial(stage_forward, 4))
        run(3, stage_act)
        run(2, stage_second)
        run(1, stage_first)

        @pl.when(j == tiles // 2 - 2)
        def _():
            tokens_in(0, 1)
            tokens_in(1, 1)
            pltpu.make_async_copy(rows, tok_hbm, store_sem.at[1]).start()

        run(0, stage_partials)
        run(6, stage_outputs)
        return carry

    lax.fori_loop(0, n_iter + STARTS[6], body, 0)

    out_copy = pltpu.make_async_copy(acc, out_hbm, store_sem.at[2])
    out_copy.start()
    for mb in range(2):
        for arr in range(2):
            part15 = tok.at[arr, mb, pl.ds(0, 15)]
            pltpu.make_async_copy(part15, part15, tok_send.at[arr, mb]).wait()
    pltpu.make_async_copy(rows, tok_hbm, store_sem.at[1]).wait()
    pltpu.make_async_copy(act, act_hbm, store_sem.at[0]).wait()
    out_copy.wait()


def exchange(x_loc, dy_loc, w_gate, w_up, w_down):
    d_loc, f_loc = w_gate.shape
    tiles = f_loc // LANES
    any_spec = pl.BlockSpec(memory_space=pl.ANY)
    f32, bf16 = jnp.float32, jnp.bfloat16
    return pl.pallas_call(
        functools.partial(exchange_kernel, tiles),
        out_shape=(jax.ShapeDtypeStruct((tiles, 3, 256, LANES), bf16),
                   jax.ShapeDtypeStruct((2, 256, d_loc), bf16),
                   jax.ShapeDtypeStruct((2, 256, d_loc), f32)),
        in_specs=[any_spec] * 5,
        out_specs=(any_spec, any_spec, any_spec),
        scratch_shapes=[
            pltpu.VMEM((2, 2, 8, 4096), bf16),
            pltpu.VMEM((2, 2, 16, 8, d_loc), bf16),
            pltpu.VMEM((2, 256, d_loc), bf16),
            pltpu.VMEM((d_loc, f_loc), bf16),
            pltpu.VMEM((d_loc, f_loc), bf16),
            pltpu.VMEM((f_loc, d_loc), bf16),
            pltpu.VMEM((SLOTS, 2, 3, 128, LANES), f32),
            pltpu.VMEM((2 * tiles, 3, 64, LANES), f32),
            pltpu.VMEM((SLOTS, 2, 3, 32, LANES), f32),
            pltpu.VMEM((2 * tiles, 3, 32, LANES), f32),
            pltpu.VMEM((SLOTS, 2, 3, 16, LANES), f32),
            pltpu.VMEM((2 * tiles, 3, 16, LANES), f32),
            pltpu.VMEM((tiles, 3, 256, LANES), bf16),
            pltpu.VMEM((2, 256, d_loc), f32),
            pltpu.SemaphoreType.DMA((5,)),
            pltpu.SemaphoreType.DMA((2, 2)),
            pltpu.SemaphoreType.DMA((2, 2)),
            pltpu.SemaphoreType.DMA((6, 2, SLOTS)),
            pltpu.SemaphoreType.DMA((6, 2, SLOTS)),
            pltpu.SemaphoreType.DMA((3,)),
        ],
        compiler_params=pltpu.CompilerParams(collective_id=0, has_side_effects=True, vmem_limit_bytes=60 * 2**20),
        cost_estimate=pl.CostEstimate(flops=9 * 10**9, bytes_accessed=28 * 10**6, transcendentals=0),
        name="exchange",
    )(x_loc, dy_loc, w_gate, w_up, w_down)


GROUP = 4


def gate_up_kernel(tok_ref, act_ref, dg_ref, du_ref, xt_ref):
    @pl.when(pl.program_id(0) == 0)
    def _():
        xt_ref[...] = tok_ref[0].T

    for k in range(GROUP):
        dg_ref[:, k * LANES:(k + 1) * LANES] = dot_f32(xt_ref[...], act_ref[k, 1])
        du_ref[:, k * LANES:(k + 1) * LANES] = dot_f32(xt_ref[...], act_ref[k, 2])


def down_kernel(tok_ref, act_ref, dd_ref):
    for k in range(GROUP):
        dd_ref[k * LANES:(k + 1) * LANES, :] = lax.dot_general(
            act_ref[k, 0], tok_ref[1], TRANS_A, preferred_element_type=jnp.float32)


def weight_grads(tok, act):
    tiles = act.shape[0]
    d_loc = tok.shape[-1]
    f_loc = tiles * LANES
    grid = (pl.cdiv(tiles, GROUP),)
    tok_spec = pl.BlockSpec((2, 256, d_loc), lambda i: (0, 0, 0))
    act_spec = pl.BlockSpec((GROUP, 3, 256, LANES), lambda i: (i, 0, 0, 0))
    flops = 2 * 256 * d_loc * f_loc
    width = GROUP * LANES
    dg, du = pl.pallas_call(
        gate_up_kernel, grid=grid, in_specs=[tok_spec, act_spec],
        out_specs=[pl.BlockSpec((d_loc, width), lambda i: (0, i))] * 2,
        out_shape=[jax.ShapeDtypeStruct((d_loc, f_loc), jnp.float32)] * 2,
        scratch_shapes=[pltpu.VMEM((d_loc, 256), jnp.bfloat16)],
        cost_estimate=pl.CostEstimate(flops=2 * flops, bytes_accessed=31 * 10**6, transcendentals=0),
        name="gate_up_grads",
    )(tok, act)
    dd = pl.pallas_call(
        down_kernel, grid=grid, in_specs=[tok_spec, act_spec],
        out_specs=pl.BlockSpec((width, d_loc), lambda i: (i, 0)),
        out_shape=jax.ShapeDtypeStruct((f_loc, d_loc), jnp.float32),
        cost_estimate=pl.CostEstimate(flops=flops, bytes_accessed=16 * 10**6, transcendentals=0),
        name="down_grads",
    )(tok, act)
    return dg, du, dd


def solution(mesh):
    row_spec = P(None, ("dp", "tp"), None)
    in_specs = (row_spec, P("dp", "tp"), P("dp", "tp"), P("tp", "dp"), row_spec)
    out_specs = (row_spec, row_spec, P("dp", "tp"), P("dp", "tp"), P("tp", "dp"))

    def local_step(x_loc, w_gate, w_up, w_down, dy_loc):
        act, tok, part = exchange(x_loc, dy_loc, w_gate, w_up, w_down)
        tp = lax.axis_index("tp")
        part = part.reshape(2, 2, 8, 2, 8, 512)
        keep = lax.dynamic_index_in_dim(part, tp, axis=3, keepdims=False)
        send = lax.dynamic_index_in_dim(part, 1 - tp, axis=3, keepdims=False)
        recv = lax.ppermute(send, "tp", [(0, 1), (1, 0)])
        base = lax.dynamic_index_in_dim(tok.reshape(2, 2, 8, 2, 8, 512), tp, axis=3, keepdims=False)
        out = (base.astype(jnp.float32) + (keep + recv)).astype(jnp.bfloat16)
        out = lax.all_to_all(out, "dp", split_axis=2, concat_axis=4, tiled=True)
        out = out.reshape(2, 2, 8, 4096)
        dg, du, dd = weight_grads(tok, act)
        return out[0], out[1], dg, du, dd

    return jax.shard_map(local_step, mesh=mesh, in_specs=in_specs, out_specs=out_specs, check_vma=False)
```

```python
import functools

import jax
import jax.numpy as jnp
from jax import lax
from jax.experimental import pallas as pl
from jax.experimental.pallas import tpu as pltpu
from jax.sharding import PartitionSpec as P

MESH = pl.DeviceIdType.MESH
LANES = 128
SLOTS = 8
LAGS = (1, 2, 2, 2, 2, 1)
STARTS = tuple(sum(LAGS[:k]) for k in range(len(LAGS) + 1))
TRANS_B = (((1,), (1,)), ((), ()))
TRANS_A = (((0,), (0,)), ((), ()))


def dot_f32(lhs, rhs):
    return jnp.dot(lhs, rhs, preferred_element_type=jnp.float32)


def dot_t(lhs, rhs):
    return lax.dot_general(lhs, rhs, TRANS_B, preferred_element_type=jnp.float32)


def exchange_kernel(tiles, x_hbm, dy_hbm, wg_hbm, wu_hbm, wd_hbm,
                    act_hbm, tok_hbm, sum_hbm,
                    loc, tok, rows, wg, wu, wd, part, core_in, first_out, first_in, second_out, second_in, act, acc,
                    load_sem, tok_send, tok_recv, send_sem, recv_sem, store_sem):
    tp = lax.axis_index("tp")
    dp = lax.axis_index("dp")
    core = lax.rem(dp, 2)
    xpos = lax.rem(lax.div(dp, 2), 2)
    ypos = lax.div(dp, 4)
    me = dp * 2 + tp

    def device(fc, fx, fy, fz):
        dc = 1 - core if fc else core
        dx = 1 - xpos if fx else xpos
        dy = 1 - ypos if fy else ypos
        return (1 - tp if fz else tp, dy * 4 + dx * 2 + dc)

    core_peer = device(1, 0, 0, 0)
    x_peer = device(0, 1, 0, 0)
    y_peer = device(0, 0, 1, 0)

    token_loads = [pltpu.make_async_copy(x_hbm, loc.at[0], load_sem.at[0]),
                   pltpu.make_async_copy(dy_hbm, loc.at[1], load_sem.at[1])]
    weight_loads = [pltpu.make_async_copy(wg_hbm, wg, load_sem.at[2]),
                    pltpu.make_async_copy(wu_hbm, wu, load_sem.at[3]),
                    pltpu.make_async_copy(wd_hbm, wd, load_sem.at[4])]
    for cp in token_loads + weight_loads:
        cp.start()

    others = [((k >> 0) & 1, (k >> 1) & 1, (k >> 2) & 1, (k >> 3) & 1) for k in range(1, 16)]
    barrier = pltpu.get_barrier_semaphore()
    for flags in others:
        pl.semaphore_signal(barrier, 1, device_id=device(*flags), device_id_type=MESH)
    for cp in token_loads:
        cp.wait()
    pl.semaphore_wait(barrier, 15)

    for mb in range(2):
        for arr in range(2):
            for flags in others:
                dest = device(*flags)
                pltpu.make_async_remote_copy(
                    src_ref=loc.at[arr, mb, :, pl.ds(pl.multiple_of(dest[1] * 512, 512), 512)],
                    dst_ref=tok.at[arr, mb, me],
                    send_sem=tok_send.at[arr, mb], recv_sem=tok_recv.at[arr, mb],
                    device_id=dest, device_id_type=MESH).start()
    for mb in range(2):
        for arr in range(2):
            tok[arr, mb, me] = loc[arr, mb, :, pl.ds(pl.multiple_of(dp * 512, 512), 512)]

    def tokens_in(arr, mb):
        part15 = tok.at[arr, mb, pl.ds(0, 15)]
        pltpu.make_async_copy(part15, part15, tok_recv.at[arr, mb]).wait()
        for pair in range(8):
            lo = tok[arr, mb, 2 * pair].astype(jnp.float32)
            hi = tok[arr, mb, 2 * pair + 1].astype(jnp.float32)
            rows[arr, pl.ds(mb * 128 + 16 * pair, 16), :] = jnp.concatenate([lo, hi], axis=0).astype(jnp.bfloat16)

    acc[...] = jnp.zeros_like(acc)
    tokens_in(0, 0)
    tokens_in(1, 0)
    for cp in weight_loads:
        cp.wait()

    n_iter = tiles

    def unit(i, h):
        u = 2 * i + h
        mb = lax.div(u, tiles)
        return u, mb, u - tiles * mb

    keep_core = pl.multiple_of(core * 64, 64)
    send_core = pl.multiple_of((1 - core) * 64, 64)
    pos1 = (xpos, ypos)
    pos2 = (ypos, xpos)
    peer1 = (x_peer, y_peer)
    peer2 = (y_peer, x_peer)

    def off(v):
        return pl.multiple_of(v, 16)

    def copies(stage, i, h):
        u, mb, t = unit(i, h)
        slot = lax.rem(i, SLOTS)
        base = mb * 128 + core * 64
        if stage == 0:
            src, dst, dev = part.at[slot, h, :, pl.ds(send_core, 64), :], core_in.at[u], core_peer
        elif stage == 1:
            src, dst, dev = first_out.at[slot, h], first_in.at[u], peer1[h]
        elif stage == 2:
            src, dst, dev = second_out.at[slot, h], second_in.at[u], peer2[h]
        elif stage == 3:
            src = dst = act.at[t, :, pl.ds(off(base + 32 * pos1[h] + 16 * pos2[h]), 16), :]
            dev = peer2[h]
        elif stage == 4:
            src = dst = act.at[t, :, pl.ds(off(base + 32 * pos1[h]), 32), :]
            dev = peer1[h]
        else:
            src = dst = act.at[t, :, pl.ds(off(base), 64), :]
            dev = core_peer
        return pltpu.make_async_remote_copy(
            src_ref=src, dst_ref=dst, send_sem=send_sem.at[stage, h, slot], recv_sem=recv_sem.at[stage, h, slot],
            device_id=dev, device_id_type=MESH)

    def stage_partials(i):
        for h in range(2):
            u, mb, t = unit(i, h)
            slot = lax.rem(i, SLOTS)
            cols = pl.ds(pl.multiple_of(t * LANES, LANES), LANES)
            r = pl.ds(pl.multiple_of(mb * 128, 128), 128)
            pair = jnp.concatenate([wg[:, cols], wu[:, cols]], axis=1)
            ab = dot_f32(rows[0, r, :], pair)
            part[slot, h, 0] = ab[:, :LANES]
            part[slot, h, 1] = ab[:, LANES:]
            part[slot, h, 2] = dot_t(rows[1, r, :], wd[cols, :])
            copies(0, i, h).start()

    def stage_first(i):
        slot = lax.rem(i, SLOTS)
        for h in range(2):
            u, _, _ = unit(i, h)
            copies(0, i, h).wait()
            o = (1 - pos1[h]) * 32
            first_out[slot, h] = (part[slot, h, :, pl.ds(off(core * 64 + o), 32), :] + core_in[u, :, pl.ds(off(o), 32), :])
            copies(1, i, h).start()

    def stage_second(i):
        slot = lax.rem(i, SLOTS)
        for h in range(2):
            u, _, _ = unit(i, h)
            copies(1, i, h).wait()
            o2 = (1 - pos2[h]) * 16
            o = pos1[h] * 32 + o2
            second_out[slot, h] = (part[slot, h, :, pl.ds(off(core * 64 + o), 16), :] + core_in[u, :, pl.ds(off(o), 16), :]
                                   + first_in[u, :, pl.ds(off(o2), 16), :])
            copies(2, i, h).start()

    def stage_act(i):
        slot = lax.rem(i, SLOTS)
        for h in range(2):
            u, mb, t = unit(i, h)
            copies(2, i, h).wait()
            o2 = pos2[h] * 16
            o = pos1[h] * 32 + o2
            tot = (part[slot, h, :, pl.ds(off(core * 64 + o), 16), :] + core_in[u, :, pl.ds(off(o), 16), :]
                   + first_in[u, :, pl.ds(off(o2), 16), :] + second_in[u])
            a, b, g = tot[0], tot[1], tot[2]
            s = jax.nn.sigmoid(a)
            silu = a * s
            r = pl.ds(off(mb * 128 + core * 64 + o), 16)
            act[t, 0, r, :] = (silu * b).astype(jnp.bfloat16)
            act[t, 1, r, :] = (g * b * s * (1.0 + a * (1.0 - s))).astype(jnp.bfloat16)
            act[t, 2, r, :] = (g * silu).astype(jnp.bfloat16)
            copies(3, i, h).start()

    def stage_forward(stage, i):
        for h in range(2):
            copies(stage - 1, i, h).wait()
            copies(stage, i, h).start()

    def add_to(arr, mb, term):
        blocks = pl.ds(mb * 8, 8)
        acc[arr, blocks] += term.reshape(8, 2, 8, term.shape[-1])

    def stage_outputs(i):
        for h in range(2):
            u, mb, t = unit(i, h)
            copies(5, i, h).wait()
            cols = pl.ds(pl.multiple_of(t * LANES, LANES), LANES)
            r = pl.ds(pl.multiple_of(mb * 128, 128), 128)
            add_to(0, mb, dot_f32(act[t, 0, r, :], wd[cols, :]))
            grads = jnp.concatenate([act[t, 1, r, :], act[t, 2, r, :]], axis=1)
            pair = jnp.concatenate([wg[:, cols], wu[:, cols]], axis=1)
            add_to(1, mb, dot_t(grads, pair))

            pltpu.make_async_copy(act.at[t, :, r, :], act_hbm.at[t, :, r, :], store_sem.at[0]).start()

    def body(j, carry):
        def run(stage, fn):
            i = j - STARTS[stage]
            pl.when(jnp.logical_and(i >= 0, i < n_iter))(functools.partial(fn, i))

        run(5, functools.partial(stage_forward, 5))
        run(4, functools.partial(stage_forward, 4))
        run(3, stage_act)
        run(2, stage_second)
        run(1, stage_first)

        @pl.when(j == tiles // 2 - 2)
        def _():
            tokens_in(0, 1)
            tokens_in(1, 1)
            pltpu.make_async_copy(rows, tok_hbm, store_sem.at[1]).start()

        run(0, stage_partials)
        run(6, stage_outputs)
        return carry

    lax.fori_loop(0, n_iter + STARTS[6], body, 0)

    sums = [pltpu.make_async_copy(acc.at[arr, pl.ds(8 * mb, 8)], sum_hbm.at[:, :, arr, mb], store_sem.at[2 + 2 * arr + mb])
            for arr in range(2) for mb in range(2)]
    for cp in sums:
        cp.start()
    for mb in range(2):
        for arr in range(2):
            part15 = tok.at[arr, mb, pl.ds(0, 15)]
            pltpu.make_async_copy(part15, part15, tok_send.at[arr, mb]).wait()
    pltpu.make_async_copy(rows, tok_hbm, store_sem.at[1]).wait()
    pltpu.make_async_copy(act, act_hbm, store_sem.at[0]).wait()
    for cp in sums:
        cp.wait()


def exchange(x_loc, dy_loc, w_gate, w_up, w_down):
    d_loc, f_loc = w_gate.shape
    tiles = f_loc // LANES
    any_spec = pl.BlockSpec(memory_space=pl.ANY)
    f32, bf16 = jnp.float32, jnp.bfloat16
    return pl.pallas_call(
        functools.partial(exchange_kernel, tiles),
        out_shape=(jax.ShapeDtypeStruct((tiles, 3, 256, LANES), bf16),
                   jax.ShapeDtypeStruct((2, 256, d_loc), bf16),
                   jax.ShapeDtypeStruct((8, 2, 2, 2, 8, d_loc), f32)),
        in_specs=[any_spec] * 5,
        out_specs=(any_spec,) * 3,
        scratch_shapes=[
            pltpu.VMEM((2, 2, 8, 4096), bf16),
            pltpu.VMEM((2, 2, 16, 8, d_loc), bf16),
            pltpu.VMEM((2, 256, d_loc), bf16),
            pltpu.VMEM((d_loc, f_loc), bf16),
            pltpu.VMEM((d_loc, f_loc), bf16),
            pltpu.VMEM((f_loc, d_loc), bf16),
            pltpu.VMEM((SLOTS, 2, 3, 128, LANES), f32),
            pltpu.VMEM((2 * tiles, 3, 64, LANES), f32),
            pltpu.VMEM((SLOTS, 2, 3, 32, LANES), f32),
            pltpu.VMEM((2 * tiles, 3, 32, LANES), f32),
            pltpu.VMEM((SLOTS, 2, 3, 16, LANES), f32),
            pltpu.VMEM((2 * tiles, 3, 16, LANES), f32),
            pltpu.VMEM((tiles, 3, 256, LANES), bf16),
            pltpu.VMEM((2, 16, 2, 8, d_loc), f32),
            pltpu.SemaphoreType.DMA((5,)),
            pltpu.SemaphoreType.DMA((2, 2)),
            pltpu.SemaphoreType.DMA((2, 2)),
            pltpu.SemaphoreType.DMA((6, 2, SLOTS)),
            pltpu.SemaphoreType.DMA((6, 2, SLOTS)),
            pltpu.SemaphoreType.DMA((6,)),
        ],
        compiler_params=pltpu.CompilerParams(collective_id=0, has_side_effects=True, vmem_limit_bytes=60 * 2**20),
        cost_estimate=pl.CostEstimate(flops=9 * 10**9, bytes_accessed=28 * 10**6, transcendentals=0),
        name="exchange",
    )(x_loc, dy_loc, w_gate, w_up, w_down)


OUT_SLOTS = 4
WIDTH = 2 * LANES


def grads_kernel(tiles, tok_hbm, act_hbm, dg_hbm, du_hbm, dd_hbm, tok, xt, act, gate, up, down, load_sem, out_sem):
    pairs = tiles // 2
    tok_copy = pltpu.make_async_copy(tok_hbm, tok, load_sem.at[pairs + 1])
    tok_copy.start()

    def act_copy(i, n):
        span = pl.ds(2 * i, n)
        return pltpu.make_async_copy(act_hbm.at[span], act.at[span], load_sem.at[i])

    for i in range(pairs):
        act_copy(i, 2).start()
    if tiles % 2:
        act_copy(pairs, 1).start()
    tok_copy.wait()
    xt[...] = tok[0].T

    def out_copies(i, slot, width):
        cols = pl.ds(pl.multiple_of(i * WIDTH, WIDTH), width)
        part = pl.ds(0, width)
        return [pltpu.make_async_copy(gate.at[slot, :, part], dg_hbm.at[:, cols], out_sem.at[0, slot]),
                pltpu.make_async_copy(up.at[slot, :, part], du_hbm.at[:, cols], out_sem.at[1, slot]),
                pltpu.make_async_copy(down.at[slot, part, :], dd_hbm.at[cols, :], out_sem.at[2, slot])]

    def step(i, n):
        slot = lax.rem(i, OUT_SLOTS)
        act_copy(i, n).wait()

        def wait_old():
            for cp in out_copies(i - OUT_SLOTS, slot, WIDTH):
                cp.wait()

        pl.when(i >= OUT_SLOTS)(wait_old)

        def cols(kind):
            return jnp.concatenate([act[2 * i + k, kind] for k in range(n)], axis=1)

        part = slice(0, n * LANES)
        gate[slot, :, part] = dot_f32(xt[...], cols(1))
        up[slot, :, part] = dot_f32(xt[...], cols(2))
        down[slot, part, :] = lax.dot_general(cols(0), tok[1], TRANS_A, preferred_element_type=jnp.float32)
        for cp in out_copies(i, slot, n * LANES):
            cp.start()

    def body(i, carry):
        step(i, 2)
        return carry

    lax.fori_loop(0, pairs, body, 0)
    last = pairs
    if tiles % 2:
        step(pairs, 1)
        last = pairs + 1
    for i in range(last - OUT_SLOTS, last):
        for cp in out_copies(i, i % OUT_SLOTS, WIDTH if i < pairs else LANES):
            cp.wait()


def weight_grads(tok, act):
    tiles = act.shape[0]
    d_loc = tok.shape[-1]
    f_loc = tiles * LANES
    any_spec = pl.BlockSpec(memory_space=pl.ANY)
    f32, bf16 = jnp.float32, jnp.bfloat16
    return pl.pallas_call(
        functools.partial(grads_kernel, tiles), in_specs=[any_spec] * 2, out_specs=[any_spec] * 3,
        out_shape=[jax.ShapeDtypeStruct((d_loc, f_loc), f32)] * 2 + [jax.ShapeDtypeStruct((f_loc, d_loc), f32)],
        scratch_shapes=[
            pltpu.VMEM((2, 256, d_loc), bf16),
            pltpu.VMEM((d_loc, 256), bf16),
            pltpu.VMEM(act.shape, bf16),
            pltpu.VMEM((OUT_SLOTS, d_loc, WIDTH), f32),
            pltpu.VMEM((OUT_SLOTS, d_loc, WIDTH), f32),
            pltpu.VMEM((OUT_SLOTS, WIDTH, d_loc), f32),
            pltpu.SemaphoreType.DMA((tiles // 2 + 2,)),
            pltpu.SemaphoreType.DMA((3, OUT_SLOTS)),
        ],
        compiler_params=pltpu.CompilerParams(vmem_limit_bytes=62 * 2**20),
        cost_estimate=pl.CostEstimate(flops=6 * 256 * d_loc * f_loc, bytes_accessed=44 * 10**6, transcendentals=0),
        name="weight_grads",
    )(tok, act)


def solution(mesh):
    row_spec = P(None, ("dp", "tp"), None)
    in_specs = (row_spec, P("dp", "tp"), P("dp", "tp"), P("tp", "dp"), row_spec)
    out_specs = (row_spec, row_spec, P("dp", "tp"), P("dp", "tp"), P("tp", "dp"))

    def local_step(x_loc, w_gate, w_up, w_down, dy_loc):
        act, tok, part = exchange(x_loc, dy_loc, w_gate, w_up, w_down)
        part = lax.all_to_all(part.reshape(16, 2, 2, 8, -1), ("dp", "tp"), split_axis=0, concat_axis=0, tiled=True)
        part = part.reshape(8, 2, 2, 2, 8, -1)
        out = (part[:, 0] + part[:, 1]).transpose(1, 2, 3, 0, 4).reshape(2, 2, 8, 4096)
        y = (x_loc.astype(jnp.float32) + out[0]).astype(jnp.bfloat16)
        dx = (dy_loc.astype(jnp.float32) + out[1]).astype(jnp.bfloat16)
        dg, du, dd = weight_grads(tok, act)
        return y, dx, dg, du, dd

    return jax.shard_map(local_step, mesh=mesh, in_specs=in_specs, out_specs=out_specs, check_vma=False)
```

```python
import functools

import jax
import jax.numpy as jnp
from jax import lax
from jax.experimental import pallas as pl
from jax.experimental.pallas import tpu as pltpu
from jax.sharding import PartitionSpec as P

MESH = pl.DeviceIdType.MESH
LANES = 128
SLOTS = 8
LAGS = (1, 2, 2, 2, 2, 1)
STARTS = tuple(sum(LAGS[:k]) for k in range(len(LAGS) + 1))
TRANS_B = (((1,), (1,)), ((), ()))
TRANS_A = (((0,), (0,)), ((), ()))


def dot_f32(lhs, rhs):
    return jnp.dot(lhs, rhs, preferred_element_type=jnp.float32)


def dot_t(lhs, rhs):
    return lax.dot_general(lhs, rhs, TRANS_B, preferred_element_type=jnp.float32)


def exchange_kernel(tiles, x_hbm, dy_hbm, wg_hbm, wu_hbm, wd_hbm,
                    act_hbm, tok_hbm, sum_hbm, first_hbm,
                    loc, tok, rows, wg, wu, wd, part, core_in, first_out, first_in, second_out, second_in, act, acc, zin, fin, yin,
                    load_sem, tok_send, tok_recv, send_sem, recv_sem, store_sem, z_sem, fin_sem):
    tp = lax.axis_index("tp")
    dp = lax.axis_index("dp")
    core = lax.rem(dp, 2)
    xpos = lax.rem(lax.div(dp, 2), 2)
    ypos = lax.div(dp, 4)
    me = dp * 2 + tp

    def device(fc, fx, fy, fz):
        dc = 1 - core if fc else core
        dx = 1 - xpos if fx else xpos
        dy = 1 - ypos if fy else ypos
        return (1 - tp if fz else tp, dy * 4 + dx * 2 + dc)

    core_peer = device(1, 0, 0, 0)
    x_peer = device(0, 1, 0, 0)
    y_peer = device(0, 0, 1, 0)

    token_loads = [pltpu.make_async_copy(x_hbm, loc.at[0], load_sem.at[0]),
                   pltpu.make_async_copy(dy_hbm, loc.at[1], load_sem.at[1])]
    weight_loads = [pltpu.make_async_copy(wg_hbm, wg, load_sem.at[2]),
                    pltpu.make_async_copy(wu_hbm, wu, load_sem.at[3]),
                    pltpu.make_async_copy(wd_hbm, wd, load_sem.at[4])]
    for cp in token_loads + weight_loads:
        cp.start()

    others = [((k >> 0) & 1, (k >> 1) & 1, (k >> 2) & 1, (k >> 3) & 1) for k in range(15, 0, -1)]
    barrier = pltpu.get_barrier_semaphore()
    for flags in others:
        pl.semaphore_signal(barrier, 1, device_id=device(*flags), device_id_type=MESH)
    for cp in token_loads:
        cp.wait()
    pl.semaphore_wait(barrier, 15)

    for mb in range(2):
        for arr in range(2):
            for flags in others:
                dest = device(*flags)
                pltpu.make_async_remote_copy(
                    src_ref=loc.at[arr, mb, :, pl.ds(pl.multiple_of(dest[1] * 512, 512), 512)],
                    dst_ref=tok.at[arr, mb, me],
                    send_sem=tok_send.at[arr, mb], recv_sem=tok_recv.at[arr, mb],
                    device_id=dest, device_id_type=MESH).start()
    for mb in range(2):
        for arr in range(2):
            tok[arr, mb, me] = loc[arr, mb, :, pl.ds(pl.multiple_of(dp * 512, 512), 512)]

    def tokens_in(arr, mb):
        part15 = tok.at[arr, mb, pl.ds(0, 15)]
        pltpu.make_async_copy(part15, part15, tok_recv.at[arr, mb]).wait()
        for pair in range(8):
            lo = tok[arr, mb, 2 * pair].astype(jnp.float32)
            hi = tok[arr, mb, 2 * pair + 1].astype(jnp.float32)
            rows[arr, pl.ds(mb * 128 + 16 * pair, 16), :] = jnp.concatenate([lo, hi], axis=0).astype(jnp.bfloat16)

    acc[...] = jnp.zeros_like(acc)
    tokens_in(0, 0)
    tokens_in(1, 0)
    for cp in weight_loads:
        cp.wait()

    n_iter = tiles

    def unit(i, h):
        u = 2 * i + h
        mb = lax.div(u, tiles)
        return u, mb, u - tiles * mb

    keep_core = pl.multiple_of(core * 64, 64)
    send_core = pl.multiple_of((1 - core) * 64, 64)
    pos1 = (xpos, ypos)
    pos2 = (ypos, xpos)
    peer1 = (x_peer, y_peer)
    peer2 = (y_peer, x_peer)

    def off(v):
        return pl.multiple_of(v, 16)

    def copies(stage, i, h):
        u, mb, t = unit(i, h)
        slot = lax.rem(i, SLOTS)
        base = mb * 128 + core * 64
        if stage == 0:
            src, dst, dev = part.at[slot, h, :, pl.ds(send_core, 64), :], core_in.at[u], core_peer
        elif stage == 1:
            src, dst, dev = first_out.at[slot, h], first_in.at[u], peer1[h]
        elif stage == 2:
            src, dst, dev = second_out.at[slot, h], second_in.at[u], peer2[h]
        elif stage == 3:
            src = dst = act.at[t, :, pl.ds(off(base + 32 * pos1[h] + 16 * pos2[h]), 16), :]
            dev = peer2[h]
        elif stage == 4:
            src = dst = act.at[t, :, pl.ds(off(base + 32 * pos1[h]), 32), :]
            dev = peer1[h]
        else:
            src = dst = act.at[t, :, pl.ds(off(base), 64), :]
            dev = core_peer
        return pltpu.make_async_remote_copy(
            src_ref=src, dst_ref=dst, send_sem=send_sem.at[stage, h, slot], recv_sem=recv_sem.at[stage, h, slot],
            device_id=dev, device_id_type=MESH)

    def stage_partials(i):
        for h in range(2):
            u, mb, t = unit(i, h)
            slot = lax.rem(i, SLOTS)
            cols = pl.ds(pl.multiple_of(t * LANES, LANES), LANES)
            r = pl.ds(pl.multiple_of(mb * 128, 128), 128)
            pair = jnp.concatenate([wg[:, cols], wu[:, cols]], axis=1)
            ab = dot_f32(rows[0, r, :], pair)
            part[slot, h, 0] = ab[:, :LANES]
            part[slot, h, 1] = ab[:, LANES:]
            part[slot, h, 2] = dot_t(rows[1, r, :], wd[cols, :])
            copies(0, i, h).start()

    def stage_first(i):
        slot = lax.rem(i, SLOTS)
        for h in range(2):
            u, _, _ = unit(i, h)
            copies(0, i, h).wait()
            o = (1 - pos1[h]) * 32
            first_out[slot, h] = (part[slot, h, :, pl.ds(off(core * 64 + o), 32), :] + core_in[u, :, pl.ds(off(o), 32), :])
            copies(1, i, h).start()

    def stage_second(i):
        slot = lax.rem(i, SLOTS)
        for h in range(2):
            u, _, _ = unit(i, h)
            copies(1, i, h).wait()
            o2 = (1 - pos2[h]) * 16
            o = pos1[h] * 32 + o2
            second_out[slot, h] = (part[slot, h, :, pl.ds(off(core * 64 + o), 16), :] + core_in[u, :, pl.ds(off(o), 16), :]
                                   + first_in[u, :, pl.ds(off(o2), 16), :])
            copies(2, i, h).start()

    def stage_act(i):
        slot = lax.rem(i, SLOTS)
        for h in range(2):
            u, mb, t = unit(i, h)
            copies(2, i, h).wait()
            o2 = pos2[h] * 16
            o = pos1[h] * 32 + o2
            tot = (part[slot, h, :, pl.ds(off(core * 64 + o), 16), :] + core_in[u, :, pl.ds(off(o), 16), :]
                   + first_in[u, :, pl.ds(off(o2), 16), :] + second_in[u])
            a, b, g = tot[0], tot[1], tot[2]
            s = jax.nn.sigmoid(a)
            silu = a * s
            r = pl.ds(off(mb * 128 + core * 64 + o), 16)
            act[t, 0, r, :] = (silu * b).astype(jnp.bfloat16)
            act[t, 1, r, :] = (g * b * s * (1.0 + a * (1.0 - s))).astype(jnp.bfloat16)
            act[t, 2, r, :] = (g * silu).astype(jnp.bfloat16)
            copies(3, i, h).start()

    def stage_forward(stage, i):
        for h in range(2):
            copies(stage - 1, i, h).wait()
            copies(stage, i, h).start()

    def add_to(arr, mb, term):
        blocks = pl.ds(mb * 8, 8)
        acc[arr, blocks] += term.reshape(8, 2, 8, term.shape[-1])

    def stage_outputs(i):
        for h in range(2):
            u, mb, t = unit(i, h)
            copies(5, i, h).wait()
            cols = pl.ds(pl.multiple_of(t * LANES, LANES), LANES)
            r = pl.ds(pl.multiple_of(mb * 128, 128), 128)
            add_to(0, mb, dot_f32(act[t, 0, r, :], wd[cols, :]))
            grads = jnp.concatenate([act[t, 1, r, :], act[t, 2, r, :]], axis=1)
            pair = jnp.concatenate([wg[:, cols], wu[:, cols]], axis=1)
            add_to(1, mb, dot_t(grads, pair))

            pltpu.make_async_copy(act.at[t, :, r, :], act_hbm.at[t, :, r, :], store_sem.at[0]).start()

    z_copy = pltpu.make_async_remote_copy(
        src_ref=acc.at[:, pl.ds(0, 8), 1 - tp], dst_ref=zin, send_sem=z_sem.at[0], recv_sem=z_sem.at[1],
        device_id=device(0, 0, 0, 1), device_id_type=MESH)
    plane = [flags for flags in others if not flags[3]]
    my_cols = pl.ds(pl.multiple_of(dp * 512, 512), 512)

    def finish_first():
        z_copy.wait()
        for arr in range(2):
            for blk in range(8):
                total = acc[arr, blk, tp] + zin[arr, blk]
                fin[blk, arr] = (tok[arr, 0, 2 * blk + tp].astype(jnp.float32) + total).astype(jnp.bfloat16)

    def send_first():
        for flags in plane:
            dest = device(*flags)
            pltpu.make_async_remote_copy(
                src_ref=fin.at[dest[1]], dst_ref=yin.at[:, :, my_cols], send_sem=fin_sem.at[0], recv_sem=fin_sem.at[1],
                device_id=dest, device_id_type=MESH).start()
        yin[:, :, my_cols] = fin[dp]

    z_start = (tiles - 1) // 2 + STARTS[6] + 1

    def body(j, carry):
        pl.when(j == z_start)(z_copy.start)
        pl.when(j == z_start + 8)(finish_first)
        pl.when(j == n_iter + 4)(send_first)

        def run(stage, fn):
            i = j - STARTS[stage]
            pl.when(jnp.logical_and(i >= 0, i < n_iter))(functools.partial(fn, i))

        run(5, functools.partial(stage_forward, 5))
        run(4, functools.partial(stage_forward, 4))
        run(3, stage_act)
        run(2, stage_second)
        run(1, stage_first)

        @pl.when(j == tiles // 2 - 2)
        def _():
            tokens_in(0, 1)
            tokens_in(1, 1)
            pltpu.make_async_copy(rows, tok_hbm, store_sem.at[1]).start()

        run(0, stage_partials)
        run(6, stage_outputs)
        return carry

    lax.fori_loop(0, n_iter + STARTS[6], body, 0)

    sums = [pltpu.make_async_copy(acc.at[arr, pl.ds(8, 8)], sum_hbm.at[:, :, arr], store_sem.at[2 + arr]) for arr in range(2)]
    for cp in sums:
        cp.start()
    blocks = fin.at[pl.ds(0, 7)]
    for k in range(2):
        pltpu.make_async_copy(blocks, blocks, fin_sem.at[k]).wait()
    first_copy = pltpu.make_async_copy(yin, first_hbm, store_sem.at[4])
    first_copy.start()
    for mb in range(2):
        for arr in range(2):
            part15 = tok.at[arr, mb, pl.ds(0, 15)]
            pltpu.make_async_copy(part15, part15, tok_send.at[arr, mb]).wait()
    pltpu.make_async_copy(rows, tok_hbm, store_sem.at[1]).wait()
    pltpu.make_async_copy(act, act_hbm, store_sem.at[0]).wait()
    for cp in sums:
        cp.wait()
    first_copy.wait()


def exchange(x_loc, dy_loc, w_gate, w_up, w_down):
    d_loc, f_loc = w_gate.shape
    tiles = f_loc // LANES
    any_spec = pl.BlockSpec(memory_space=pl.ANY)
    f32, bf16 = jnp.float32, jnp.bfloat16
    return pl.pallas_call(
        functools.partial(exchange_kernel, tiles),
        out_shape=(jax.ShapeDtypeStruct((tiles, 3, 256, LANES), bf16),
                   jax.ShapeDtypeStruct((2, 256, d_loc), bf16),
                   jax.ShapeDtypeStruct((8, 2, 2, 8, d_loc), f32),
                   jax.ShapeDtypeStruct((2, 8, 4096), bf16)),
        in_specs=[any_spec] * 5,
        out_specs=(any_spec,) * 4,
        scratch_shapes=[
            pltpu.VMEM((2, 2, 8, 4096), bf16),
            pltpu.VMEM((2, 2, 16, 8, d_loc), bf16),
            pltpu.VMEM((2, 256, d_loc), bf16),
            pltpu.VMEM((d_loc, f_loc), bf16),
            pltpu.VMEM((d_loc, f_loc), bf16),
            pltpu.VMEM((f_loc, d_loc), bf16),
            pltpu.VMEM((SLOTS, 2, 3, 128, LANES), f32),
            pltpu.VMEM((2 * tiles, 3, 64, LANES), f32),
            pltpu.VMEM((SLOTS, 2, 3, 32, LANES), f32),
            pltpu.VMEM((2 * tiles, 3, 32, LANES), f32),
            pltpu.VMEM((SLOTS, 2, 3, 16, LANES), f32),
            pltpu.VMEM((2 * tiles, 3, 16, LANES), f32),
            pltpu.VMEM((tiles, 3, 256, LANES), bf16),
            pltpu.VMEM((2, 16, 2, 8, d_loc), f32),
            pltpu.VMEM((2, 8, 8, d_loc), f32),
            pltpu.VMEM((8, 2, 8, d_loc), bf16),
            pltpu.VMEM((2, 8, 4096), bf16),
            pltpu.SemaphoreType.DMA((5,)),
            pltpu.SemaphoreType.DMA((2, 2)),
            pltpu.SemaphoreType.DMA((2, 2)),
            pltpu.SemaphoreType.DMA((6, 2, SLOTS)),
            pltpu.SemaphoreType.DMA((6, 2, SLOTS)),
            pltpu.SemaphoreType.DMA((5,)),
            pltpu.SemaphoreType.DMA((2,)),
            pltpu.SemaphoreType.DMA((2,)),
        ],
        compiler_params=pltpu.CompilerParams(collective_id=0, has_side_effects=True, vmem_limit_bytes=60 * 2**20),
        cost_estimate=pl.CostEstimate(flops=9 * 10**9, bytes_accessed=28 * 10**6, transcendentals=0),
        name="exchange",
    )(x_loc, dy_loc, w_gate, w_up, w_down)


OUT_SLOTS = 4
WIDTH = 2 * LANES


def grads_kernel(tiles, tok_hbm, act_hbm, dg_hbm, du_hbm, dd_hbm, tok, xt, act, gate, up, down, load_sem, out_sem):
    pairs = tiles // 2
    tok_copy = pltpu.make_async_copy(tok_hbm, tok, load_sem.at[pairs + 1])
    tok_copy.start()

    def act_copy(i, n):
        span = pl.ds(2 * i, n)
        return pltpu.make_async_copy(act_hbm.at[span], act.at[span], load_sem.at[i])

    for i in range(pairs):
        act_copy(i, 2).start()
    if tiles % 2:
        act_copy(pairs, 1).start()
    tok_copy.wait()
    xt[...] = tok[0].T

    def out_copies(i, slot, width):
        cols = pl.ds(pl.multiple_of(i * WIDTH, WIDTH), width)
        part = pl.ds(0, width)
        return [pltpu.make_async_copy(gate.at[slot, :, part], dg_hbm.at[:, cols], out_sem.at[0, slot]),
                pltpu.make_async_copy(up.at[slot, :, part], du_hbm.at[:, cols], out_sem.at[1, slot]),
                pltpu.make_async_copy(down.at[slot, part, :], dd_hbm.at[cols, :], out_sem.at[2, slot])]

    def step(i, n):
        slot = lax.rem(i, OUT_SLOTS)
        act_copy(i, n).wait()

        def wait_old():
            for cp in out_copies(i - OUT_SLOTS, slot, WIDTH):
                cp.wait()

        pl.when(i >= OUT_SLOTS)(wait_old)

        def cols(kind):
            return jnp.concatenate([act[2 * i + k, kind] for k in range(n)], axis=1)

        part = slice(0, n * LANES)
        gate[slot, :, part] = dot_f32(xt[...], cols(1))
        up[slot, :, part] = dot_f32(xt[...], cols(2))
        down[slot, part, :] = lax.dot_general(cols(0), tok[1], TRANS_A, preferred_element_type=jnp.float32)
        for cp in out_copies(i, slot, n * LANES):
            cp.start()

    def body(i, carry):
        step(i, 2)
        return carry

    lax.fori_loop(0, pairs, body, 0)
    last = pairs
    if tiles % 2:
        step(pairs, 1)
        last = pairs + 1
    for i in range(last - OUT_SLOTS, last):
        for cp in out_copies(i, i % OUT_SLOTS, WIDTH if i < pairs else LANES):
            cp.wait()


def weight_grads(tok, act):
    tiles = act.shape[0]
    d_loc = tok.shape[-1]
    f_loc = tiles * LANES
    any_spec = pl.BlockSpec(memory_space=pl.ANY)
    f32, bf16 = jnp.float32, jnp.bfloat16
    return pl.pallas_call(
        functools.partial(grads_kernel, tiles), in_specs=[any_spec] * 2, out_specs=[any_spec] * 3,
        out_shape=[jax.ShapeDtypeStruct((d_loc, f_loc), f32)] * 2 + [jax.ShapeDtypeStruct((f_loc, d_loc), f32)],
        scratch_shapes=[
            pltpu.VMEM((2, 256, d_loc), bf16),
            pltpu.VMEM((d_loc, 256), bf16),
            pltpu.VMEM(act.shape, bf16),
            pltpu.VMEM((OUT_SLOTS, d_loc, WIDTH), f32),
            pltpu.VMEM((OUT_SLOTS, d_loc, WIDTH), f32),
            pltpu.VMEM((OUT_SLOTS, WIDTH, d_loc), f32),
            pltpu.SemaphoreType.DMA((tiles // 2 + 2,)),
            pltpu.SemaphoreType.DMA((3, OUT_SLOTS)),
        ],
        compiler_params=pltpu.CompilerParams(vmem_limit_bytes=62 * 2**20),
        cost_estimate=pl.CostEstimate(flops=6 * 256 * d_loc * f_loc, bytes_accessed=44 * 10**6, transcendentals=0),
        name="weight_grads",
    )(tok, act)


def solution(mesh):
    row_spec = P(None, ("dp", "tp"), None)
    in_specs = (row_spec, P("dp", "tp"), P("dp", "tp"), P("tp", "dp"), row_spec)
    out_specs = (row_spec, row_spec, P("dp", "tp"), P("dp", "tp"), P("tp", "dp"))

    def local_step(x_loc, w_gate, w_up, w_down, dy_loc):
        act, tok, part, first = exchange(x_loc, dy_loc, w_gate, w_up, w_down)
        part = lax.all_to_all(part.reshape(16, 2, 8, -1), ("dp", "tp"), split_axis=0, concat_axis=0, tiled=True)
        part = part.reshape(8, 2, 2, 8, -1)
        out = (part[:, 0] + part[:, 1]).transpose(1, 2, 0, 3).reshape(2, 8, 4096)
        y = jnp.stack([first[0], (x_loc[1].astype(jnp.float32) + out[0]).astype(jnp.bfloat16)])
        dx = jnp.stack([first[1], (dy_loc[1].astype(jnp.float32) + out[1]).astype(jnp.bfloat16)])
        dg, du, dd = weight_grads(tok, act)
        return y, dx, dg, du, dd

    return jax.shard_map(local_step, mesh=mesh, in_specs=in_specs, out_specs=out_specs, check_vma=False)
```

```python
import functools

import jax
import jax.numpy as jnp
from jax import lax
from jax.experimental import pallas as pl
from jax.experimental.pallas import tpu as pltpu
from jax.sharding import PartitionSpec as P

MESH = pl.DeviceIdType.MESH
LANES = 128
SLOTS = 8
LATE_SLOTS = 16
DEFER = 7
LAGS = (1, 2, 2, 2, 2, 1)
STARTS = tuple(sum(LAGS[:k]) for k in range(len(LAGS) + 1))
TRANS_B = (((1,), (1,)), ((), ()))
TRANS_A = (((0,), (0,)), ((), ()))


def dot_f32(lhs, rhs):
    return jnp.dot(lhs, rhs, preferred_element_type=jnp.float32)


def dot_t(lhs, rhs):
    return lax.dot_general(lhs, rhs, TRANS_B, preferred_element_type=jnp.float32)


def exchange_kernel(tiles, x_hbm, dy_hbm, wg_hbm, wu_hbm, wd_hbm,
                    act_hbm, tok_hbm, sum_hbm, y_hbm, dx_hbm,
                    loc, tok, rows, wg, wu, wd, part, core_in, first_out, first_in, second_out, second_in, act, acc, zin, fin, yin,
                    load_sem, tok_send, tok_recv, send_sem, recv_sem, late_sem, gather_sem, store_sem, z_sem, fin_sem):
    tp = lax.axis_index("tp")
    dp = lax.axis_index("dp")
    core = lax.rem(dp, 2)
    xpos = lax.rem(lax.div(dp, 2), 2)
    ypos = lax.div(dp, 4)
    me = dp * 2 + tp

    def device(fc, fx, fy, fz):
        dc = 1 - core if fc else core
        dx = 1 - xpos if fx else xpos
        dy = 1 - ypos if fy else ypos
        return (1 - tp if fz else tp, dy * 4 + dx * 2 + dc)

    core_peer = device(1, 0, 0, 0)
    x_peer = device(0, 1, 0, 0)
    y_peer = device(0, 0, 1, 0)

    token_loads = [pltpu.make_async_copy(x_hbm, loc.at[0], load_sem.at[0]),
                   pltpu.make_async_copy(dy_hbm, loc.at[1], load_sem.at[1])]
    weight_loads = [pltpu.make_async_copy(wg_hbm, wg, load_sem.at[2]),
                    pltpu.make_async_copy(wu_hbm, wu, load_sem.at[3]),
                    pltpu.make_async_copy(wd_hbm, wd, load_sem.at[4])]
    for cp in token_loads + weight_loads:
        cp.start()

    others = [((k >> 0) & 1, (k >> 1) & 1, (k >> 2) & 1, (k >> 3) & 1) for k in range(15, 0, -1)]
    barrier = pltpu.get_barrier_semaphore()
    for flags in others:
        pl.semaphore_signal(barrier, 1, device_id=device(*flags), device_id_type=MESH)
    for cp in token_loads:
        cp.wait()
    pl.semaphore_wait(barrier, 15)

    for mb in range(2):
        for arr in range(2):
            for flags in others:
                dest = device(*flags)
                pltpu.make_async_remote_copy(
                    src_ref=loc.at[arr, mb, :, pl.ds(pl.multiple_of(dest[1] * 512, 512), 512)],
                    dst_ref=tok.at[arr, mb, me],
                    send_sem=tok_send.at[arr, mb], recv_sem=tok_recv.at[arr, mb],
                    device_id=dest, device_id_type=MESH).start()
    for mb in range(2):
        for arr in range(2):
            tok[arr, mb, me] = loc[arr, mb, :, pl.ds(pl.multiple_of(dp * 512, 512), 512)]

    def tokens_in(arr, mb):
        part15 = tok.at[arr, mb, pl.ds(0, 15)]
        pltpu.make_async_copy(part15, part15, tok_recv.at[arr, mb]).wait()
        for pair in range(8):
            lo = tok[arr, mb, 2 * pair].astype(jnp.float32)
            hi = tok[arr, mb, 2 * pair + 1].astype(jnp.float32)
            rows[arr, pl.ds(mb * 128 + 16 * pair, 16), :] = jnp.concatenate([lo, hi], axis=0).astype(jnp.bfloat16)

    acc[...] = jnp.zeros_like(acc)
    tokens_in(0, 0)
    tokens_in(1, 0)
    for cp in weight_loads:
        cp.wait()

    n_iter = tiles

    def unit(i, h):
        u = 2 * i + h
        mb = lax.div(u, tiles)
        return u, mb, u - tiles * mb

    keep_core = pl.multiple_of(core * 64, 64)
    send_core = pl.multiple_of((1 - core) * 64, 64)
    pos1 = (xpos, ypos)
    pos2 = (ypos, xpos)
    peer1 = (x_peer, y_peer)
    peer2 = (y_peer, x_peer)

    def off(v):
        return pl.multiple_of(v, 16)

    def copies(stage, i, h):
        u, mb, t = unit(i, h)
        slot = lax.rem(i, SLOTS)
        base = mb * 128 + core * 64
        if stage == 0:
            src, dst, dev = part.at[slot, h, :, pl.ds(send_core, 64), :], core_in.at[u], core_peer
        elif stage == 1:
            src, dst, dev = first_out.at[slot, h], first_in.at[u], peer1[h]
        elif stage == 2:
            src, dst, dev = second_out.at[slot, h], second_in.at[u], peer2[h]
        elif stage == 3:
            src = dst = act.at[t, :, pl.ds(off(base + 32 * pos1[h] + 16 * pos2[h]), 16), :]
            dev = peer2[h]
        elif stage == 4:
            src = dst = act.at[t, :, pl.ds(off(base + 32 * pos1[h]), 32), :]
            dev = peer1[h]
        else:
            src = dst = act.at[t, :, pl.ds(off(base), 64), :]
            dev = core_peer
        return pltpu.make_async_remote_copy(
            src_ref=src, dst_ref=dst, send_sem=send_sem.at[stage, slot] if stage < 3 else gather_sem.at[0],
            recv_sem=arrival(stage, i), device_id=dev, device_id_type=MESH)

    def arrival(stage, i):
        if stage < 3:
            return recv_sem.at[stage, lax.rem(i, SLOTS)]
        return late_sem.at[stage - 3, lax.rem(i, LATE_SLOTS)]

    def start_pair(stage, i):
        for h in range(2):
            copies(stage, i, h).start()

    def wait_pair(stage, i):
        if stage < 3:
            into = (core_in, first_in, second_in)[stage].at[pl.ds(2 * i, 2)]
            pltpu.make_async_copy(into, into, send_sem.at[stage, lax.rem(i, SLOTS)]).wait()
        else:
            into = act.at[0, :, pl.ds(0, 32 << (stage - 3)), :]
        pltpu.make_async_copy(into, into, arrival(stage, i)).wait()

    def stage_partials(i):
        for h in range(2):
            u, mb, t = unit(i, h)
            slot = lax.rem(i, SLOTS)
            cols = pl.ds(pl.multiple_of(t * LANES, LANES), LANES)
            r = pl.ds(pl.multiple_of(mb * 128, 128), 128)
            pair = jnp.concatenate([wg[:, cols], wu[:, cols]], axis=1)
            ab = dot_f32(rows[0, r, :], pair)
            part[slot, h, 0] = ab[:, :LANES]
            part[slot, h, 1] = ab[:, LANES:]
            part[slot, h, 2] = dot_t(rows[1, r, :], wd[cols, :])
        start_pair(0, i)

    def stage_first(i):
        slot = lax.rem(i, SLOTS)
        wait_pair(0, i)
        for h in range(2):
            u, _, _ = unit(i, h)
            o = (1 - pos1[h]) * 32
            first_out[slot, h] = (part[slot, h, :, pl.ds(off(core * 64 + o), 32), :] + core_in[u, :, pl.ds(off(o), 32), :])
            copies(1, i, h).start()

    def stage_second(i):
        slot = lax.rem(i, SLOTS)
        wait_pair(1, i)
        for h in range(2):
            u, _, _ = unit(i, h)
            o2 = (1 - pos2[h]) * 16
            o = pos1[h] * 32 + o2
            second_out[slot, h] = (part[slot, h, :, pl.ds(off(core * 64 + o), 16), :] + core_in[u, :, pl.ds(off(o), 16), :]
                                   + first_in[u, :, pl.ds(off(o2), 16), :])
            copies(2, i, h).start()

    def stage_act(i):
        slot = lax.rem(i, SLOTS)
        wait_pair(2, i)
        for h in range(2):
            u, mb, t = unit(i, h)
            o2 = pos2[h] * 16
            o = pos1[h] * 32 + o2
            tot = (part[slot, h, :, pl.ds(off(core * 64 + o), 16), :] + core_in[u, :, pl.ds(off(o), 16), :]
                   + first_in[u, :, pl.ds(off(o2), 16), :] + second_in[u])
            a, b, g = tot[0], tot[1], tot[2]
            s = jax.nn.sigmoid(a)
            silu = a * s
            r = pl.ds(off(mb * 128 + core * 64 + o), 16)
            act[t, 0, r, :] = (silu * b).astype(jnp.bfloat16)
            act[t, 1, r, :] = (g * b * s * (1.0 + a * (1.0 - s))).astype(jnp.bfloat16)
            act[t, 2, r, :] = (g * silu).astype(jnp.bfloat16)
            copies(3, i, h).start()

    def stage_forward(stage, i):
        wait_pair(stage - 1, i)
        start_pair(stage, i)

    def add_to(arr, mb, term):
        blocks = pl.ds(mb * 8, 8)
        acc[arr, blocks] += term.reshape(8, 2, 8, term.shape[-1])

    def stage_outputs(i):
        wait_pair(5, i)
        for h in range(2):
            u, mb, t = unit(i, h)
            cols = pl.ds(pl.multiple_of(t * LANES, LANES), LANES)
            r = pl.ds(pl.multiple_of(mb * 128, 128), 128)
            add_to(0, mb, dot_f32(act[t, 0, r, :], wd[cols, :]))
            grads = jnp.concatenate([act[t, 1, r, :], act[t, 2, r, :]], axis=1)
            pair = jnp.concatenate([wg[:, cols], wu[:, cols]], axis=1)
            add_to(1, mb, dot_t(grads, pair))

            pltpu.make_async_copy(act.at[t, :, r, :], act_hbm.at[t, :, r, :], store_sem.at[0]).start()

    z_copy = pltpu.make_async_remote_copy(
        src_ref=acc.at[:, pl.ds(0, 8), 1 - tp], dst_ref=zin, send_sem=z_sem.at[0], recv_sem=z_sem.at[1],
        device_id=device(0, 0, 0, 1), device_id_type=MESH)
    plane = [flags for flags in others if not flags[3]]
    my_cols = pl.ds(pl.multiple_of(dp * 512, 512), 512)

    def finish_first():
        z_copy.wait()
        for arr in range(2):
            for blk in range(8):
                total = acc[arr, blk, tp] + zin[arr, blk]
                fin[blk, arr] = (tok[arr, 0, 2 * blk + tp].astype(jnp.float32) + total).astype(jnp.bfloat16)

    def send_first():
        for flags in plane:
            dest = device(*flags)
            pltpu.make_async_remote_copy(
                src_ref=fin.at[dest[1]], dst_ref=yin.at[:, :, my_cols], send_sem=fin_sem.at[0], recv_sem=fin_sem.at[1],
                device_id=dest, device_id_type=MESH).start()
        yin[:, :, my_cols] = fin[dp]

    z_start = (tiles - 1) // 2 + STARTS[6] + DEFER + 1

    def forwarded(j):
        ready = jnp.maximum(j - STARTS[4] + 1, 0)
        late = jnp.maximum(j - STARTS[4] + 1 - DEFER, 0) + jnp.maximum(j - n_iter + 1, 0)
        return jnp.minimum(n_iter, jnp.minimum(ready, late))

    def run_late(j, fn):
        def step(i, carry):
            fn(i)
            return carry

        lax.fori_loop(forwarded(j - 1), forwarded(j), step, 0)

    def body(j, carry):
        pl.when(j == z_start)(z_copy.start)
        pl.when(j == z_start + 5)(finish_first)
        pl.when(j == n_iter + 4)(send_first)

        def run(stage, fn):
            i = j - STARTS[stage]
            pl.when(jnp.logical_and(i >= 0, i < n_iter))(functools.partial(fn, i))

        run(3, stage_act)
        run(2, stage_second)
        run(1, stage_first)
        run_late(j, functools.partial(stage_forward, 4))
        run_late(j - LAGS[4], functools.partial(stage_forward, 5))

        @pl.when(j == tiles // 2 - 2)
        def _():
            tokens_in(0, 1)
            tokens_in(1, 1)
            pltpu.make_async_copy(rows, tok_hbm, store_sem.at[1]).start()

        run(0, stage_partials)
        run_late(j - LAGS[4] - LAGS[5], stage_outputs)
        return carry

    lax.fori_loop(0, n_iter + STARTS[6], body, 0)

    sums = [pltpu.make_async_copy(acc.at[arr, pl.ds(8, 8)], sum_hbm.at[:, :, arr], store_sem.at[2 + arr]) for arr in range(2)]
    for cp in sums:
        cp.start()
    blocks = fin.at[pl.ds(0, 7)]
    for k in range(2):
        pltpu.make_async_copy(blocks, blocks, fin_sem.at[k]).wait()
    firsts = [pltpu.make_async_copy(yin.at[k], ref, store_sem.at[4 + k]) for k, ref in enumerate((y_hbm, dx_hbm))]
    for cp in firsts:
        cp.start()
    for mb in range(2):
        for arr in range(2):
            part15 = tok.at[arr, mb, pl.ds(0, 15)]
            pltpu.make_async_copy(part15, part15, tok_send.at[arr, mb]).wait()
    pltpu.make_async_copy(rows, tok_hbm, store_sem.at[1]).wait()
    pltpu.make_async_copy(act, act_hbm, store_sem.at[0]).wait()
    sent = act.at[:, :, pl.ds(0, 224), :]
    pltpu.make_async_copy(sent, sent, gather_sem.at[0]).wait()
    for cp in sums + firsts:
        cp.wait()


def exchange(x_loc, dy_loc, w_gate, w_up, w_down):
    d_loc, f_loc = w_gate.shape
    tiles = f_loc // LANES
    any_spec = pl.BlockSpec(memory_space=pl.ANY)
    f32, bf16 = jnp.float32, jnp.bfloat16
    return pl.pallas_call(
        functools.partial(exchange_kernel, tiles),
        out_shape=(jax.ShapeDtypeStruct((tiles, 3, 256, LANES), bf16),
                   jax.ShapeDtypeStruct((2, 256, d_loc), bf16),
                   jax.ShapeDtypeStruct((8, 2, 2, 8, d_loc), f32),
                   *[jax.ShapeDtypeStruct((8, 4096), bf16)] * 2),
        in_specs=[any_spec] * 5,
        out_specs=(any_spec,) * 5,
        scratch_shapes=[
            pltpu.VMEM((2, 2, 8, 4096), bf16),
            pltpu.VMEM((2, 2, 16, 8, d_loc), bf16),
            pltpu.VMEM((2, 256, d_loc), bf16),
            pltpu.VMEM((d_loc, f_loc), bf16),
            pltpu.VMEM((d_loc, f_loc), bf16),
            pltpu.VMEM((f_loc, d_loc), bf16),
            pltpu.VMEM((SLOTS, 2, 3, 128, LANES), f32),
            pltpu.VMEM((2 * tiles, 3, 64, LANES), f32),
            pltpu.VMEM((SLOTS, 2, 3, 32, LANES), f32),
            pltpu.VMEM((2 * tiles, 3, 32, LANES), f32),
            pltpu.VMEM((SLOTS, 2, 3, 16, LANES), f32),
            pltpu.VMEM((2 * tiles, 3, 16, LANES), f32),
            pltpu.VMEM((tiles, 3, 256, LANES), bf16),
            pltpu.VMEM((2, 16, 2, 8, d_loc), f32),
            pltpu.VMEM((2, 8, 8, d_loc), f32),
            pltpu.VMEM((8, 2, 8, d_loc), bf16),
            pltpu.VMEM((2, 8, 4096), bf16),
            pltpu.SemaphoreType.DMA((5,)),
            pltpu.SemaphoreType.DMA((2, 2)),
            pltpu.SemaphoreType.DMA((2, 2)),
            pltpu.SemaphoreType.DMA((3, SLOTS)),
            pltpu.SemaphoreType.DMA((3, SLOTS)),
            pltpu.SemaphoreType.DMA((3, LATE_SLOTS)),
            pltpu.SemaphoreType.DMA((1,)),
            pltpu.SemaphoreType.DMA((6,)),
            pltpu.SemaphoreType.DMA((2,)),
            pltpu.SemaphoreType.DMA((2,)),
        ],
        compiler_params=pltpu.CompilerParams(collective_id=0, has_side_effects=True, vmem_limit_bytes=60 * 2**20),
        cost_estimate=pl.CostEstimate(flops=9 * 10**9, bytes_accessed=28 * 10**6, transcendentals=0),
        name="exchange",
    )(x_loc, dy_loc, w_gate, w_up, w_down)


OUT_SLOTS = 4
WIDTH = 2 * LANES


def grads_kernel(tiles, tok_hbm, act_hbm, dg_hbm, du_hbm, dd_hbm, tok, xt, act, gate, up, down, load_sem, out_sem):
    pairs = tiles // 2
    tok_copy = pltpu.make_async_copy(tok_hbm, tok, load_sem.at[pairs + 1])
    tok_copy.start()

    def act_copy(i, n):
        span = pl.ds(2 * i, n)
        return pltpu.make_async_copy(act_hbm.at[span], act.at[span], load_sem.at[i])

    for i in range(pairs):
        act_copy(i, 2).start()
    if tiles % 2:
        act_copy(pairs, 1).start()
    tok_copy.wait()
    xt[...] = tok[0].T

    def out_copies(i, slot, width):
        cols = pl.ds(pl.multiple_of(i * WIDTH, WIDTH), width)
        part = pl.ds(0, width)
        return [pltpu.make_async_copy(gate.at[slot, :, part], dg_hbm.at[:, cols], out_sem.at[0, slot]),
                pltpu.make_async_copy(up.at[slot, :, part], du_hbm.at[:, cols], out_sem.at[1, slot]),
                pltpu.make_async_copy(down.at[slot, part, :], dd_hbm.at[cols, :], out_sem.at[2, slot])]

    def step(i, n):
        slot = lax.rem(i, OUT_SLOTS)
        act_copy(i, n).wait()

        def wait_old():
            for cp in out_copies(i - OUT_SLOTS, slot, WIDTH):
                cp.wait()

        pl.when(i >= OUT_SLOTS)(wait_old)

        def cols(kind):
            return jnp.concatenate([act[2 * i + k, kind] for k in range(n)], axis=1)

        part = slice(0, n * LANES)
        gate[slot, :, part] = dot_f32(xt[...], cols(1))
        up[slot, :, part] = dot_f32(xt[...], cols(2))
        down[slot, part, :] = lax.dot_general(cols(0), tok[1], TRANS_A, preferred_element_type=jnp.float32)
        for cp in out_copies(i, slot, n * LANES):
            cp.start()

    def body(i, carry):
        step(i, 2)
        return carry

    lax.fori_loop(0, pairs, body, 0)
    last = pairs
    if tiles % 2:
        step(pairs, 1)
        last = pairs + 1
    for i in range(last - OUT_SLOTS, last):
        for cp in out_copies(i, i % OUT_SLOTS, WIDTH if i < pairs else LANES):
            cp.wait()


def weight_grads(tok, act):
    tiles = act.shape[0]
    d_loc = tok.shape[-1]
    f_loc = tiles * LANES
    any_spec = pl.BlockSpec(memory_space=pl.ANY)
    f32, bf16 = jnp.float32, jnp.bfloat16
    return pl.pallas_call(
        functools.partial(grads_kernel, tiles), in_specs=[any_spec] * 2, out_specs=[any_spec] * 3,
        out_shape=[jax.ShapeDtypeStruct((d_loc, f_loc), f32)] * 2 + [jax.ShapeDtypeStruct((f_loc, d_loc), f32)],
        scratch_shapes=[
            pltpu.VMEM((2, 256, d_loc), bf16),
            pltpu.VMEM((d_loc, 256), bf16),
            pltpu.VMEM(act.shape, bf16),
            pltpu.VMEM((OUT_SLOTS, d_loc, WIDTH), f32),
            pltpu.VMEM((OUT_SLOTS, d_loc, WIDTH), f32),
            pltpu.VMEM((OUT_SLOTS, WIDTH, d_loc), f32),
            pltpu.SemaphoreType.DMA((tiles // 2 + 2,)),
            pltpu.SemaphoreType.DMA((3, OUT_SLOTS)),
        ],
        compiler_params=pltpu.CompilerParams(vmem_limit_bytes=62 * 2**20),
        cost_estimate=pl.CostEstimate(flops=6 * 256 * d_loc * f_loc, bytes_accessed=44 * 10**6, transcendentals=0),
        name="weight_grads",
    )(tok, act)


def solution(mesh):
    row_spec = P(None, ("dp", "tp"), None)
    in_specs = (row_spec, P("dp", "tp"), P("dp", "tp"), P("tp", "dp"), row_spec)
    out_specs = (row_spec, row_spec, P("dp", "tp"), P("dp", "tp"), P("tp", "dp"))

    def local_step(x_loc, w_gate, w_up, w_down, dy_loc):
        act, tok, part, y_first, dx_first = exchange(x_loc, dy_loc, w_gate, w_up, w_down)
        part = lax.all_to_all(part.reshape(16, 2, 8, -1), ("dp", "tp"), split_axis=0, concat_axis=0, tiled=True)
        part = part.reshape(8, 2, 2, 8, -1)
        out = (part[:, 0] + part[:, 1]).transpose(1, 2, 0, 3).reshape(2, 8, 4096)
        y = jnp.stack([y_first, (x_loc[1].astype(jnp.float32) + out[0]).astype(jnp.bfloat16)])
        dx = jnp.stack([dx_first, (dy_loc[1].astype(jnp.float32) + out[1]).astype(jnp.bfloat16)])
        dg, du, dd = weight_grads(tok, act)
        return y, dx, dg, du, dd

    return jax.shard_map(local_step, mesh=mesh, in_specs=in_specs, out_specs=out_specs, check_vma=False)
```

```python
import functools

import jax
import jax.numpy as jnp
from jax import lax
from jax.experimental import pallas as pl
from jax.experimental.pallas import tpu as pltpu
from jax.sharding import PartitionSpec as P

MESH = pl.DeviceIdType.MESH
LANES = 128
SLOTS = 8
LATE_SLOTS = 16
DEFER = 8
LAGS = (3, 3, 2, 2, 2, 1)
STARTS = tuple(sum(LAGS[:k]) for k in range(len(LAGS) + 1))
TRANS_B = (((1,), (1,)), ((), ()))
TRANS_A = (((0,), (0,)), ((), ()))


def dot_f32(lhs, rhs):
    return jnp.dot(lhs, rhs, preferred_element_type=jnp.float32)


def dot_t(lhs, rhs):
    return lax.dot_general(lhs, rhs, TRANS_B, preferred_element_type=jnp.float32)


def exchange_kernel(tiles, x_hbm, dy_hbm, wg_hbm, wu_hbm, wd_hbm,
                    act_hbm, xt_hbm, dy_rows_hbm, sum_hbm, y_hbm, dx_hbm,
                    loc, tok, rows, wg, wu, wd, part, core_in, first_out, first_in, second_out, second_in, act, acc, zin, fin, yin, xt,
                    load_sem, tok_send, tok_recv, send_sem, recv_sem, late_sem, gather_sem, lead_sem, store_sem, z_sem, fin_sem):
    tp = lax.axis_index("tp")
    dp = lax.axis_index("dp")
    core = lax.rem(dp, 2)
    xpos = lax.rem(lax.div(dp, 2), 2)
    ypos = lax.div(dp, 4)
    me = dp * 2 + tp

    def device(fc, fx, fy, fz):
        dc = 1 - core if fc else core
        dx = 1 - xpos if fx else xpos
        dy = 1 - ypos if fy else ypos
        return (1 - tp if fz else tp, dy * 4 + dx * 2 + dc)

    core_peer = device(1, 0, 0, 0)
    x_peer = device(0, 1, 0, 0)
    y_peer = device(0, 0, 1, 0)

    token_loads = [pltpu.make_async_copy(x_hbm, loc.at[0], load_sem.at[0]),
                   pltpu.make_async_copy(dy_hbm, loc.at[1], load_sem.at[1])]
    weight_loads = [pltpu.make_async_copy(wg_hbm, wg, load_sem.at[2]),
                    pltpu.make_async_copy(wu_hbm, wu, load_sem.at[3]),
                    pltpu.make_async_copy(wd_hbm, wd, load_sem.at[4])]
    for cp in token_loads + weight_loads:
        cp.start()

    others = [((k >> 0) & 1, (k >> 1) & 1, (k >> 2) & 1, (k >> 3) & 1) for k in range(15, 0, -1)]
    barrier = pltpu.get_barrier_semaphore()
    for flags in others:
        pl.semaphore_signal(barrier, 1, device_id=device(*flags), device_id_type=MESH)
    for cp in token_loads:
        cp.wait()
    pl.semaphore_wait(barrier, 15)

    for mb in range(2):
        for arr in range(2):
            for flags in others:
                dest = device(*flags)
                pltpu.make_async_remote_copy(
                    src_ref=loc.at[arr, mb, :, pl.ds(pl.multiple_of(dest[1] * 512, 512), 512)],
                    dst_ref=tok.at[arr, mb, me],
                    send_sem=tok_send.at[arr, mb], recv_sem=tok_recv.at[arr, mb],
                    device_id=dest, device_id_type=MESH).start()
    for mb in range(2):
        for arr in range(2):
            tok[arr, mb, me] = loc[arr, mb, :, pl.ds(pl.multiple_of(dp * 512, 512), 512)]

    def tokens_in(arr, mb):
        part15 = tok.at[arr, mb, pl.ds(0, 15)]
        pltpu.make_async_copy(part15, part15, tok_recv.at[arr, mb]).wait()
        for pair in range(8):
            lo = tok[arr, mb, 2 * pair].astype(jnp.float32)
            hi = tok[arr, mb, 2 * pair + 1].astype(jnp.float32)
            rows[arr, pl.ds(mb * 128 + 16 * pair, 16), :] = jnp.concatenate([lo, hi], axis=0).astype(jnp.bfloat16)

    acc[...] = jnp.zeros_like(acc)

    n_iter = tiles

    def unit(i, h):
        u = 2 * i + h
        mb = lax.div(u, tiles)
        return u, mb, u - tiles * mb

    keep_core = pl.multiple_of(core * 64, 64)
    send_core = pl.multiple_of((1 - core) * 64, 64)
    pos1 = (xpos, ypos)
    pos2 = (ypos, xpos)
    peer1 = (x_peer, y_peer)
    peer2 = (y_peer, x_peer)

    def off(v):
        return pl.multiple_of(v, 16)

    def copies(stage, i, h):
        u, mb, t = unit(i, h)
        slot = lax.rem(i, SLOTS)
        base = mb * 128 + core * 64
        if stage == 0:
            src, dst, dev = part.at[slot, h, :, pl.ds(send_core, 64), :], core_in.at[u], core_peer
        elif stage == 1:
            src, dst, dev = first_out.at[slot, h], first_in.at[u], peer1[h]
        elif stage == 2:
            src, dst, dev = second_out.at[slot, h], second_in.at[u], peer2[h]
        elif stage == 3:
            src = dst = act.at[t, :, pl.ds(off(base + 32 * pos1[h] + 16 * pos2[h]), 16), :]
            dev = peer2[h]
        elif stage == 4:
            src = dst = act.at[t, :, pl.ds(off(base + 32 * pos1[h]), 32), :]
            dev = peer1[h]
        else:
            src = dst = act.at[t, :, pl.ds(off(base), 64), :]
            dev = core_peer
        return pltpu.make_async_remote_copy(
            src_ref=src, dst_ref=dst, send_sem=send_sem.at[stage, slot] if stage < 3 else gather_sem.at[0],
            recv_sem=arrival(stage, i), device_id=dev, device_id_type=MESH)

    def arrival(stage, i):
        if stage < 3:
            return recv_sem.at[stage, lax.rem(i, SLOTS)]
        return late_sem.at[stage - 3, lax.rem(i, LATE_SLOTS)]

    def start_pair(stage, i):
        for h in range(2):
            copies(stage, i, h).start()

    def wait_pair(stage, i):
        if stage < 3:
            into = (core_in, first_in, second_in)[stage].at[pl.ds(2 * i, 2)]
            pltpu.make_async_copy(into, into, send_sem.at[stage, lax.rem(i, SLOTS)]).wait()
        else:
            into = act.at[0, :, pl.ds(0, 32 << (stage - 3)), :]
        pltpu.make_async_copy(into, into, arrival(stage, i)).wait()

    def gate_up_partials(i, h):
        u, mb, t = unit(i, h)
        slot = lax.rem(i, SLOTS)
        cols = pl.ds(pl.multiple_of(t * LANES, LANES), LANES)
        r = pl.ds(pl.multiple_of(mb * 128, 128), 128)
        pair = jnp.concatenate([wg[:, cols], wu[:, cols]], axis=1)
        ab = dot_f32(rows[0, r, :], pair)
        part[slot, h, 0] = ab[:, :LANES]
        part[slot, h, 1] = ab[:, LANES:]

    def down_partials(i, h):
        u, mb, t = unit(i, h)
        cols = pl.ds(pl.multiple_of(t * LANES, LANES), LANES)
        r = pl.ds(pl.multiple_of(mb * 128, 128), 128)
        part[lax.rem(i, SLOTS), h, 2] = dot_t(rows[1, r, :], wd[cols, :])

    def stage_partials(i):
        for h in range(2):
            gate_up_partials(i, h)
            down_partials(i, h)
        start_pair(0, i)

    def lead_in():
        kinds = (pl.ds(0, 2), pl.ds(2, 1))

        def to_core(k):
            for h in range(2):
                pltpu.make_async_remote_copy(
                    src_ref=part.at[0, h, kinds[k], pl.ds(send_core, 64), :], dst_ref=core_in.at[h, kinds[k]],
                    send_sem=lead_sem.at[0, k], recv_sem=lead_sem.at[1, k], device_id=core_peer, device_id_type=MESH).start()

        def to_first(k):
            both = core_in.at[pl.ds(0, 2), kinds[k]]
            for way in range(2):
                pltpu.make_async_copy(both, both, lead_sem.at[way, k]).wait()
            for h in range(2):
                o = (1 - pos1[h]) * 32
                first_out[0, h, kinds[k]] = (part[0, h, kinds[k], pl.ds(off(core * 64 + o), 32), :]
                                             + core_in[h, kinds[k], pl.ds(off(o), 32), :])
                pltpu.make_async_remote_copy(
                    src_ref=first_out.at[0, h, kinds[k]], dst_ref=first_in.at[h, kinds[k]], send_sem=send_sem.at[1, 0],
                    recv_sem=arrival(1, 0), device_id=peer1[h], device_id_type=MESH).start()

        tokens_in(0, 0)
        for cp in weight_loads[:2]:
            cp.wait()
        for h in range(2):
            gate_up_partials(0, h)
        to_core(0)
        tokens_in(1, 0)
        weight_loads[2].wait()
        for h in range(2):
            down_partials(0, h)
        to_core(1)
        to_first(0)
        for i in range(1, STARTS[1]):
            stage_partials(i)
        to_first(1)

    def stage_first(i):
        slot = lax.rem(i, SLOTS)
        wait_pair(0, i)
        for h in range(2):
            u, _, _ = unit(i, h)
            o = (1 - pos1[h]) * 32
            first_out[slot, h] = (part[slot, h, :, pl.ds(off(core * 64 + o), 32), :] + core_in[u, :, pl.ds(off(o), 32), :])
            copies(1, i, h).start()

    def stage_second(i):
        slot = lax.rem(i, SLOTS)
        wait_pair(1, i)
        for h in range(2):
            u, _, _ = unit(i, h)
            o2 = (1 - pos2[h]) * 16
            o = pos1[h] * 32 + o2
            second_out[slot, h] = (part[slot, h, :, pl.ds(off(core * 64 + o), 16), :] + core_in[u, :, pl.ds(off(o), 16), :]
                                   + first_in[u, :, pl.ds(off(o2), 16), :])
            copies(2, i, h).start()

    def stage_act(i):
        slot = lax.rem(i, SLOTS)
        wait_pair(2, i)
        for h in range(2):
            u, mb, t = unit(i, h)
            o2 = pos2[h] * 16
            o = pos1[h] * 32 + o2
            tot = (part[slot, h, :, pl.ds(off(core * 64 + o), 16), :] + core_in[u, :, pl.ds(off(o), 16), :]
                   + first_in[u, :, pl.ds(off(o2), 16), :] + second_in[u])
            a, b, g = tot[0], tot[1], tot[2]
            s = jax.nn.sigmoid(a)
            silu = a * s
            r = pl.ds(off(mb * 128 + core * 64 + o), 16)
            act[t, 0, r, :] = (silu * b).astype(jnp.bfloat16)
            act[t, 1, r, :] = (g * b * s * (1.0 + a * (1.0 - s))).astype(jnp.bfloat16)
            act[t, 2, r, :] = (g * silu).astype(jnp.bfloat16)
            copies(3, i, h).start()

    def stage_forward(stage, i):
        wait_pair(stage - 1, i)
        start_pair(stage, i)

    def add_to(arr, mb, term):
        blocks = pl.ds(mb * 8, 8)
        acc[arr, blocks] += term.reshape(8, 2, 8, term.shape[-1])

    def stage_outputs(i):
        wait_pair(5, i)
        for h in range(2):
            u, mb, t = unit(i, h)
            cols = pl.ds(pl.multiple_of(t * LANES, LANES), LANES)
            r = pl.ds(pl.multiple_of(mb * 128, 128), 128)
            pltpu.make_async_copy(act.at[t, :, r, :], act_hbm.at[t, :, r, :], store_sem.at[0]).start()
            add_to(0, mb, dot_f32(act[t, 0, r, :], wd[cols, :]))
            grads = jnp.concatenate([act[t, 1, r, :], act[t, 2, r, :]], axis=1)
            pair = jnp.concatenate([wg[:, cols], wu[:, cols]], axis=1)
            add_to(1, mb, dot_t(grads, pair))

    z_copy = pltpu.make_async_remote_copy(
        src_ref=acc.at[:, pl.ds(0, 8), 1 - tp], dst_ref=zin, send_sem=z_sem.at[0], recv_sem=z_sem.at[1],
        device_id=device(0, 0, 0, 1), device_id_type=MESH)
    plane = [flags for flags in others if not flags[3]]
    my_cols = pl.ds(pl.multiple_of(dp * 512, 512), 512)

    def finish_first():
        z_copy.wait()
        for arr in range(2):
            for blk in range(8):
                total = acc[arr, blk, tp] + zin[arr, blk]
                fin[blk, arr] = (tok[arr, 0, 2 * blk + tp].astype(jnp.float32) + total).astype(jnp.bfloat16)

    def send_first():
        for flags in plane:
            dest = device(*flags)
            pltpu.make_async_remote_copy(
                src_ref=fin.at[dest[1]], dst_ref=yin.at[:, :, my_cols], send_sem=fin_sem.at[0], recv_sem=fin_sem.at[1],
                device_id=dest, device_id_type=MESH).start()
        yin[:, :, my_cols] = fin[dp]

    firsts = [pltpu.make_async_copy(yin.at[k], ref, store_sem.at[4 + k]) for k, ref in enumerate((y_hbm, dx_hbm))]

    def store_first():
        blocks = fin.at[pl.ds(0, 7)]
        for k in range(2):
            pltpu.make_async_copy(blocks, blocks, fin_sem.at[k]).wait()
        for cp in firsts:
            cp.start()

    z_start = (tiles - 1) // 2 + STARTS[6] + DEFER + 1

    def forwarded(j):
        ready = jnp.maximum(j - STARTS[4] + 1, 0)
        late = jnp.maximum(j - STARTS[4] + 1 - DEFER, 0) + jnp.maximum(j - n_iter - STARTS[1] + 2, 0)
        return jnp.minimum(n_iter, jnp.minimum(ready, late))

    def run_late(j, fn):
        def step(i, carry):
            fn(i)
            return carry

        lax.fori_loop(forwarded(j - 1), forwarded(j), step, 0)

    row_stores = [pltpu.make_async_copy(xt, xt_hbm, store_sem.at[1]), pltpu.make_async_copy(rows.at[1], dy_rows_hbm, store_sem.at[6])]

    def body(j, carry):
        pl.when(j == z_start)(z_copy.start)
        pl.when(j == n_iter + STARTS[3] - 2)(finish_first)
        pl.when(j == n_iter + STARTS[3] - 1)(send_first)
        pl.when(j == n_iter + STARTS[6] - 2)(store_first)

        def run(stage, fn):
            i = j - STARTS[stage]
            pl.when(jnp.logical_and(i >= (1 if stage == 1 else 0), i < n_iter))(functools.partial(fn, i))

        run(3, stage_act)
        run(2, stage_second)
        run(1, stage_first)
        run_late(j, functools.partial(stage_forward, 4))
        run_late(j - LAGS[4], functools.partial(stage_forward, 5))

        @pl.when(j == tiles // 2 - 2)
        def _():
            tokens_in(0, 1)
            tokens_in(1, 1)
            xt[...] = rows[0].T
            for cp in row_stores:
                cp.start()

        run(0, stage_partials)
        run_late(j - LAGS[4] - LAGS[5], stage_outputs)
        return carry

    lead_in()
    lax.fori_loop(STARTS[1], n_iter + STARTS[6], body, 0)

    sums = [pltpu.make_async_copy(acc.at[arr, pl.ds(8, 8)], sum_hbm.at[:, :, arr], store_sem.at[2 + arr]) for arr in range(2)]
    for cp in sums:
        cp.start()
    for mb in range(2):
        for arr in range(2):
            part15 = tok.at[arr, mb, pl.ds(0, 15)]
            pltpu.make_async_copy(part15, part15, tok_send.at[arr, mb]).wait()
    for cp in row_stores:
        cp.wait()
    pltpu.make_async_copy(act, act_hbm, store_sem.at[0]).wait()
    sent = act.at[:, :, pl.ds(0, 224), :]
    pltpu.make_async_copy(sent, sent, gather_sem.at[0]).wait()
    for cp in sums + firsts:
        cp.wait()


def exchange(x_loc, dy_loc, w_gate, w_up, w_down):
    d_loc, f_loc = w_gate.shape
    tiles = f_loc // LANES
    any_spec = pl.BlockSpec(memory_space=pl.ANY)
    f32, bf16 = jnp.float32, jnp.bfloat16
    return pl.pallas_call(
        functools.partial(exchange_kernel, tiles),
        out_shape=(jax.ShapeDtypeStruct((tiles, 3, 256, LANES), bf16),
                   jax.ShapeDtypeStruct((d_loc, 256), bf16),
                   jax.ShapeDtypeStruct((256, d_loc), bf16),
                   jax.ShapeDtypeStruct((8, 2, 2, 8, d_loc), f32),
                   *[jax.ShapeDtypeStruct((8, 4096), bf16)] * 2),
        in_specs=[any_spec] * 5,
        out_specs=(any_spec,) * 6,
        scratch_shapes=[
            pltpu.VMEM((2, 2, 8, 4096), bf16),
            pltpu.VMEM((2, 2, 16, 8, d_loc), bf16),
            pltpu.VMEM((2, 256, d_loc), bf16),
            pltpu.VMEM((d_loc, f_loc), bf16),
            pltpu.VMEM((d_loc, f_loc), bf16),
            pltpu.VMEM((f_loc, d_loc), bf16),
            pltpu.VMEM((SLOTS, 2, 3, 128, LANES), f32),
            pltpu.VMEM((2 * tiles, 3, 64, LANES), f32),
            pltpu.VMEM((SLOTS, 2, 3, 32, LANES), f32),
            pltpu.VMEM((2 * tiles, 3, 32, LANES), f32),
            pltpu.VMEM((SLOTS, 2, 3, 16, LANES), f32),
            pltpu.VMEM((2 * tiles, 3, 16, LANES), f32),
            pltpu.VMEM((tiles, 3, 256, LANES), bf16),
            pltpu.VMEM((2, 16, 2, 8, d_loc), f32),
            pltpu.VMEM((2, 8, 8, d_loc), f32),
            pltpu.VMEM((8, 2, 8, d_loc), bf16),
            pltpu.VMEM((2, 8, 4096), bf16),
            pltpu.VMEM((d_loc, 256), bf16),
            pltpu.SemaphoreType.DMA((5,)),
            pltpu.SemaphoreType.DMA((2, 2)),
            pltpu.SemaphoreType.DMA((2, 2)),
            pltpu.SemaphoreType.DMA((3, SLOTS)),
            pltpu.SemaphoreType.DMA((3, SLOTS)),
            pltpu.SemaphoreType.DMA((3, LATE_SLOTS)),
            pltpu.SemaphoreType.DMA((1,)),
            pltpu.SemaphoreType.DMA((2, 2)),
            pltpu.SemaphoreType.DMA((7,)),
            pltpu.SemaphoreType.DMA((2,)),
            pltpu.SemaphoreType.DMA((2,)),
        ],
        compiler_params=pltpu.CompilerParams(collective_id=0, has_side_effects=True, vmem_limit_bytes=60 * 2**20),
        cost_estimate=pl.CostEstimate(flops=9 * 10**9, bytes_accessed=28 * 10**6, transcendentals=0),
        name="exchange",
    )(x_loc, dy_loc, w_gate, w_up, w_down)


OUT_SLOTS = 4
WIDTH = 2 * LANES


def grads_kernel(tiles, xt_hbm, dy_hbm, act_hbm, dg_hbm, du_hbm, dd_hbm, xt, dy, act, gate, up, down, load_sem, out_sem):
    pairs = tiles // 2
    row_loads = [pltpu.make_async_copy(xt_hbm, xt, load_sem.at[pairs + 1]), pltpu.make_async_copy(dy_hbm, dy, load_sem.at[pairs + 2])]
    for cp in row_loads:
        cp.start()

    def act_copy(i, n):
        span = pl.ds(2 * i, n)
        return pltpu.make_async_copy(act_hbm.at[span], act.at[span], load_sem.at[i])

    for i in range(pairs):
        act_copy(i, 2).start()
    if tiles % 2:
        act_copy(pairs, 1).start()
    for cp in row_loads:
        cp.wait()

    def out_copies(i, slot, width):
        cols = pl.ds(pl.multiple_of(i * WIDTH, WIDTH), width)
        part = pl.ds(0, width)
        return [pltpu.make_async_copy(gate.at[slot, :, part], dg_hbm.at[:, cols], out_sem.at[0, slot]),
                pltpu.make_async_copy(up.at[slot, :, part], du_hbm.at[:, cols], out_sem.at[1, slot]),
                pltpu.make_async_copy(down.at[slot, part, :], dd_hbm.at[cols, :], out_sem.at[2, slot])]

    def step(i, n):
        slot = lax.rem(i, OUT_SLOTS)
        act_copy(i, n).wait()

        def wait_old():
            for cp in out_copies(i - OUT_SLOTS, slot, WIDTH):
                cp.wait()

        pl.when(i >= OUT_SLOTS)(wait_old)

        def cols(kind):
            return jnp.concatenate([act[2 * i + k, kind] for k in range(n)], axis=1)

        part = slice(0, n * LANES)
        gate[slot, :, part] = dot_f32(xt[...], cols(1))
        up[slot, :, part] = dot_f32(xt[...], cols(2))
        down[slot, part, :] = lax.dot_general(cols(0), dy[...], TRANS_A, preferred_element_type=jnp.float32)
        for cp in out_copies(i, slot, n * LANES):
            cp.start()

    def body(i, carry):
        step(i, 2)
        return carry

    lax.fori_loop(0, pairs, body, 0)
    last = pairs
    if tiles % 2:
        step(pairs, 1)
        last = pairs + 1
    for i in range(last - OUT_SLOTS, last):
        for cp in out_copies(i, i % OUT_SLOTS, WIDTH if i < pairs else LANES):
            cp.wait()


def weight_grads(xt, dy_rows, act):
    tiles = act.shape[0]
    d_loc = xt.shape[0]
    f_loc = tiles * LANES
    any_spec = pl.BlockSpec(memory_space=pl.ANY)
    f32, bf16 = jnp.float32, jnp.bfloat16
    return pl.pallas_call(
        functools.partial(grads_kernel, tiles), in_specs=[any_spec] * 3, out_specs=[any_spec] * 3,
        out_shape=[jax.ShapeDtypeStruct((d_loc, f_loc), f32)] * 2 + [jax.ShapeDtypeStruct((f_loc, d_loc), f32)],
        scratch_shapes=[
            pltpu.VMEM((d_loc, 256), bf16),
            pltpu.VMEM((256, d_loc), bf16),
            pltpu.VMEM(act.shape, bf16),
            pltpu.VMEM((OUT_SLOTS, d_loc, WIDTH), f32),
            pltpu.VMEM((OUT_SLOTS, d_loc, WIDTH), f32),
            pltpu.VMEM((OUT_SLOTS, WIDTH, d_loc), f32),
            pltpu.SemaphoreType.DMA((tiles // 2 + 3,)),
            pltpu.SemaphoreType.DMA((3, OUT_SLOTS)),
        ],
        compiler_params=pltpu.CompilerParams(vmem_limit_bytes=62 * 2**20),
        cost_estimate=pl.CostEstimate(flops=6 * 256 * d_loc * f_loc, bytes_accessed=44 * 10**6, transcendentals=0),
        name="weight_grads",
    )(xt, dy_rows, act)


def solution(mesh):
    row_spec = P(None, ("dp", "tp"), None)
    in_specs = (row_spec, P("dp", "tp"), P("dp", "tp"), P("tp", "dp"), row_spec)
    out_specs = (row_spec, row_spec, P("dp", "tp"), P("dp", "tp"), P("tp", "dp"))

    def local_step(x_loc, w_gate, w_up, w_down, dy_loc):
        act, xt, dy_rows, part, y_first, dx_first = exchange(x_loc, dy_loc, w_gate, w_up, w_down)
        part = lax.all_to_all(part.reshape(16, 2, 8, -1), ("dp", "tp"), split_axis=0, concat_axis=0, tiled=True)
        part = part.reshape(8, 2, 2, 8, -1)
        out = (part[:, 0] + part[:, 1]).transpose(1, 2, 0, 3).reshape(2, 8, 4096)
        y = jnp.stack([y_first, (x_loc[1].astype(jnp.float32) + out[0]).astype(jnp.bfloat16)])
        dx = jnp.stack([dx_first, (dy_loc[1].astype(jnp.float32) + out[1]).astype(jnp.bfloat16)])
        dg, du, dd = weight_grads(xt, dy_rows, act)
        return y, dx, dg, du, dd

    return jax.shard_map(local_step, mesh=mesh, in_specs=in_specs, out_specs=out_specs, check_vma=False)
```

```python
import functools

import jax
import jax.numpy as jnp
from jax import lax
from jax.experimental import pallas as pl
from jax.experimental.pallas import tpu as pltpu
from jax.sharding import PartitionSpec as P

MESH = pl.DeviceIdType.MESH
LANES = 128
SLOTS = 8
LATE_SLOTS = 12
DEFER = 6
LAGS = (3, 3, 2, 2, 2, 1)
STARTS = tuple(sum(LAGS[:k]) for k in range(len(LAGS) + 1))
TRANS_B = (((1,), (1,)), ((), ()))
TRANS_A = (((0,), (0,)), ((), ()))


def dot_f32(lhs, rhs):
    return jnp.dot(lhs, rhs, preferred_element_type=jnp.float32)


def dot_t(lhs, rhs):
    return lax.dot_general(lhs, rhs, TRANS_B, preferred_element_type=jnp.float32)


def exchange_kernel(tiles, x_hbm, dy_hbm, wg_hbm, wu_hbm, wd_hbm,
                    act_hbm, xt_hbm, dy_rows_hbm, sum_hbm, y_hbm, dx_hbm,
                    loc, tok, rows, wg, wu, wd, part, core_in, first_out, first_in, second_out, second_in, act, acc, zin, fin, yin, xt,
                    load_sem, tok_send, tok_recv, send_sem, recv_sem, late_sem, gather_sem, lead_sem, plane_sem, store_sem, z_sem, fin_sem):
    tp = lax.axis_index("tp")
    dp = lax.axis_index("dp")
    core = lax.rem(dp, 2)
    xpos = lax.rem(lax.div(dp, 2), 2)
    ypos = lax.div(dp, 4)
    me = tp * 8 + dp

    def device(fc, fx, fy, fz):
        dc = 1 - core if fc else core
        dx = 1 - xpos if fx else xpos
        dy = 1 - ypos if fy else ypos
        return (1 - tp if fz else tp, dy * 4 + dx * 2 + dc)

    core_peer = device(1, 0, 0, 0)
    x_peer = device(0, 1, 0, 0)
    y_peer = device(0, 0, 1, 0)

    token_loads = [pltpu.make_async_copy(x_hbm, loc.at[0], load_sem.at[0]),
                   pltpu.make_async_copy(dy_hbm, loc.at[1], load_sem.at[1])]
    weight_loads = [pltpu.make_async_copy(wg_hbm, wg, load_sem.at[2]),
                    pltpu.make_async_copy(wu_hbm, wu, load_sem.at[3]),
                    pltpu.make_async_copy(wd_hbm, wd, load_sem.at[4])]
    for cp in token_loads + weight_loads:
        cp.start()

    others = [((k >> 0) & 1, (k >> 1) & 1, (k >> 2) & 1, (k >> 3) & 1) for k in range(15, 0, -1)]
    barrier = pltpu.get_barrier_semaphore()
    for flags in others:
        pl.semaphore_signal(barrier, 1, device_id=device(*flags), device_id_type=MESH)
    for cp in token_loads:
        cp.wait()
    pl.semaphore_wait(barrier, 15)

    plane = [flags for flags in others if not flags[3]]
    for mb in range(2):
        for arr in range(2):
            for flags in (plane if mb else others):
                dest = device(*flags)
                pltpu.make_async_remote_copy(
                    src_ref=loc.at[arr, mb, :, pl.ds(pl.multiple_of(dest[1] * 512, 512), 512)],
                    dst_ref=tok.at[arr, mb, me],
                    send_sem=tok_send.at[arr, mb], recv_sem=tok_recv.at[arr, mb],
                    device_id=dest, device_id_type=MESH).start()
    for mb in range(2):
        for arr in range(2):
            tok[arr, mb, me] = loc[arr, mb, :, pl.ds(pl.multiple_of(dp * 512, 512), 512)]

    def plane_copy(arr):
        slab = tok.at[arr, 1, pl.ds(pl.multiple_of(8 * tp, 8), 8)]
        return pltpu.make_async_remote_copy(
            src_ref=slab, dst_ref=slab, send_sem=plane_sem.at[0, arr], recv_sem=plane_sem.at[1, arr],
            device_id=device(0, 0, 0, 1), device_id_type=MESH)

    def send_plane():
        for arr in range(2):
            got = tok.at[arr, 1, pl.ds(0, 7)]
            pltpu.make_async_copy(got, got, tok_recv.at[arr, 1]).wait()
            plane_copy(arr).start()

    def tokens_in(arr, mb):
        if mb:
            plane_copy(arr).wait()
        else:
            part15 = tok.at[arr, 0, pl.ds(0, 15)]
            pltpu.make_async_copy(part15, part15, tok_recv.at[arr, 0]).wait()
        for pair in range(8):
            lo = tok[arr, mb, pair].astype(jnp.float32)
            hi = tok[arr, mb, 8 + pair].astype(jnp.float32)
            rows[arr, pl.ds(mb * 128 + 16 * pair, 16), :] = jnp.concatenate([lo, hi], axis=0).astype(jnp.bfloat16)

    acc[...] = jnp.zeros_like(acc)

    n_iter = tiles

    def unit(i, h):
        u = 2 * i + h
        mb = lax.div(u, tiles)
        return u, mb, u - tiles * mb

    keep_core = pl.multiple_of(core * 64, 64)
    send_core = pl.multiple_of((1 - core) * 64, 64)
    pos1 = (xpos, ypos)
    pos2 = (ypos, xpos)
    peer1 = (x_peer, y_peer)
    peer2 = (y_peer, x_peer)

    def off(v):
        return pl.multiple_of(v, 16)

    def copies(stage, i, h):
        u, mb, t = unit(i, h)
        slot = lax.rem(i, SLOTS)
        base = mb * 128 + core * 64
        if stage == 0:
            src, dst, dev = part.at[slot, h, :, pl.ds(send_core, 64), :], core_in.at[u], core_peer
        elif stage == 1:
            src, dst, dev = first_out.at[slot, h], first_in.at[u], peer1[h]
        elif stage == 2:
            src, dst, dev = second_out.at[slot, h], second_in.at[u], peer2[h]
        elif stage == 3:
            src = dst = act.at[t, :, pl.ds(off(base + 32 * pos1[h] + 16 * pos2[h]), 16), :]
            dev = peer2[h]
        elif stage == 4:
            src = dst = act.at[t, :, pl.ds(off(base + 32 * pos1[h]), 32), :]
            dev = peer1[h]
        else:
            src = dst = act.at[t, :, pl.ds(off(base), 64), :]
            dev = core_peer
        return pltpu.make_async_remote_copy(
            src_ref=src, dst_ref=dst, send_sem=send_sem.at[stage, slot] if stage < 3 else gather_sem.at[0],
            recv_sem=arrival(stage, i), device_id=dev, device_id_type=MESH)

    def arrival(stage, i):
        if stage < 3:
            return recv_sem.at[stage, lax.rem(i, SLOTS)]
        return late_sem.at[stage - 3, lax.rem(i, LATE_SLOTS)]

    def start_pair(stage, i):
        for h in range(2):
            copies(stage, i, h).start()

    def wait_pair(stage, i):
        if stage < 3:
            into = (core_in, first_in, second_in)[stage].at[pl.ds(2 * i, 2)]
            pltpu.make_async_copy(into, into, send_sem.at[stage, lax.rem(i, SLOTS)]).wait()
        else:
            into = act.at[0, :, pl.ds(0, 32 << (stage - 3)), :]
        pltpu.make_async_copy(into, into, arrival(stage, i)).wait()

    def gate_up_partials(i, h):
        u, mb, t = unit(i, h)
        slot = lax.rem(i, SLOTS)
        cols = pl.ds(pl.multiple_of(t * LANES, LANES), LANES)
        r = pl.ds(pl.multiple_of(mb * 128, 128), 128)
        pair = jnp.concatenate([wg[:, cols], wu[:, cols]], axis=1)
        ab = dot_f32(rows[0, r, :], pair)
        part[slot, h, 0] = ab[:, :LANES]
        part[slot, h, 1] = ab[:, LANES:]

    def down_partials(i, h):
        u, mb, t = unit(i, h)
        cols = pl.ds(pl.multiple_of(t * LANES, LANES), LANES)
        r = pl.ds(pl.multiple_of(mb * 128, 128), 128)
        part[lax.rem(i, SLOTS), h, 2] = dot_t(rows[1, r, :], wd[cols, :])

    def stage_partials(i):
        for h in range(2):
            gate_up_partials(i, h)
            down_partials(i, h)
        start_pair(0, i)

    def lead_in():
        kinds = (pl.ds(0, 2), pl.ds(2, 1))

        def to_core(k):
            for h in range(2):
                pltpu.make_async_remote_copy(
                    src_ref=part.at[0, h, kinds[k], pl.ds(send_core, 64), :], dst_ref=core_in.at[h, kinds[k]],
                    send_sem=lead_sem.at[0, k], recv_sem=lead_sem.at[1, k], device_id=core_peer, device_id_type=MESH).start()

        def to_first(k):
            both = core_in.at[pl.ds(0, 2), kinds[k]]
            for way in range(2):
                pltpu.make_async_copy(both, both, lead_sem.at[way, k]).wait()
            for h in range(2):
                o = (1 - pos1[h]) * 32
                first_out[0, h, kinds[k]] = (part[0, h, kinds[k], pl.ds(off(core * 64 + o), 32), :]
                                             + core_in[h, kinds[k], pl.ds(off(o), 32), :])
                pltpu.make_async_remote_copy(
                    src_ref=first_out.at[0, h, kinds[k]], dst_ref=first_in.at[h, kinds[k]], send_sem=send_sem.at[1, 0],
                    recv_sem=arrival(1, 0), device_id=peer1[h], device_id_type=MESH).start()

        tokens_in(0, 0)
        for cp in weight_loads[:2]:
            cp.wait()
        for h in range(2):
            gate_up_partials(0, h)
        to_core(0)
        tokens_in(1, 0)
        weight_loads[2].wait()
        for h in range(2):
            down_partials(0, h)
        to_core(1)
        to_first(0)
        for i in range(1, STARTS[1]):
            stage_partials(i)
        to_first(1)

    def stage_first(i):
        slot = lax.rem(i, SLOTS)
        wait_pair(0, i)
        for h in range(2):
            u, _, _ = unit(i, h)
            o = (1 - pos1[h]) * 32
            first_out[slot, h] = (part[slot, h, :, pl.ds(off(core * 64 + o), 32), :] + core_in[u, :, pl.ds(off(o), 32), :])
            copies(1, i, h).start()

    def stage_second(i):
        slot = lax.rem(i, SLOTS)
        wait_pair(1, i)
        for h in range(2):
            u, _, _ = unit(i, h)
            o2 = (1 - pos2[h]) * 16
            o = pos1[h] * 32 + o2
            second_out[slot, h] = (part[slot, h, :, pl.ds(off(core * 64 + o), 16), :] + core_in[u, :, pl.ds(off(o), 16), :]
                                   + first_in[u, :, pl.ds(off(o2), 16), :])
            copies(2, i, h).start()

    def stage_act(i):
        slot = lax.rem(i, SLOTS)
        wait_pair(2, i)
        for h in range(2):
            u, mb, t = unit(i, h)
            o2 = pos2[h] * 16
            o = pos1[h] * 32 + o2
            tot = (part[slot, h, :, pl.ds(off(core * 64 + o), 16), :] + core_in[u, :, pl.ds(off(o), 16), :]
                   + first_in[u, :, pl.ds(off(o2), 16), :] + second_in[u])
            a, b, g = tot[0], tot[1], tot[2]
            s = jax.nn.sigmoid(a)
            silu = a * s
            r = pl.ds(off(mb * 128 + core * 64 + o), 16)
            act[t, 0, r, :] = (silu * b).astype(jnp.bfloat16)
            act[t, 1, r, :] = (g * b * s * (1.0 + a * (1.0 - s))).astype(jnp.bfloat16)
            act[t, 2, r, :] = (g * silu).astype(jnp.bfloat16)
            copies(3, i, h).start()

    def stage_forward(stage, i):
        wait_pair(stage - 1, i)
        start_pair(stage, i)

    def add_to(arr, mb, term):
        blocks = pl.ds(mb * 8, 8)
        acc[arr, blocks] += term.reshape(8, 2, 8, term.shape[-1])

    def stage_outputs(i):
        wait_pair(5, i)
        for h in range(2):
            u, mb, t = unit(i, h)
            cols = pl.ds(pl.multiple_of(t * LANES, LANES), LANES)
            r = pl.ds(pl.multiple_of(mb * 128, 128), 128)
            pltpu.make_async_copy(act.at[t, :, r, :], act_hbm.at[t, :, r, :], store_sem.at[0]).start()
            add_to(0, mb, dot_f32(act[t, 0, r, :], wd[cols, :]))
            grads = jnp.concatenate([act[t, 1, r, :], act[t, 2, r, :]], axis=1)
            pair = jnp.concatenate([wg[:, cols], wu[:, cols]], axis=1)
            add_to(1, mb, dot_t(grads, pair))

    z_copy = pltpu.make_async_remote_copy(
        src_ref=acc.at[:, pl.ds(0, 8), 1 - tp], dst_ref=zin, send_sem=z_sem.at[0], recv_sem=z_sem.at[1],
        device_id=device(0, 0, 0, 1), device_id_type=MESH)
    my_cols = pl.ds(pl.multiple_of(dp * 512, 512), 512)

    def finish_first():
        z_copy.wait()
        for arr in range(2):
            for blk in range(8):
                total = acc[arr, blk, tp] + zin[arr, blk]
                fin[blk, arr] = (tok[arr, 0, 8 * tp + blk].astype(jnp.float32) + total).astype(jnp.bfloat16)

    def send_first():
        for flags in plane:
            dest = device(*flags)
            pltpu.make_async_remote_copy(
                src_ref=fin.at[dest[1]], dst_ref=yin.at[:, :, my_cols], send_sem=fin_sem.at[0], recv_sem=fin_sem.at[1],
                device_id=dest, device_id_type=MESH).start()
        yin[:, :, my_cols] = fin[dp]

    firsts = [pltpu.make_async_copy(yin.at[k], ref, store_sem.at[4 + k]) for k, ref in enumerate((y_hbm, dx_hbm))]

    def store_first():
        blocks = fin.at[pl.ds(0, 7)]
        for k in range(2):
            pltpu.make_async_copy(blocks, blocks, fin_sem.at[k]).wait()
        for cp in firsts:
            cp.start()

    z_start = (tiles - 1) // 2 + STARTS[6] + DEFER + 1

    def forwarded(j):
        ready = jnp.maximum(j - STARTS[4] + 1, 0)
        late = jnp.maximum(j - STARTS[4] + 1 - DEFER, 0) + jnp.maximum(j - n_iter - STARTS[1] + 2, 0)
        return jnp.minimum(n_iter, jnp.minimum(ready, late))

    def run_late(j, fn):
        def step(i, carry):
            fn(i)
            return carry

        lax.fori_loop(forwarded(j - 1), forwarded(j), step, 0)

    row_stores = [pltpu.make_async_copy(xt, xt_hbm, store_sem.at[1]), pltpu.make_async_copy(rows.at[1], dy_rows_hbm, store_sem.at[6])]

    def body(j, carry):
        pl.when(j == STARTS[1] + 4)(send_plane)
        pl.when(j == z_start)(z_copy.start)
        pl.when(j == n_iter + STARTS[3] - 2)(finish_first)

        def run(stage, fn):
            i = j - STARTS[stage]
            pl.when(jnp.logical_and(i >= (1 if stage == 1 else 0), i < n_iter))(functools.partial(fn, i))

        run(1, stage_first)
        run(2, stage_second)
        run(3, stage_act)
        run_late(j, functools.partial(stage_forward, 4))
        pl.when(j == n_iter + STARTS[4] - 1)(send_first)
        run_late(j - LAGS[4], functools.partial(stage_forward, 5))

        @pl.when(j == tiles // 2 - 2)
        def _():
            tokens_in(0, 1)
            tokens_in(1, 1)
            xt[...] = rows[0].T
            for cp in row_stores:
                cp.start()

        run(0, stage_partials)
        run_late(j - LAGS[4] - LAGS[5], stage_outputs)
        return carry

    lead_in()
    lax.fori_loop(STARTS[1], n_iter + STARTS[6], body, 0)

    sums = [pltpu.make_async_copy(acc.at[arr, pl.ds(8, 8)], sum_hbm.at[:, :, arr], store_sem.at[2 + arr]) for arr in range(2)]
    for cp in sums:
        cp.start()
    store_first()
    for mb in range(2):
        for arr in range(2):
            sent = tok.at[arr, mb, pl.ds(0, 7 if mb else 15)]
            pltpu.make_async_copy(sent, sent, tok_send.at[arr, mb]).wait()
    for cp in row_stores:
        cp.wait()
    pltpu.make_async_copy(act, act_hbm, store_sem.at[0]).wait()
    sent = act.at[:, :, pl.ds(0, 224), :]
    pltpu.make_async_copy(sent, sent, gather_sem.at[0]).wait()
    for cp in sums + firsts:
        cp.wait()


def exchange(x_loc, dy_loc, w_gate, w_up, w_down):
    d_loc, f_loc = w_gate.shape
    tiles = f_loc // LANES
    any_spec = pl.BlockSpec(memory_space=pl.ANY)
    f32, bf16 = jnp.float32, jnp.bfloat16
    return pl.pallas_call(
        functools.partial(exchange_kernel, tiles),
        out_shape=(jax.ShapeDtypeStruct((tiles, 3, 256, LANES), bf16),
                   jax.ShapeDtypeStruct((d_loc, 256), bf16),
                   jax.ShapeDtypeStruct((256, d_loc), bf16),
                   jax.ShapeDtypeStruct((8, 2, 2, 8, d_loc), f32),
                   *[jax.ShapeDtypeStruct((8, 4096), bf16)] * 2),
        in_specs=[any_spec] * 5,
        out_specs=(any_spec,) * 6,
        scratch_shapes=[
            pltpu.VMEM((2, 2, 8, 4096), bf16),
            pltpu.VMEM((2, 2, 16, 8, d_loc), bf16),
            pltpu.VMEM((2, 256, d_loc), bf16),
            pltpu.VMEM((d_loc, f_loc), bf16),
            pltpu.VMEM((d_loc, f_loc), bf16),
            pltpu.VMEM((f_loc, d_loc), bf16),
            pltpu.VMEM((SLOTS, 2, 3, 128, LANES), f32),
            pltpu.VMEM((2 * tiles, 3, 64, LANES), f32),
            pltpu.VMEM((SLOTS, 2, 3, 32, LANES), f32),
            pltpu.VMEM((2 * tiles, 3, 32, LANES), f32),
            pltpu.VMEM((SLOTS, 2, 3, 16, LANES), f32),
            pltpu.VMEM((2 * tiles, 3, 16, LANES), f32),
            pltpu.VMEM((tiles, 3, 256, LANES), bf16),
            pltpu.VMEM((2, 16, 2, 8, d_loc), f32),
            pltpu.VMEM((2, 8, 8, d_loc), f32),
            pltpu.VMEM((8, 2, 8, d_loc), bf16),
            pltpu.VMEM((2, 8, 4096), bf16),
            pltpu.VMEM((d_loc, 256), bf16),
            pltpu.SemaphoreType.DMA((5,)),
            pltpu.SemaphoreType.DMA((2, 2)),
            pltpu.SemaphoreType.DMA((2, 2)),
            pltpu.SemaphoreType.DMA((3, SLOTS)),
            pltpu.SemaphoreType.DMA((3, SLOTS)),
            pltpu.SemaphoreType.DMA((3, LATE_SLOTS)),
            pltpu.SemaphoreType.DMA((1,)),
            pltpu.SemaphoreType.DMA((2, 2)),
            pltpu.SemaphoreType.DMA((2, 2)),
            pltpu.SemaphoreType.DMA((7,)),
            pltpu.SemaphoreType.DMA((2,)),
            pltpu.SemaphoreType.DMA((2,)),
        ],
        compiler_params=pltpu.CompilerParams(collective_id=0, has_side_effects=True, vmem_limit_bytes=60 * 2**20),
        cost_estimate=pl.CostEstimate(flops=9 * 10**9, bytes_accessed=28 * 10**6, transcendentals=0),
        name="exchange",
    )(x_loc, dy_loc, w_gate, w_up, w_down)


OUT_SLOTS = 4
WIDTH = 2 * LANES


def grads_kernel(tiles, xt_hbm, dy_hbm, act_hbm, dg_hbm, du_hbm, dd_hbm, xt, dy, act, gate, up, down, load_sem, out_sem):
    pairs = tiles // 2
    row_loads = [pltpu.make_async_copy(xt_hbm, xt, load_sem.at[pairs + 1]), pltpu.make_async_copy(dy_hbm, dy, load_sem.at[pairs + 2])]
    for cp in row_loads:
        cp.start()

    def act_copy(i, n):
        span = pl.ds(2 * i, n)
        return pltpu.make_async_copy(act_hbm.at[span], act.at[span], load_sem.at[i])

    for i in range(pairs):
        act_copy(i, 2).start()
    if tiles % 2:
        act_copy(pairs, 1).start()
    for cp in row_loads:
        cp.wait()

    def out_copies(i, slot, width):
        cols = pl.ds(pl.multiple_of(i * WIDTH, WIDTH), width)
        part = pl.ds(0, width)
        return [pltpu.make_async_copy(gate.at[slot, :, part], dg_hbm.at[:, cols], out_sem.at[0, slot]),
                pltpu.make_async_copy(up.at[slot, :, part], du_hbm.at[:, cols], out_sem.at[1, slot]),
                pltpu.make_async_copy(down.at[slot, part, :], dd_hbm.at[cols, :], out_sem.at[2, slot])]

    def step(i, n):
        slot = lax.rem(i, OUT_SLOTS)
        act_copy(i, n).wait()

        def wait_old():
            for cp in out_copies(i - OUT_SLOTS, slot, WIDTH):
                cp.wait()

        pl.when(i >= OUT_SLOTS)(wait_old)

        def cols(kind):
            return jnp.concatenate([act[2 * i + k, kind] for k in range(n)], axis=1)

        part = slice(0, n * LANES)
        gate[slot, :, part] = dot_f32(xt[...], cols(1))
        up[slot, :, part] = dot_f32(xt[...], cols(2))
        down[slot, part, :] = lax.dot_general(cols(0), dy[...], TRANS_A, preferred_element_type=jnp.float32)
        for cp in out_copies(i, slot, n * LANES):
            cp.start()

    def body(i, carry):
        step(i, 2)
        return carry

    lax.fori_loop(0, pairs, body, 0)
    last = pairs
    if tiles % 2:
        step(pairs, 1)
        last = pairs + 1
    for i in range(last - OUT_SLOTS, last):
        for cp in out_copies(i, i % OUT_SLOTS, WIDTH if i < pairs else LANES):
            cp.wait()


def weight_grads(xt, dy_rows, act):
    tiles = act.shape[0]
    d_loc = xt.shape[0]
    f_loc = tiles * LANES
    any_spec = pl.BlockSpec(memory_space=pl.ANY)
    f32, bf16 = jnp.float32, jnp.bfloat16
    return pl.pallas_call(
        functools.partial(grads_kernel, tiles), in_specs=[any_spec] * 3, out_specs=[any_spec] * 3,
        out_shape=[jax.ShapeDtypeStruct((d_loc, f_loc), f32)] * 2 + [jax.ShapeDtypeStruct((f_loc, d_loc), f32)],
        scratch_shapes=[
            pltpu.VMEM((d_loc, 256), bf16),
            pltpu.VMEM((256, d_loc), bf16),
            pltpu.VMEM(act.shape, bf16),
            pltpu.VMEM((OUT_SLOTS, d_loc, WIDTH), f32),
            pltpu.VMEM((OUT_SLOTS, d_loc, WIDTH), f32),
            pltpu.VMEM((OUT_SLOTS, WIDTH, d_loc), f32),
            pltpu.SemaphoreType.DMA((tiles // 2 + 3,)),
            pltpu.SemaphoreType.DMA((3, OUT_SLOTS)),
        ],
        compiler_params=pltpu.CompilerParams(vmem_limit_bytes=62 * 2**20),
        cost_estimate=pl.CostEstimate(flops=6 * 256 * d_loc * f_loc, bytes_accessed=44 * 10**6, transcendentals=0),
        name="weight_grads",
    )(xt, dy_rows, act)


def solution(mesh):
    row_spec = P(None, ("dp", "tp"), None)
    in_specs = (row_spec, P("dp", "tp"), P("dp", "tp"), P("tp", "dp"), row_spec)
    out_specs = (row_spec, row_spec, P("dp", "tp"), P("dp", "tp"), P("tp", "dp"))

    def local_step(x_loc, w_gate, w_up, w_down, dy_loc):
        act, xt, dy_rows, part, y_first, dx_first = exchange(x_loc, dy_loc, w_gate, w_up, w_down)
        part = lax.all_to_all(part.reshape(16, 2, 8, -1), ("dp", "tp"), split_axis=0, concat_axis=0, tiled=True)
        part = part.reshape(8, 2, 2, 8, -1)
        out = (part[:, 0] + part[:, 1]).transpose(1, 2, 0, 3).reshape(2, 8, 4096)
        y = jnp.stack([y_first, (x_loc[1].astype(jnp.float32) + out[0]).astype(jnp.bfloat16)])
        dx = jnp.stack([dx_first, (dy_loc[1].astype(jnp.float32) + out[1]).astype(jnp.bfloat16)])
        dg, du, dd = weight_grads(xt, dy_rows, act)
        return y, dx, dg, du, dd

    return jax.shard_map(local_step, mesh=mesh, in_specs=in_specs, out_specs=out_specs, check_vma=False)
```

```python
import functools

import jax
import jax.numpy as jnp
from jax import lax
from jax.experimental import pallas as pl
from jax.experimental.pallas import tpu as pltpu
from jax.sharding import PartitionSpec as P

MESH = pl.DeviceIdType.MESH
LANES = 128
SLOTS = 8
LATE_SLOTS = 12
DEFER = 6
LEAD = 2
LAGS = (3, 3, 2, 2, 2, 1)
STARTS = tuple(sum(LAGS[:k]) for k in range(len(LAGS) + 1))
TRANS_B = (((1,), (1,)), ((), ()))
TRANS_A = (((0,), (0,)), ((), ()))


def dot_f32(lhs, rhs):
    return jnp.dot(lhs, rhs, preferred_element_type=jnp.float32)


def dot_t(lhs, rhs):
    return lax.dot_general(lhs, rhs, TRANS_B, preferred_element_type=jnp.float32)


def exchange_kernel(tiles, x_hbm, dy_hbm, wg_hbm, wu_hbm, wd_hbm,
                    act_hbm, xt_hbm, dy_rows_hbm, sum_hbm, y_hbm, dx_hbm,
                    loc, tok, rows, wg, wu, wd, part, core_in, first_out, first_in, second_out, second_in, act, acc, zin, fin, yin, xt,
                    load_sem, tok_send, tok_recv, send_sem, recv_sem, late_sem, gather_sem, lead_sem, plane_sem, store_sem, z_sem, fin_sem):
    tp = lax.axis_index("tp")
    dp = lax.axis_index("dp")
    core = lax.rem(dp, 2)
    xpos = lax.rem(lax.div(dp, 2), 2)
    ypos = lax.div(dp, 4)
    me = tp * 8 + dp

    def device(fc, fx, fy, fz):
        dc = 1 - core if fc else core
        dx = 1 - xpos if fx else xpos
        dy = 1 - ypos if fy else ypos
        return (1 - tp if fz else tp, dy * 4 + dx * 2 + dc)

    core_peer = device(1, 0, 0, 0)
    x_peer = device(0, 1, 0, 0)
    y_peer = device(0, 0, 1, 0)

    token_loads = [pltpu.make_async_copy(x_hbm, loc.at[0], load_sem.at[0]),
                   pltpu.make_async_copy(dy_hbm, loc.at[1], load_sem.at[1])]
    weight_loads = [pltpu.make_async_copy(wg_hbm, wg, load_sem.at[2]),
                    pltpu.make_async_copy(wu_hbm, wu, load_sem.at[3]),
                    pltpu.make_async_copy(wd_hbm, wd, load_sem.at[4])]
    for cp in token_loads + weight_loads:
        cp.start()

    others = [((k >> 0) & 1, (k >> 1) & 1, (k >> 2) & 1, (k >> 3) & 1) for k in range(15, 0, -1)]
    barrier = pltpu.get_barrier_semaphore()
    for flags in others:
        pl.semaphore_signal(barrier, 1, device_id=device(*flags), device_id_type=MESH)
    pl.semaphore_wait(barrier, 15)

    plane = [flags for flags in others if not flags[3]]
    for mb in range(2):
        for arr in range(2):
            if mb == 0:
                token_loads[arr].wait()
            for flags in (plane if mb else others):
                dest = device(*flags)
                pltpu.make_async_remote_copy(
                    src_ref=loc.at[arr, mb, :, pl.ds(pl.multiple_of(dest[1] * 512, 512), 512)],
                    dst_ref=tok.at[arr, mb, me],
                    send_sem=tok_send.at[arr, mb], recv_sem=tok_recv.at[arr, mb],
                    device_id=dest, device_id_type=MESH).start()
    for mb in range(2):
        for arr in range(2):
            tok[arr, mb, me] = loc[arr, mb, :, pl.ds(pl.multiple_of(dp * 512, 512), 512)]

    def plane_copy(arr):
        slab = tok.at[arr, 1, pl.ds(pl.multiple_of(8 * tp, 8), 8)]
        return pltpu.make_async_remote_copy(
            src_ref=slab, dst_ref=slab, send_sem=plane_sem.at[0, arr], recv_sem=plane_sem.at[1, arr],
            device_id=device(0, 0, 0, 1), device_id_type=MESH)

    def send_plane():
        for arr in range(2):
            got = tok.at[arr, 1, pl.ds(0, 7)]
            pltpu.make_async_copy(got, got, tok_recv.at[arr, 1]).wait()
            plane_copy(arr).start()

    def tokens_in(arr, mb):
        if mb:
            plane_copy(arr).wait()
        else:
            part15 = tok.at[arr, 0, pl.ds(0, 15)]
            pltpu.make_async_copy(part15, part15, tok_recv.at[arr, 0]).wait()
        for pair in range(8):
            lo = tok[arr, mb, pair].astype(jnp.float32)
            hi = tok[arr, mb, 8 + pair].astype(jnp.float32)
            rows[arr, pl.ds(mb * 128 + 16 * pair, 16), :] = jnp.concatenate([lo, hi], axis=0).astype(jnp.bfloat16)

    acc[...] = jnp.zeros_like(acc)

    n_iter = tiles

    def unit(i, h):
        u = 2 * i + h
        mb = lax.div(u, tiles)
        return u, mb, u - tiles * mb

    keep_core = pl.multiple_of(core * 64, 64)
    send_core = pl.multiple_of((1 - core) * 64, 64)
    pos1 = (xpos, ypos)
    pos2 = (ypos, xpos)
    peer1 = (x_peer, y_peer)
    peer2 = (y_peer, x_peer)

    def off(v):
        return pl.multiple_of(v, 16)

    def copies(stage, i, h):
        u, mb, t = unit(i, h)
        slot = lax.rem(i, SLOTS)
        base = mb * 128 + core * 64
        if stage == 0:
            src, dst, dev = part.at[slot, h, :, pl.ds(send_core, 64), :], core_in.at[u], core_peer
        elif stage == 1:
            src, dst, dev = first_out.at[slot, h], first_in.at[u], peer1[h]
        elif stage == 2:
            src, dst, dev = second_out.at[slot, h], second_in.at[u], peer2[h]
        elif stage == 3:
            src = dst = act.at[t, :, pl.ds(off(base + 32 * pos1[h] + 16 * pos2[h]), 16), :]
            dev = peer2[h]
        elif stage == 4:
            src = dst = act.at[t, :, pl.ds(off(base + 32 * pos1[h]), 32), :]
            dev = peer1[h]
        else:
            src = dst = act.at[t, :, pl.ds(off(base), 64), :]
            dev = core_peer
        return pltpu.make_async_remote_copy(
            src_ref=src, dst_ref=dst, send_sem=send_sem.at[stage, lax.rem(i, 4)] if stage < 3 else gather_sem.at[0],
            recv_sem=arrival(stage, i), device_id=dev, device_id_type=MESH)

    def arrival(stage, i):
        if stage < 3:
            return recv_sem.at[stage, lax.rem(i, SLOTS)]
        return late_sem.at[stage - 3, lax.rem(i, LATE_SLOTS)]

    def start_pair(stage, i):
        for h in range(2):
            copies(stage, i, h).start()

    def wait_pair(stage, i):
        if stage < 3:
            into = (core_in, first_in, second_in)[stage].at[pl.ds(2 * i, 2)]
            pltpu.make_async_copy(into, into, send_sem.at[stage, lax.rem(i, 4)]).wait()
        else:
            into = act.at[0, :, pl.ds(0, 32 << (stage - 3)), :]
        pltpu.make_async_copy(into, into, arrival(stage, i)).wait()

    def gate_up_partials(i, h):
        u, mb, t = unit(i, h)
        slot = lax.rem(i, SLOTS)
        cols = pl.ds(pl.multiple_of(t * LANES, LANES), LANES)
        r = pl.ds(pl.multiple_of(mb * 128, 128), 128)
        pair = jnp.concatenate([wg[:, cols], wu[:, cols]], axis=1)
        ab = dot_f32(rows[0, r, :], pair)
        part[slot, h, 0] = ab[:, :LANES]
        part[slot, h, 1] = ab[:, LANES:]

    def down_partials(i, h):
        u, mb, t = unit(i, h)
        cols = pl.ds(pl.multiple_of(t * LANES, LANES), LANES)
        r = pl.ds(pl.multiple_of(mb * 128, 128), 128)
        part[lax.rem(i, SLOTS), h, 2] = dot_t(rows[1, r, :], wd[cols, :])

    def stage_partials(i):
        for h in range(2):
            gate_up_partials(i, h)
            down_partials(i, h)
        start_pair(0, i)

    def lead_in():
        kinds = (pl.ds(0, 2), pl.ds(2, 1))

        def to_core(i, k):
            for h in range(2):
                pltpu.make_async_remote_copy(
                    src_ref=part.at[i, h, kinds[k], pl.ds(send_core, 64), :], dst_ref=core_in.at[2 * i + h, kinds[k]],
                    send_sem=lead_sem.at[0, k, i], recv_sem=lead_sem.at[1, k, i], device_id=core_peer, device_id_type=MESH).start()

        def to_first(i, k):
            both = core_in.at[pl.ds(2 * i, 2), kinds[k]]
            for way in range(2):
                pltpu.make_async_copy(both, both, lead_sem.at[way, k, i]).wait()
            for h in range(2):
                o = (1 - pos1[h]) * 32
                first_out[i, h, kinds[k]] = (part[i, h, kinds[k], pl.ds(off(core * 64 + o), 32), :]
                                             + core_in[2 * i + h, kinds[k], pl.ds(off(o), 32), :])
                pltpu.make_async_remote_copy(
                    src_ref=first_out.at[i, h, kinds[k]], dst_ref=first_in.at[2 * i + h, kinds[k]], send_sem=send_sem.at[1, i],
                    recv_sem=arrival(1, i), device_id=peer1[h], device_id_type=MESH).start()

        tokens_in(0, 0)
        for cp in weight_loads[:2]:
            cp.wait()
        for i in range(LEAD):
            for h in range(2):
                gate_up_partials(i, h)
            to_core(i, 0)
        for i in range(LEAD):
            to_first(i, 0)
        tokens_in(1, 0)
        weight_loads[2].wait()
        for i in range(LEAD):
            for h in range(2):
                down_partials(i, h)
            to_core(i, 1)
        for i in range(LEAD, STARTS[1]):
            stage_partials(i)
        for i in range(LEAD):
            to_first(i, 1)

    def stage_first(i):
        slot = lax.rem(i, SLOTS)
        wait_pair(0, i)
        for h in range(2):
            u, _, _ = unit(i, h)
            o = (1 - pos1[h]) * 32
            first_out[slot, h] = (part[slot, h, :, pl.ds(off(core * 64 + o), 32), :] + core_in[u, :, pl.ds(off(o), 32), :])
            copies(1, i, h).start()

    def stage_second(i):
        slot = lax.rem(i, SLOTS)
        wait_pair(1, i)
        for h in range(2):
            u, _, _ = unit(i, h)
            o2 = (1 - pos2[h]) * 16
            o = pos1[h] * 32 + o2
            second_out[slot, h] = (part[slot, h, :, pl.ds(off(core * 64 + o), 16), :] + core_in[u, :, pl.ds(off(o), 16), :]
                                   + first_in[u, :, pl.ds(off(o2), 16), :])
            copies(2, i, h).start()

    def stage_act(i):
        slot = lax.rem(i, SLOTS)
        wait_pair(2, i)
        for h in range(2):
            u, mb, t = unit(i, h)
            o2 = pos2[h] * 16
            o = pos1[h] * 32 + o2
            tot = (part[slot, h, :, pl.ds(off(core * 64 + o), 16), :] + core_in[u, :, pl.ds(off(o), 16), :]
                   + first_in[u, :, pl.ds(off(o2), 16), :] + second_in[u])
            a, b, g = tot[0], tot[1], tot[2]
            s = jax.nn.sigmoid(a)
            silu = a * s
            r = pl.ds(off(mb * 128 + core * 64 + o), 16)
            act[t, 0, r, :] = (silu * b).astype(jnp.bfloat16)
            act[t, 1, r, :] = (g * b * s * (1.0 + a * (1.0 - s))).astype(jnp.bfloat16)
            act[t, 2, r, :] = (g * silu).astype(jnp.bfloat16)
            copies(3, i, h).start()

    def stage_forward(stage, i):
        wait_pair(stage - 1, i)
        start_pair(stage, i)

    def add_to(arr, mb, term):
        blocks = pl.ds(mb * 8, 8)
        acc[arr, blocks] += term.reshape(8, 2, 8, term.shape[-1])

    def stage_outputs(i):
        wait_pair(5, i)
        for h in range(2):
            u, mb, t = unit(i, h)
            cols = pl.ds(pl.multiple_of(t * LANES, LANES), LANES)
            r = pl.ds(pl.multiple_of(mb * 128, 128), 128)
            pltpu.make_async_copy(act.at[t, :, r, :], act_hbm.at[t, :, r, :], store_sem.at[0]).start()
            add_to(0, mb, dot_f32(act[t, 0, r, :], wd[cols, :]))
            grads = jnp.concatenate([act[t, 1, r, :], act[t, 2, r, :]], axis=1)
            pair = jnp.concatenate([wg[:, cols], wu[:, cols]], axis=1)
            add_to(1, mb, dot_t(grads, pair))

    z_copy = pltpu.make_async_remote_copy(
        src_ref=acc.at[:, pl.ds(0, 8), 1 - tp], dst_ref=zin, send_sem=z_sem.at[0], recv_sem=z_sem.at[1],
        device_id=device(0, 0, 0, 1), device_id_type=MESH)
    my_cols = pl.ds(pl.multiple_of(dp * 512, 512), 512)

    def finish_first():
        z_copy.wait()
        for arr in range(2):
            for blk in range(8):
                total = acc[arr, blk, tp] + zin[arr, blk]
                fin[blk, arr] = (tok[arr, 0, 8 * tp + blk].astype(jnp.float32) + total).astype(jnp.bfloat16)

    def send_first():
        for flags in plane:
            dest = device(*flags)
            pltpu.make_async_remote_copy(
                src_ref=fin.at[dest[1]], dst_ref=yin.at[:, :, my_cols], send_sem=fin_sem.at[0], recv_sem=fin_sem.at[1],
                device_id=dest, device_id_type=MESH).start()
        yin[:, :, my_cols] = fin[dp]

    firsts = [pltpu.make_async_copy(yin.at[k], ref, store_sem.at[4 + k]) for k, ref in enumerate((y_hbm, dx_hbm))]

    def store_first():
        blocks = fin.at[pl.ds(0, 7)]
        for k in range(2):
            pltpu.make_async_copy(blocks, blocks, fin_sem.at[k]).wait()
        for cp in firsts:
            cp.start()

    z_start = (tiles - 1) // 2 + STARTS[6] + DEFER + 1

    def forwarded(j):
        ready = jnp.maximum(j - STARTS[4] + 1, 0)
        late = jnp.maximum(j - STARTS[4] + 1 - DEFER, 0) + jnp.maximum(j - n_iter - STARTS[1] + 2, 0)
        return jnp.minimum(n_iter, jnp.minimum(ready, late))

    def run_late(j, fn):
        def step(i, carry):
            fn(i)
            return carry

        lax.fori_loop(forwarded(j - 1), forwarded(j), step, 0)

    row_stores = [pltpu.make_async_copy(xt, xt_hbm, store_sem.at[1]), pltpu.make_async_copy(rows.at[1], dy_rows_hbm, store_sem.at[6])]

    def body(j, carry):
        pl.when(j == STARTS[1] + 4)(send_plane)
        pl.when(j == z_start)(z_copy.start)
        pl.when(j == n_iter + STARTS[3] - 2)(finish_first)

        def run(stage, fn):
            i = j - STARTS[stage]
            pl.when(jnp.logical_and(i >= (LEAD if stage == 1 else 0), i < n_iter))(functools.partial(fn, i))

        run(1, stage_first)
        run(2, stage_second)
        run(3, stage_act)
        run_late(j, functools.partial(stage_forward, 4))
        pl.when(j == n_iter + STARTS[4] - 1)(send_first)
        run_late(j - LAGS[4], functools.partial(stage_forward, 5))

        @pl.when(j == tiles // 2 - 2)
        def _():
            tokens_in(0, 1)
            tokens_in(1, 1)
            xt[...] = rows[0].T
            for cp in row_stores:
                cp.start()

        run(0, stage_partials)
        run_late(j - LAGS[4] - LAGS[5], stage_outputs)
        return carry

    lead_in()
    lax.fori_loop(STARTS[1], n_iter + STARTS[6], body, 0)

    sums = [pltpu.make_async_copy(acc.at[arr, pl.ds(8, 8)], sum_hbm.at[:, :, arr], store_sem.at[2 + arr]) for arr in range(2)]
    for cp in sums:
        cp.start()
    store_first()
    for mb in range(2):
        for arr in range(2):
            sent = tok.at[arr, mb, pl.ds(0, 7 if mb else 15)]
            pltpu.make_async_copy(sent, sent, tok_send.at[arr, mb]).wait()
    for cp in row_stores:
        cp.wait()
    pltpu.make_async_copy(act, act_hbm, store_sem.at[0]).wait()
    sent = act.at[:, :, pl.ds(0, 224), :]
    pltpu.make_async_copy(sent, sent, gather_sem.at[0]).wait()
    for cp in sums + firsts:
        cp.wait()


def exchange(x_loc, dy_loc, w_gate, w_up, w_down):
    d_loc, f_loc = w_gate.shape
    tiles = f_loc // LANES
    any_spec = pl.BlockSpec(memory_space=pl.ANY)
    f32, bf16 = jnp.float32, jnp.bfloat16
    return pl.pallas_call(
        functools.partial(exchange_kernel, tiles),
        out_shape=(jax.ShapeDtypeStruct((tiles, 3, 256, LANES), bf16),
                   jax.ShapeDtypeStruct((d_loc, 256), bf16),
                   jax.ShapeDtypeStruct((256, d_loc), bf16),
                   jax.ShapeDtypeStruct((8, 2, 2, 8, d_loc), f32),
                   *[jax.ShapeDtypeStruct((8, 4096), bf16)] * 2),
        in_specs=[any_spec] * 5,
        out_specs=(any_spec,) * 6,
        scratch_shapes=[
            pltpu.VMEM((2, 2, 8, 4096), bf16),
            pltpu.VMEM((2, 2, 16, 8, d_loc), bf16),
            pltpu.VMEM((2, 256, d_loc), bf16),
            pltpu.VMEM((d_loc, f_loc), bf16),
            pltpu.VMEM((d_loc, f_loc), bf16),
            pltpu.VMEM((f_loc, d_loc), bf16),
            pltpu.VMEM((SLOTS, 2, 3, 128, LANES), f32),
            pltpu.VMEM((2 * tiles, 3, 64, LANES), f32),
            pltpu.VMEM((SLOTS, 2, 3, 32, LANES), f32),
            pltpu.VMEM((2 * tiles, 3, 32, LANES), f32),
            pltpu.VMEM((SLOTS, 2, 3, 16, LANES), f32),
            pltpu.VMEM((2 * tiles, 3, 16, LANES), f32),
            pltpu.VMEM((tiles, 3, 256, LANES), bf16),
            pltpu.VMEM((2, 16, 2, 8, d_loc), f32),
            pltpu.VMEM((2, 8, 8, d_loc), f32),
            pltpu.VMEM((8, 2, 8, d_loc), bf16),
            pltpu.VMEM((2, 8, 4096), bf16),
            pltpu.VMEM((d_loc, 256), bf16),
            pltpu.SemaphoreType.DMA((5,)),
            pltpu.SemaphoreType.DMA((2, 2)),
            pltpu.SemaphoreType.DMA((2, 2)),
            pltpu.SemaphoreType.DMA((3, 4)),
            pltpu.SemaphoreType.DMA((3, SLOTS)),
            pltpu.SemaphoreType.DMA((3, LATE_SLOTS)),
            pltpu.SemaphoreType.DMA((1,)),
            pltpu.SemaphoreType.DMA((2, 2, LEAD)),
            pltpu.SemaphoreType.DMA((2, 2)),
            pltpu.SemaphoreType.DMA((7,)),
            pltpu.SemaphoreType.DMA((2,)),
            pltpu.SemaphoreType.DMA((2,)),
        ],
        compiler_params=pltpu.CompilerParams(collective_id=0, has_side_effects=True, vmem_limit_bytes=60 * 2**20),
        cost_estimate=pl.CostEstimate(flops=9 * 10**9, bytes_accessed=28 * 10**6, transcendentals=0),
        name="exchange",
    )(x_loc, dy_loc, w_gate, w_up, w_down)


OUT_SLOTS = 4
WIDTH = 2 * LANES


def grads_kernel(tiles, xt_hbm, dy_hbm, act_hbm, dg_hbm, du_hbm, dd_hbm, xt, dy, act, gate, up, down, load_sem, out_sem):
    pairs = tiles // 2
    row_loads = [pltpu.make_async_copy(xt_hbm, xt, load_sem.at[pairs + 1]), pltpu.make_async_copy(dy_hbm, dy, load_sem.at[pairs + 2])]
    for cp in row_loads:
        cp.start()

    def act_copy(i, n):
        span = pl.ds(2 * i, n)
        return pltpu.make_async_copy(act_hbm.at[span], act.at[span], load_sem.at[i])

    for i in range(pairs):
        act_copy(i, 2).start()
    if tiles % 2:
        act_copy(pairs, 1).start()
    for cp in row_loads:
        cp.wait()

    def out_copies(i, slot, width):
        cols = pl.ds(pl.multiple_of(i * WIDTH, WIDTH), width)
        part = pl.ds(0, width)
        return [pltpu.make_async_copy(gate.at[slot, :, part], dg_hbm.at[:, cols], out_sem.at[0, slot]),
                pltpu.make_async_copy(up.at[slot, :, part], du_hbm.at[:, cols], out_sem.at[1, slot]),
                pltpu.make_async_copy(down.at[slot, part, :], dd_hbm.at[cols, :], out_sem.at[2, slot])]

    def step(i, n):
        slot = lax.rem(i, OUT_SLOTS)
        act_copy(i, n).wait()

        def wait_old():
            for cp in out_copies(i - OUT_SLOTS, slot, WIDTH):
                cp.wait()

        pl.when(i >= OUT_SLOTS)(wait_old)

        def cols(kind):
            return jnp.concatenate([act[2 * i + k, kind] for k in range(n)], axis=1)

        part = slice(0, n * LANES)
        gate[slot, :, part] = dot_f32(xt[...], cols(1))
        up[slot, :, part] = dot_f32(xt[...], cols(2))
        down[slot, part, :] = lax.dot_general(cols(0), dy[...], TRANS_A, preferred_element_type=jnp.float32)
        for cp in out_copies(i, slot, n * LANES):
            cp.start()

    def body(i, carry):
        step(i, 2)
        return carry

    lax.fori_loop(0, pairs, body, 0)
    last = pairs
    if tiles % 2:
        step(pairs, 1)
        last = pairs + 1
    for i in range(last - OUT_SLOTS, last):
        for cp in out_copies(i, i % OUT_SLOTS, WIDTH if i < pairs else LANES):
            cp.wait()


def weight_grads(xt, dy_rows, act):
    tiles = act.shape[0]
    d_loc = xt.shape[0]
    f_loc = tiles * LANES
    any_spec = pl.BlockSpec(memory_space=pl.ANY)
    f32, bf16 = jnp.float32, jnp.bfloat16
    return pl.pallas_call(
        functools.partial(grads_kernel, tiles), in_specs=[any_spec] * 3, out_specs=[any_spec] * 3,
        out_shape=[jax.ShapeDtypeStruct((d_loc, f_loc), f32)] * 2 + [jax.ShapeDtypeStruct((f_loc, d_loc), f32)],
        scratch_shapes=[
            pltpu.VMEM((d_loc, 256), bf16),
            pltpu.VMEM((256, d_loc), bf16),
            pltpu.VMEM(act.shape, bf16),
            pltpu.VMEM((OUT_SLOTS, d_loc, WIDTH), f32),
            pltpu.VMEM((OUT_SLOTS, d_loc, WIDTH), f32),
            pltpu.VMEM((OUT_SLOTS, WIDTH, d_loc), f32),
            pltpu.SemaphoreType.DMA((tiles // 2 + 3,)),
            pltpu.SemaphoreType.DMA((3, OUT_SLOTS)),
        ],
        compiler_params=pltpu.CompilerParams(vmem_limit_bytes=62 * 2**20),
        cost_estimate=pl.CostEstimate(flops=6 * 256 * d_loc * f_loc, bytes_accessed=44 * 10**6, transcendentals=0),
        name="weight_grads",
    )(xt, dy_rows, act)


def solution(mesh):
    row_spec = P(None, ("dp", "tp"), None)
    in_specs = (row_spec, P("dp", "tp"), P("dp", "tp"), P("tp", "dp"), row_spec)
    out_specs = (row_spec, row_spec, P("dp", "tp"), P("dp", "tp"), P("tp", "dp"))

    def local_step(x_loc, w_gate, w_up, w_down, dy_loc):
        act, xt, dy_rows, part, y_first, dx_first = exchange(x_loc, dy_loc, w_gate, w_up, w_down)
        part = lax.all_to_all(part.reshape(16, 2, 8, -1), ("dp", "tp"), split_axis=0, concat_axis=0, tiled=True)
        part = part.reshape(8, 2, 2, 8, -1)
        out = (part[:, 0] + part[:, 1]).transpose(1, 2, 0, 3).reshape(2, 8, 4096)
        y = jnp.stack([y_first, (x_loc[1].astype(jnp.float32) + out[0]).astype(jnp.bfloat16)])
        dx = jnp.stack([dx_first, (dy_loc[1].astype(jnp.float32) + out[1]).astype(jnp.bfloat16)])
        dg, du, dd = weight_grads(xt, dy_rows, act)
        return y, dx, dg, du, dd

    return jax.shard_map(local_step, mesh=mesh, in_specs=in_specs, out_specs=out_specs, check_vma=False)
```

```python
import functools

import jax
import jax.numpy as jnp
from jax import lax
from jax.experimental import pallas as pl
from jax.experimental.pallas import tpu as pltpu
from jax.sharding import PartitionSpec as P

MESH = pl.DeviceIdType.MESH
LANES = 128
SLOTS = 8
LATE_SLOTS = 12
DEFER = 6
LEAD = 2
LAGS = (3, 3, 2, 2, 2, 1)
STARTS = tuple(sum(LAGS[:k]) for k in range(len(LAGS) + 1))
TRANS_B = (((1,), (1,)), ((), ()))
TRANS_A = (((0,), (0,)), ((), ()))


def dot_f32(lhs, rhs):
    return jnp.dot(lhs, rhs, preferred_element_type=jnp.float32)


def dot_t(lhs, rhs):
    return lax.dot_general(lhs, rhs, TRANS_B, preferred_element_type=jnp.float32)


def exchange_kernel(tiles, x_hbm, dy_hbm, wg_hbm, wu_hbm, wd_hbm,
                    act_hbm, xt_hbm, dy_rows_hbm, sum_hbm, y_hbm, dx_hbm,
                    loc, tok, rows, wg, wu, wd, part, core_in, first_out, first_in, second_out, second_in, act, acc, zin, fin, yin, xt,
                    load_sem, tok_send, tok_recv, send_sem, recv_sem, late_sem, gather_sem, lead_sem, plane_sem, store_sem, z_sem, fin_sem):
    tp = lax.axis_index("tp")
    dp = lax.axis_index("dp")
    core = lax.rem(dp, 2)
    xpos = lax.rem(lax.div(dp, 2), 2)
    ypos = lax.div(dp, 4)
    me = tp * 8 + dp

    def device(fc, fx, fy, fz):
        dc = 1 - core if fc else core
        dx = 1 - xpos if fx else xpos
        dy = 1 - ypos if fy else ypos
        return (1 - tp if fz else tp, dy * 4 + dx * 2 + dc)

    core_peer = device(1, 0, 0, 0)
    x_peer = device(0, 1, 0, 0)
    y_peer = device(0, 0, 1, 0)

    token_loads = [pltpu.make_async_copy(x_hbm, loc.at[0], load_sem.at[0]),
                   pltpu.make_async_copy(dy_hbm, loc.at[1], load_sem.at[1])]
    weight_loads = [pltpu.make_async_copy(wg_hbm, wg, load_sem.at[2]),
                    pltpu.make_async_copy(wu_hbm, wu, load_sem.at[3]),
                    pltpu.make_async_copy(wd_hbm, wd, load_sem.at[4])]
    for cp in token_loads + weight_loads:
        cp.start()

    others = [((k >> 0) & 1, (k >> 1) & 1, (k >> 2) & 1, (k >> 3) & 1) for k in range(15, 0, -1)]
    barrier = pltpu.get_barrier_semaphore()
    for flags in others:
        pl.semaphore_signal(barrier, 1, device_id=device(*flags), device_id_type=MESH)
    pl.semaphore_wait(barrier, 15)

    plane = [flags for flags in others if not flags[3]]
    for mb in range(2):
        for arr in range(2):
            if mb == 0:
                token_loads[arr].wait()
            for flags in (plane if mb else others):
                dest = device(*flags)
                pltpu.make_async_remote_copy(
                    src_ref=loc.at[arr, mb, :, pl.ds(pl.multiple_of(dest[1] * 512, 512), 512)],
                    dst_ref=tok.at[arr, mb, me],
                    send_sem=tok_send.at[arr, mb], recv_sem=tok_recv.at[arr, mb],
                    device_id=dest, device_id_type=MESH).start()
    for mb in range(2):
        for arr in range(2):
            tok[arr, mb, me] = loc[arr, mb, :, pl.ds(pl.multiple_of(dp * 512, 512), 512)]

    def plane_copy(arr):
        slab = tok.at[arr, 1, pl.ds(pl.multiple_of(8 * tp, 8), 8)]
        return pltpu.make_async_remote_copy(
            src_ref=slab, dst_ref=slab, send_sem=plane_sem.at[0, arr], recv_sem=plane_sem.at[1, arr],
            device_id=device(0, 0, 0, 1), device_id_type=MESH)

    def send_plane():
        for arr in range(2):
            got = tok.at[arr, 1, pl.ds(0, 7)]
            pltpu.make_async_copy(got, got, tok_recv.at[arr, 1]).wait()
            plane_copy(arr).start()

    def tokens_in(arr, mb):
        if mb:
            plane_copy(arr).wait()
        else:
            part15 = tok.at[arr, 0, pl.ds(0, 15)]
            pltpu.make_async_copy(part15, part15, tok_recv.at[arr, 0]).wait()
        for pair in range(8):
            lo = tok[arr, mb, pair].astype(jnp.float32)
            hi = tok[arr, mb, 8 + pair].astype(jnp.float32)
            rows[arr, pl.ds(mb * 128 + 16 * pair, 16), :] = jnp.concatenate([lo, hi], axis=0).astype(jnp.bfloat16)

    acc[...] = jnp.zeros_like(acc)

    n_iter = tiles

    def unit(i, h):
        u = 2 * i + h
        mb = lax.div(u, tiles)
        return u, mb, u - tiles * mb

    keep_core = pl.multiple_of(core * 64, 64)
    send_core = pl.multiple_of((1 - core) * 64, 64)
    pos1 = (xpos, ypos)
    pos2 = (ypos, xpos)
    peer1 = (x_peer, y_peer)
    peer2 = (y_peer, x_peer)

    def off(v):
        return pl.multiple_of(v, 16)

    def copies(stage, i, h):
        u, mb, t = unit(i, h)
        slot = lax.rem(i, SLOTS)
        base = mb * 128 + core * 64
        if stage == 0:
            src, dst, dev = part.at[slot, h, :, pl.ds(send_core, 64), :], core_in.at[u], core_peer
        elif stage == 1:
            src, dst, dev = first_out.at[slot, h], first_in.at[u], peer1[h]
        elif stage == 2:
            src, dst, dev = second_out.at[slot, h], second_in.at[u], peer2[h]
        elif stage == 3:
            src = dst = act.at[t, :, pl.ds(off(base + 32 * pos1[h] + 16 * pos2[h]), 16), :]
            dev = peer2[h]
        elif stage == 4:
            src = dst = act.at[t, :, pl.ds(off(base + 32 * pos1[h]), 32), :]
            dev = peer1[h]
        else:
            src = dst = act.at[t, :, pl.ds(off(base), 64), :]
            dev = core_peer
        return pltpu.make_async_remote_copy(
            src_ref=src, dst_ref=dst, send_sem=send_sem.at[stage, lax.rem(i, 4)] if stage < 3 else gather_sem.at[0],
            recv_sem=arrival(stage, i), device_id=dev, device_id_type=MESH)

    def arrival(stage, i):
        if stage < 3:
            return recv_sem.at[stage, lax.rem(i, SLOTS)]
        return late_sem.at[stage - 3, lax.rem(i, LATE_SLOTS)]

    def start_pair(stage, i):
        for h in range(2):
            copies(stage, i, h).start()

    def wait_pair(stage, i):
        if stage < 3:
            into = (core_in, first_in, second_in)[stage].at[pl.ds(2 * i, 2)]
            pltpu.make_async_copy(into, into, send_sem.at[stage, lax.rem(i, 4)]).wait()
        else:
            into = act.at[0, :, pl.ds(0, 32 << (stage - 3)), :]
        pltpu.make_async_copy(into, into, arrival(stage, i)).wait()

    def gate_up_partials(i, h):
        u, mb, t = unit(i, h)
        slot = lax.rem(i, SLOTS)
        cols = pl.ds(pl.multiple_of(t * LANES, LANES), LANES)
        r = pl.ds(pl.multiple_of(mb * 128, 128), 128)
        pair = jnp.concatenate([wg[:, cols], wu[:, cols]], axis=1)
        ab = dot_f32(rows[0, r, :], pair)
        part[slot, h, 0] = ab[:, :LANES]
        part[slot, h, 1] = ab[:, LANES:]

    def down_partials(i, h):
        u, mb, t = unit(i, h)
        cols = pl.ds(pl.multiple_of(t * LANES, LANES), LANES)
        r = pl.ds(pl.multiple_of(mb * 128, 128), 128)
        part[lax.rem(i, SLOTS), h, 2] = dot_t(rows[1, r, :], wd[cols, :])

    def stage_partials(i):
        for h in range(2):
            gate_up_partials(i, h)
            down_partials(i, h)
        start_pair(0, i)

    def lead_in():
        kinds = (pl.ds(0, 2), pl.ds(2, 1))

        def to_core(i, k):
            for h in range(2):
                pltpu.make_async_remote_copy(
                    src_ref=part.at[i, h, kinds[k], pl.ds(send_core, 64), :], dst_ref=core_in.at[2 * i + h, kinds[k]],
                    send_sem=lead_sem.at[0, k, i], recv_sem=lead_sem.at[1, k, i], device_id=core_peer, device_id_type=MESH).start()

        def to_first(i, k):
            both = core_in.at[pl.ds(2 * i, 2), kinds[k]]
            for way in range(2):
                pltpu.make_async_copy(both, both, lead_sem.at[way, k, i]).wait()
            for h in range(2):
                o = (1 - pos1[h]) * 32
                first_out[i, h, kinds[k]] = (part[i, h, kinds[k], pl.ds(off(core * 64 + o), 32), :]
                                             + core_in[2 * i + h, kinds[k], pl.ds(off(o), 32), :])
                pltpu.make_async_remote_copy(
                    src_ref=first_out.at[i, h, kinds[k]], dst_ref=first_in.at[2 * i + h, kinds[k]], send_sem=send_sem.at[1, i],
                    recv_sem=arrival(1, i), device_id=peer1[h], device_id_type=MESH).start()

        tokens_in(0, 0)
        for cp in weight_loads[:2]:
            cp.wait()
        for i in range(LEAD):
            for h in range(2):
                gate_up_partials(i, h)
            to_core(i, 0)
        for i in range(LEAD):
            to_first(i, 0)
        tokens_in(1, 0)
        weight_loads[2].wait()
        for i in range(LEAD):
            for h in range(2):
                down_partials(i, h)
            to_core(i, 1)
        for i in range(LEAD, STARTS[1]):
            stage_partials(i)
        for i in range(LEAD):
            to_first(i, 1)

    def stage_first(i):
        slot = lax.rem(i, SLOTS)
        wait_pair(0, i)
        for h in range(2):
            u, _, _ = unit(i, h)
            o = (1 - pos1[h]) * 32
            first_out[slot, h] = (part[slot, h, :, pl.ds(off(core * 64 + o), 32), :] + core_in[u, :, pl.ds(off(o), 32), :])
            copies(1, i, h).start()

    def stage_second(i):
        slot = lax.rem(i, SLOTS)
        wait_pair(1, i)
        for h in range(2):
            u, _, _ = unit(i, h)
            o2 = (1 - pos2[h]) * 16
            o = pos1[h] * 32 + o2
            second_out[slot, h] = (part[slot, h, :, pl.ds(off(core * 64 + o), 16), :] + core_in[u, :, pl.ds(off(o), 16), :]
                                   + first_in[u, :, pl.ds(off(o2), 16), :])
            copies(2, i, h).start()

    def stage_act(i):
        slot = lax.rem(i, SLOTS)
        wait_pair(2, i)
        for h in range(2):
            u, mb, t = unit(i, h)
            o2 = pos2[h] * 16
            o = pos1[h] * 32 + o2
            tot = (part[slot, h, :, pl.ds(off(core * 64 + o), 16), :] + core_in[u, :, pl.ds(off(o), 16), :]
                   + first_in[u, :, pl.ds(off(o2), 16), :] + second_in[u])
            a, b, g = tot[0], tot[1], tot[2]
            s = jax.nn.sigmoid(a)
            silu = a * s
            r = pl.ds(off(mb * 128 + core * 64 + o), 16)
            act[t, 0, r, :] = (silu * b).astype(jnp.bfloat16)
            act[t, 1, r, :] = (g * b * s * (1.0 + a * (1.0 - s))).astype(jnp.bfloat16)
            act[t, 2, r, :] = (g * silu).astype(jnp.bfloat16)
            copies(3, i, h).start()

    def stage_forward(stage, i):
        wait_pair(stage - 1, i)
        start_pair(stage, i)

    def add_to(arr, mb, term):
        blocks = pl.ds(mb * 8, 8)
        acc[arr, blocks] += term.reshape(8, 2, 8, term.shape[-1])

    def stage_outputs(i):
        wait_pair(5, i)
        for h in range(2):
            u, mb, t = unit(i, h)
            cols = pl.ds(pl.multiple_of(t * LANES, LANES), LANES)
            r = pl.ds(pl.multiple_of(mb * 128, 128), 128)
            pltpu.make_async_copy(act.at[t, :, r, :], act_hbm.at[t, :, r, :], store_sem.at[0]).start()
            add_to(0, mb, dot_f32(act[t, 0, r, :], wd[cols, :]))
            grads = jnp.concatenate([act[t, 1, r, :], act[t, 2, r, :]], axis=1)
            pair = jnp.concatenate([wg[:, cols], wu[:, cols]], axis=1)
            add_to(1, mb, dot_t(grads, pair))

    z_copy = pltpu.make_async_remote_copy(
        src_ref=acc.at[:, pl.ds(0, 8), 1 - tp], dst_ref=zin, send_sem=z_sem.at[0], recv_sem=z_sem.at[1],
        device_id=device(0, 0, 0, 1), device_id_type=MESH)
    my_cols = pl.ds(pl.multiple_of(dp * 512, 512), 512)

    def finish_first():
        z_copy.wait()
        for arr in range(2):
            for blk in range(8):
                total = acc[arr, blk, tp] + zin[arr, blk]
                fin[blk, arr] = (tok[arr, 0, 8 * tp + blk].astype(jnp.float32) + total).astype(jnp.bfloat16)

    def send_first():
        for flags in plane:
            dest = device(*flags)
            pltpu.make_async_remote_copy(
                src_ref=fin.at[dest[1]], dst_ref=yin.at[:, :, my_cols], send_sem=fin_sem.at[0], recv_sem=fin_sem.at[1],
                device_id=dest, device_id_type=MESH).start()
        yin[:, :, my_cols] = fin[dp]

    firsts = [pltpu.make_async_copy(yin.at[k], ref, store_sem.at[4 + k]) for k, ref in enumerate((y_hbm, dx_hbm))]

    def store_first():
        blocks = fin.at[pl.ds(0, 7)]
        for k in range(2):
            pltpu.make_async_copy(blocks, blocks, fin_sem.at[k]).wait()
        for cp in firsts:
            cp.start()

    z_start = (tiles - 1) // 2 + STARTS[6] + DEFER + 1

    def forwarded(j):
        ready = jnp.maximum(j - STARTS[4] + 1, 0)
        late = jnp.maximum(j - STARTS[4] + 1 - DEFER, 0) + jnp.maximum(j - n_iter - STARTS[1] + 2, 0)
        return jnp.minimum(n_iter, jnp.minimum(ready, late))

    def run_late(j, fn):
        def step(i, carry):
            fn(i)
            return carry

        lax.fori_loop(forwarded(j - 1), forwarded(j), step, 0)

    row_stores = [pltpu.make_async_copy(xt, xt_hbm, store_sem.at[1]), pltpu.make_async_copy(rows.at[1], dy_rows_hbm, store_sem.at[6])]

    def body(j, carry):
        pl.when(j == STARTS[1] + 4)(send_plane)
        pl.when(j == z_start)(z_copy.start)
        pl.when(j == n_iter + STARTS[3] - 2)(finish_first)

        def run(stage, fn):
            i = j - STARTS[stage]
            pl.when(jnp.logical_and(i >= (LEAD if stage == 1 else 0), i < n_iter))(functools.partial(fn, i))

        run(1, stage_first)
        run(2, stage_second)
        run(3, stage_act)
        run_late(j, functools.partial(stage_forward, 4))
        pl.when(j == n_iter + STARTS[4] - 1)(send_first)
        run_late(j - LAGS[4], functools.partial(stage_forward, 5))

        @pl.when(j == tiles // 2 - 2)
        def _():
            tokens_in(0, 1)
            tokens_in(1, 1)
            xt[...] = rows[0].T
            for cp in row_stores:
                cp.start()

        run(0, stage_partials)
        run_late(j - LAGS[4] - LAGS[5], stage_outputs)
        return carry

    lead_in()
    lax.fori_loop(STARTS[1], n_iter + STARTS[6], body, 0)

    sums = [pltpu.make_async_copy(acc.at[arr, pl.ds(8, 8)], sum_hbm.at[:, :, arr], store_sem.at[2 + arr]) for arr in range(2)]
    for cp in sums:
        cp.start()
    store_first()
    for mb in range(2):
        for arr in range(2):
            sent = tok.at[arr, mb, pl.ds(0, 7 if mb else 15)]
            pltpu.make_async_copy(sent, sent, tok_send.at[arr, mb]).wait()
    for cp in row_stores:
        cp.wait()
    pltpu.make_async_copy(act, act_hbm, store_sem.at[0]).wait()
    sent = act.at[:, :, pl.ds(0, 224), :]
    pltpu.make_async_copy(sent, sent, gather_sem.at[0]).wait()
    for cp in sums + firsts:
        cp.wait()


def exchange(x_loc, dy_loc, w_gate, w_up, w_down):
    d_loc, f_loc = w_gate.shape
    tiles = f_loc // LANES
    any_spec = pl.BlockSpec(memory_space=pl.ANY)
    f32, bf16 = jnp.float32, jnp.bfloat16
    return pl.pallas_call(
        functools.partial(exchange_kernel, tiles),
        out_shape=(jax.ShapeDtypeStruct((tiles, 3, 256, LANES), bf16),
                   jax.ShapeDtypeStruct((d_loc, 256), bf16),
                   jax.ShapeDtypeStruct((256, d_loc), bf16),
                   jax.ShapeDtypeStruct((8, 2, 2, 8, d_loc), f32),
                   *[jax.ShapeDtypeStruct((8, 4096), bf16)] * 2),
        in_specs=[any_spec] * 5,
        out_specs=(any_spec,) * 6,
        scratch_shapes=[
            pltpu.VMEM((2, 2, 8, 4096), bf16),
            pltpu.VMEM((2, 2, 16, 8, d_loc), bf16),
            pltpu.VMEM((2, 256, d_loc), bf16),
            pltpu.VMEM((d_loc, f_loc), bf16),
            pltpu.VMEM((d_loc, f_loc), bf16),
            pltpu.VMEM((f_loc, d_loc), bf16),
            pltpu.VMEM((SLOTS, 2, 3, 128, LANES), f32),
            pltpu.VMEM((2 * tiles, 3, 64, LANES), f32),
            pltpu.VMEM((SLOTS, 2, 3, 32, LANES), f32),
            pltpu.VMEM((2 * tiles, 3, 32, LANES), f32),
            pltpu.VMEM((SLOTS, 2, 3, 16, LANES), f32),
            pltpu.VMEM((2 * tiles, 3, 16, LANES), f32),
            pltpu.VMEM((tiles, 3, 256, LANES), bf16),
            pltpu.VMEM((2, 16, 2, 8, d_loc), f32),
            pltpu.VMEM((2, 8, 8, d_loc), f32),
            pltpu.VMEM((8, 2, 8, d_loc), bf16),
            pltpu.VMEM((2, 8, 4096), bf16),
            pltpu.VMEM((d_loc, 256), bf16),
            pltpu.SemaphoreType.DMA((5,)),
            pltpu.SemaphoreType.DMA((2, 2)),
            pltpu.SemaphoreType.DMA((2, 2)),
            pltpu.SemaphoreType.DMA((3, 4)),
            pltpu.SemaphoreType.DMA((3, SLOTS)),
            pltpu.SemaphoreType.DMA((3, LATE_SLOTS)),
            pltpu.SemaphoreType.DMA((1,)),
            pltpu.SemaphoreType.DMA((2, 2, LEAD)),
            pltpu.SemaphoreType.DMA((2, 2)),
            pltpu.SemaphoreType.DMA((7,)),
            pltpu.SemaphoreType.DMA((2,)),
            pltpu.SemaphoreType.DMA((2,)),
        ],
        compiler_params=pltpu.CompilerParams(collective_id=0, has_side_effects=True, vmem_limit_bytes=60 * 2**20),
        cost_estimate=pl.CostEstimate(flops=9 * 10**9, bytes_accessed=28 * 10**6, transcendentals=0),
        name="exchange",
    )(x_loc, dy_loc, w_gate, w_up, w_down)


OUT_SLOTS = 3
WIDTH = 2 * LANES


def grads_kernel(tiles, xt_hbm, dy_hbm, act_hbm, dg_hbm, du_hbm, dd_hbm, xt, dy, act, gate, up, down, load_sem, out_sem):
    pairs = tiles // 2
    row_loads = [pltpu.make_async_copy(xt_hbm, xt, load_sem.at[10]), pltpu.make_async_copy(dy_hbm, dy, load_sem.at[11])]
    for cp in row_loads:
        cp.start()

    edges = [0, 1, 3] + list(range(7, pairs, 4)) + [pairs]

    def act_copy(k):
        last = tiles if edges[k + 1] == pairs else 2 * edges[k + 1]
        span = pl.ds(2 * edges[k], last - 2 * edges[k])
        return pltpu.make_async_copy(act_hbm.at[span], act.at[span], load_sem.at[k])

    for k in range(len(edges) - 1):
        act_copy(k).start()
    for cp in row_loads:
        cp.wait()

    def out_copies(i, slot, width):
        cols = pl.ds(pl.multiple_of(i * WIDTH, WIDTH), width)
        part = pl.ds(0, width)
        return [pltpu.make_async_copy(gate.at[slot, :, part], dg_hbm.at[:, cols], out_sem.at[0, slot]),
                pltpu.make_async_copy(up.at[slot, :, part], du_hbm.at[:, cols], out_sem.at[1, slot]),
                pltpu.make_async_copy(down.at[slot, part, :], dd_hbm.at[cols, :], out_sem.at[2, slot])]

    def step(i, n):
        slot = lax.rem(i, OUT_SLOTS)
        for k in range(len(edges) - 1):
            pl.when(i == edges[k])(act_copy(k).wait)

        def wait_old():
            for cp in out_copies(i - OUT_SLOTS, slot, WIDTH):
                cp.wait()

        pl.when(i >= OUT_SLOTS)(wait_old)

        def cols(kind):
            return jnp.concatenate([act[2 * i + k, kind] for k in range(n)], axis=1)

        part = slice(0, n * LANES)
        gate[slot, :, part] = dot_f32(xt[...], cols(1))
        up[slot, :, part] = dot_f32(xt[...], cols(2))
        down[slot, part, :] = lax.dot_general(cols(0), dy[...], TRANS_A, preferred_element_type=jnp.float32)
        for cp in out_copies(i, slot, n * LANES):
            cp.start()

    def body(i, carry):
        step(i, 2)
        return carry

    lax.fori_loop(0, pairs, body, 0)
    last = pairs
    if tiles % 2:
        step(pairs, 1)
        last = pairs + 1
    for i in range(last - OUT_SLOTS, last):
        for cp in out_copies(i, i % OUT_SLOTS, WIDTH if i < pairs else LANES):
            cp.wait()


def weight_grads(xt, dy_rows, act):
    tiles = act.shape[0]
    d_loc = xt.shape[0]
    f_loc = tiles * LANES
    any_spec = pl.BlockSpec(memory_space=pl.ANY)
    f32, bf16 = jnp.float32, jnp.bfloat16
    return pl.pallas_call(
        functools.partial(grads_kernel, tiles), in_specs=[any_spec] * 3, out_specs=[any_spec] * 3,
        out_shape=[jax.ShapeDtypeStruct((d_loc, f_loc), f32)] * 2 + [jax.ShapeDtypeStruct((f_loc, d_loc), f32)],
        scratch_shapes=[
            pltpu.VMEM((d_loc, 256), bf16),
            pltpu.VMEM((256, d_loc), bf16),
            pltpu.VMEM(act.shape, bf16),
            pltpu.VMEM((OUT_SLOTS, d_loc, WIDTH), f32),
            pltpu.VMEM((OUT_SLOTS, d_loc, WIDTH), f32),
            pltpu.VMEM((OUT_SLOTS, WIDTH, d_loc), f32),
            pltpu.SemaphoreType.DMA((12,)),
            pltpu.SemaphoreType.DMA((3, OUT_SLOTS)),
        ],
        compiler_params=pltpu.CompilerParams(vmem_limit_bytes=62 * 2**20),
        cost_estimate=pl.CostEstimate(flops=6 * 256 * d_loc * f_loc, bytes_accessed=44 * 10**6, transcendentals=0),
        name="weight_grads",
    )(xt, dy_rows, act)


def solution(mesh):
    row_spec = P(None, ("dp", "tp"), None)
    in_specs = (row_spec, P("dp", "tp"), P("dp", "tp"), P("tp", "dp"), row_spec)
    out_specs = (row_spec, row_spec, P("dp", "tp"), P("dp", "tp"), P("tp", "dp"))

    def local_step(x_loc, w_gate, w_up, w_down, dy_loc):
        act, xt, dy_rows, part, y_first, dx_first = exchange(x_loc, dy_loc, w_gate, w_up, w_down)
        part = lax.all_to_all(part.reshape(16, 2, 8, -1), ("dp", "tp"), split_axis=0, concat_axis=0, tiled=True)
        part = part.reshape(8, 2, 2, 8, -1)
        out = (part[:, 0] + part[:, 1]).transpose(1, 2, 0, 3).reshape(2, 8, 4096)
        y = jnp.stack([y_first, (x_loc[1].astype(jnp.float32) + out[0]).astype(jnp.bfloat16)])
        dx = jnp.stack([dx_first, (dy_loc[1].astype(jnp.float32) + out[1]).astype(jnp.bfloat16)])
        dg, du, dd = weight_grads(xt, dy_rows, act)
        return y, dx, dg, du, dd

    return jax.shard_map(local_step, mesh=mesh, in_specs=in_specs, out_specs=out_specs, check_vma=False)
```

```python
import functools

import jax
import jax.numpy as jnp
from jax import lax
from jax.experimental import pallas as pl
from jax.experimental.pallas import tpu as pltpu
from jax.sharding import PartitionSpec as P

MESH = pl.DeviceIdType.MESH
LANES = 128
SLOTS = 8
LATE_SLOTS = 11
DEFER = 6
LEAD = 2
LAGS = (3, 3, 2, 2, 2, 1)
STARTS = tuple(sum(LAGS[:k]) for k in range(len(LAGS) + 1))
TRANS_B = (((1,), (1,)), ((), ()))
TRANS_A = (((0,), (0,)), ((), ()))


def dot_f32(lhs, rhs):
    return jnp.dot(lhs, rhs, preferred_element_type=jnp.float32)


def dot_t(lhs, rhs):
    return lax.dot_general(lhs, rhs, TRANS_B, preferred_element_type=jnp.float32)


def exchange_kernel(tiles, x_hbm, dy_hbm, wg_hbm, wu_hbm, wd_hbm,
                    act_hbm, xt_hbm, dy_rows_hbm, sum_hbm, y_hbm, dx_hbm,
                    loc, tok, rows, wg, wu, wd, part, core_in, first_out, first_in, second_out, second_in, act, acc, zin, fin, yin, xt,
                    load_sem, tok_send, tok_recv, send_sem, recv_sem, late_sem, gather_sem, lead_sem, plane_sem, store_sem, z_sem, fin_sem):
    tp = lax.axis_index("tp")
    dp = lax.axis_index("dp")
    core = lax.rem(dp, 2)
    xpos = lax.rem(lax.div(dp, 2), 2)
    ypos = lax.div(dp, 4)
    me = tp * 8 + dp

    def device(fc, fx, fy, fz):
        dc = 1 - core if fc else core
        dx = 1 - xpos if fx else xpos
        dy = 1 - ypos if fy else ypos
        return (1 - tp if fz else tp, dy * 4 + dx * 2 + dc)

    core_peer = device(1, 0, 0, 0)
    x_peer = device(0, 1, 0, 0)
    y_peer = device(0, 0, 1, 0)

    token_loads = [pltpu.make_async_copy(x_hbm, loc.at[0], load_sem.at[0]),
                   pltpu.make_async_copy(dy_hbm, loc.at[1], load_sem.at[1])]
    weight_loads = [pltpu.make_async_copy(wg_hbm, wg, load_sem.at[2]),
                    pltpu.make_async_copy(wu_hbm, wu, load_sem.at[3]),
                    pltpu.make_async_copy(wd_hbm, wd, load_sem.at[4])]
    for cp in token_loads + weight_loads:
        cp.start()

    others = [((k >> 0) & 1, (k >> 1) & 1, (k >> 2) & 1, (k >> 3) & 1) for k in range(15, 0, -1)]
    barrier = pltpu.get_barrier_semaphore()
    for flags in others:
        pl.semaphore_signal(barrier, 1, device_id=device(*flags), device_id_type=MESH)
    pl.semaphore_wait(barrier, 15)

    plane = [flags for flags in others if not flags[3]]
    for mb in range(2):
        for arr in range(2):
            if mb == 0:
                token_loads[arr].wait()
            for flags in (plane if mb else others):
                dest = device(*flags)
                pltpu.make_async_remote_copy(
                    src_ref=loc.at[arr, mb, :, pl.ds(pl.multiple_of(dest[1] * 512, 512), 512)],
                    dst_ref=tok.at[arr, mb, me],
                    send_sem=tok_send.at[arr, mb], recv_sem=tok_recv.at[arr, mb],
                    device_id=dest, device_id_type=MESH).start()
    for mb in range(2):
        for arr in range(2):
            tok[arr, mb, me] = loc[arr, mb, :, pl.ds(pl.multiple_of(dp * 512, 512), 512)]

    def plane_copy(arr):
        slab = tok.at[arr, 1, pl.ds(pl.multiple_of(8 * tp, 8), 8)]
        return pltpu.make_async_remote_copy(
            src_ref=slab, dst_ref=slab, send_sem=plane_sem.at[0, arr], recv_sem=plane_sem.at[1, arr],
            device_id=device(0, 0, 0, 1), device_id_type=MESH)

    def send_plane():
        for arr in range(2):
            got = tok.at[arr, 1, pl.ds(0, 7)]
            pltpu.make_async_copy(got, got, tok_recv.at[arr, 1]).wait()
            plane_copy(arr).start()

    def tokens_in(arr, mb):
        if mb:
            plane_copy(arr).wait()
        else:
            part15 = tok.at[arr, 0, pl.ds(0, 15)]
            pltpu.make_async_copy(part15, part15, tok_recv.at[arr, 0]).wait()
        for pair in range(8):
            lo = tok[arr, mb, pair].astype(jnp.float32)
            hi = tok[arr, mb, 8 + pair].astype(jnp.float32)
            rows[arr, pl.ds(mb * 128 + 16 * pair, 16), :] = jnp.concatenate([lo, hi], axis=0).astype(jnp.bfloat16)

    acc[...] = jnp.zeros_like(acc)

    n_iter = tiles

    def unit(i, h):
        u = 2 * i + h
        mb = lax.div(u, tiles)
        return u, mb, u - tiles * mb

    keep_core = pl.multiple_of(core * 64, 64)
    send_core = pl.multiple_of((1 - core) * 64, 64)
    pos1 = (xpos, ypos)
    pos2 = (ypos, xpos)
    peer1 = (x_peer, y_peer)
    peer2 = (y_peer, x_peer)

    def off(v):
        return pl.multiple_of(v, 16)

    def copies(stage, i, h):
        u, mb, t = unit(i, h)
        slot = lax.rem(i, SLOTS)
        base = mb * 128 + core * 64
        if stage == 0:
            src, dst, dev = part.at[slot, h, :, pl.ds(send_core, 64), :], core_in.at[u], core_peer
        elif stage == 1:
            src, dst, dev = first_out.at[slot, h], first_in.at[u], peer1[h]
        elif stage == 2:
            src, dst, dev = second_out.at[slot, h], second_in.at[u], peer2[h]
        elif stage == 3:
            src = dst = act.at[t, :, pl.ds(off(base + 32 * pos1[h] + 16 * pos2[h]), 16), :]
            dev = peer2[h]
        elif stage == 4:
            src = dst = act.at[t, :, pl.ds(off(base + 32 * pos1[h]), 32), :]
            dev = peer1[h]
        else:
            src = dst = act.at[t, :, pl.ds(off(base), 64), :]
            dev = core_peer
        return pltpu.make_async_remote_copy(
            src_ref=src, dst_ref=dst, send_sem=send_sem.at[stage, lax.rem(i, 4)] if stage < 3 else gather_sem.at[0],
            recv_sem=arrival(stage, i), device_id=dev, device_id_type=MESH)

    def arrival(stage, i):
        if stage < 3:
            return recv_sem.at[stage, lax.rem(i, SLOTS)]
        return late_sem.at[stage - 3, lax.rem(i, LATE_SLOTS)]

    def start_pair(stage, i):
        for h in range(2):
            copies(stage, i, h).start()

    def wait_pair(stage, i):
        if stage < 3:
            into = (core_in, first_in, second_in)[stage].at[pl.ds(2 * i, 2)]
            pltpu.make_async_copy(into, into, send_sem.at[stage, lax.rem(i, 4)]).wait()
        else:
            into = act.at[0, :, pl.ds(0, 32 << (stage - 3)), :]
        pltpu.make_async_copy(into, into, arrival(stage, i)).wait()

    def gate_up_partials(i, h):
        u, mb, t = unit(i, h)
        slot = lax.rem(i, SLOTS)
        cols = pl.ds(pl.multiple_of(t * LANES, LANES), LANES)
        r = pl.ds(pl.multiple_of(mb * 128, 128), 128)
        pair = jnp.concatenate([wg[:, cols], wu[:, cols]], axis=1)
        ab = dot_f32(rows[0, r, :], pair)
        part[slot, h, 0] = ab[:, :LANES]
        part[slot, h, 1] = ab[:, LANES:]

    def down_partials(i, h):
        u, mb, t = unit(i, h)
        cols = pl.ds(pl.multiple_of(t * LANES, LANES), LANES)
        r = pl.ds(pl.multiple_of(mb * 128, 128), 128)
        part[lax.rem(i, SLOTS), h, 2] = dot_t(rows[1, r, :], wd[cols, :])

    def stage_partials(i):
        for h in range(2):
            gate_up_partials(i, h)
            down_partials(i, h)
        start_pair(0, i)

    def lead_in():
        kinds = (pl.ds(0, 2), pl.ds(2, 1))

        def to_core(i, k):
            for h in range(2):
                pltpu.make_async_remote_copy(
                    src_ref=part.at[i, h, kinds[k], pl.ds(send_core, 64), :], dst_ref=core_in.at[2 * i + h, kinds[k]],
                    send_sem=lead_sem.at[0, k, i], recv_sem=lead_sem.at[1, k, i], device_id=core_peer, device_id_type=MESH).start()

        def to_first(i, k):
            both = core_in.at[pl.ds(2 * i, 2), kinds[k]]
            for way in range(2):
                pltpu.make_async_copy(both, both, lead_sem.at[way, k, i]).wait()
            for h in range(2):
                o = (1 - pos1[h]) * 32
                first_out[i, h, kinds[k]] = (part[i, h, kinds[k], pl.ds(off(core * 64 + o), 32), :]
                                             + core_in[2 * i + h, kinds[k], pl.ds(off(o), 32), :])
                pltpu.make_async_remote_copy(
                    src_ref=first_out.at[i, h, kinds[k]], dst_ref=first_in.at[2 * i + h, kinds[k]], send_sem=send_sem.at[1, i],
                    recv_sem=arrival(1, i), device_id=peer1[h], device_id_type=MESH).start()

        tokens_in(0, 0)
        for cp in weight_loads[:2]:
            cp.wait()
        for i in range(LEAD):
            for h in range(2):
                gate_up_partials(i, h)
            to_core(i, 0)
        for i in range(LEAD):
            to_first(i, 0)
        tokens_in(1, 0)
        weight_loads[2].wait()
        for i in range(LEAD):
            for h in range(2):
                down_partials(i, h)
            to_core(i, 1)
        for i in range(LEAD, STARTS[1]):
            stage_partials(i)
        for i in range(LEAD):
            to_first(i, 1)

    def stage_first(i):
        slot = lax.rem(i, SLOTS)
        wait_pair(0, i)
        for h in range(2):
            u, _, _ = unit(i, h)
            o = (1 - pos1[h]) * 32
            first_out[slot, h] = (part[slot, h, :, pl.ds(off(core * 64 + o), 32), :] + core_in[u, :, pl.ds(off(o), 32), :])
            copies(1, i, h).start()

    def stage_second(i):
        slot = lax.rem(i, SLOTS)
        wait_pair(1, i)
        for h in range(2):
            u, _, _ = unit(i, h)
            o2 = (1 - pos2[h]) * 16
            o = pos1[h] * 32 + o2
            second_out[slot, h] = (part[slot, h, :, pl.ds(off(core * 64 + o), 16), :] + core_in[u, :, pl.ds(off(o), 16), :]
                                   + first_in[u, :, pl.ds(off(o2), 16), :])
            copies(2, i, h).start()

    def stage_act(i):
        slot = lax.rem(i, SLOTS)
        wait_pair(2, i)
        for h in range(2):
            u, mb, t = unit(i, h)
            o2 = pos2[h] * 16
            o = pos1[h] * 32 + o2
            tot = (part[slot, h, :, pl.ds(off(core * 64 + o), 16), :] + core_in[u, :, pl.ds(off(o), 16), :]
                   + first_in[u, :, pl.ds(off(o2), 16), :] + second_in[u])
            a, b, g = tot[0], tot[1], tot[2]
            s = jax.nn.sigmoid(a)
            silu = a * s
            r = pl.ds(off(mb * 128 + core * 64 + o), 16)
            act[t, 0, r, :] = (silu * b).astype(jnp.bfloat16)
            act[t, 1, r, :] = (g * b * s * (1.0 + a * (1.0 - s))).astype(jnp.bfloat16)
            act[t, 2, r, :] = (g * silu).astype(jnp.bfloat16)
            copies(3, i, h).start()

    def stage_forward(stage, i):
        wait_pair(stage - 1, i)
        start_pair(stage, i)

    def add_to(arr, mb, term):
        blocks = pl.ds(mb * 8, 8)
        acc[arr, blocks] += term.reshape(8, 2, 8, term.shape[-1])

    def stage_outputs(i):
        wait_pair(5, i)
        for h in range(2):
            u, mb, t = unit(i, h)
            cols = pl.ds(pl.multiple_of(t * LANES, LANES), LANES)
            r = pl.ds(pl.multiple_of(mb * 128, 128), 128)
            pltpu.make_async_copy(act.at[t, :, r, :], act_hbm.at[t, :, r, :], store_sem.at[0]).start()
            add_to(0, mb, dot_f32(act[t, 0, r, :], wd[cols, :]))
            grads = jnp.concatenate([act[t, 1, r, :], act[t, 2, r, :]], axis=1)
            pair = jnp.concatenate([wg[:, cols], wu[:, cols]], axis=1)
            add_to(1, mb, dot_t(grads, pair))

    z_copy = pltpu.make_async_remote_copy(
        src_ref=acc.at[:, pl.ds(0, 8), 1 - tp], dst_ref=zin, send_sem=z_sem.at[0], recv_sem=z_sem.at[1],
        device_id=device(0, 0, 0, 1), device_id_type=MESH)
    my_cols = pl.ds(pl.multiple_of(dp * 512, 512), 512)

    def finish_first():
        z_copy.wait()
        for arr in range(2):
            for blk in range(8):
                total = acc[arr, blk, tp] + zin[arr, blk]
                fin[blk, arr] = (tok[arr, 0, 8 * tp + blk].astype(jnp.float32) + total).astype(jnp.bfloat16)

    def send_first():
        for flags in plane:
            dest = device(*flags)
            pltpu.make_async_remote_copy(
                src_ref=fin.at[dest[1]], dst_ref=yin.at[:, :, my_cols], send_sem=fin_sem.at[0], recv_sem=fin_sem.at[1],
                device_id=dest, device_id_type=MESH).start()
        yin[:, :, my_cols] = fin[dp]

    firsts = [pltpu.make_async_copy(yin.at[k], ref, store_sem.at[4 + k]) for k, ref in enumerate((y_hbm, dx_hbm))]

    def store_first():
        blocks = fin.at[pl.ds(0, 7)]
        for k in range(2):
            pltpu.make_async_copy(blocks, blocks, fin_sem.at[k]).wait()
        for cp in firsts:
            cp.start()

    z_start = (tiles - 1) // 2 + STARTS[6] + DEFER + 1

    def forwarded(j):
        ready = jnp.maximum(j - STARTS[4] + 1, 0)
        late = jnp.maximum(j - STARTS[4] + 1 - DEFER, 0) + jnp.maximum(j - n_iter - STARTS[1] + 2, 0)
        return jnp.minimum(n_iter, jnp.minimum(ready, late))

    def run_late(j, fn):
        def step(i, carry):
            fn(i)
            return carry

        lax.fori_loop(forwarded(j - 1), forwarded(j), step, 0)

    row_stores = [pltpu.make_async_copy(xt, xt_hbm, store_sem.at[1]), pltpu.make_async_copy(rows.at[1], dy_rows_hbm, store_sem.at[6])]

    def body(j, carry):
        pl.when(j == STARTS[1] + 4)(send_plane)
        pl.when(j == z_start)(z_copy.start)
        pl.when(j == n_iter + STARTS[3] - 2)(finish_first)

        def run(stage, fn):
            i = j - STARTS[stage]
            pl.when(jnp.logical_and(i >= (LEAD if stage == 1 else 0), i < n_iter))(functools.partial(fn, i))

        run(1, stage_first)
        run(2, stage_second)
        run(3, stage_act)
        run_late(j, functools.partial(stage_forward, 4))
        pl.when(j == n_iter + STARTS[4] - 1)(send_first)
        run_late(j - LAGS[4], functools.partial(stage_forward, 5))

        @pl.when(j == tiles // 2 - 2)
        def _():
            tokens_in(0, 1)
            tokens_in(1, 1)
            xt[...] = rows[0].T
            for cp in row_stores:
                cp.start()

        run(0, stage_partials)
        run_late(j - LAGS[4] - LAGS[5], stage_outputs)
        return carry

    lead_in()
    lax.fori_loop(STARTS[1], n_iter + STARTS[6], body, 0)

    sums = [pltpu.make_async_copy(acc.at[arr, pl.ds(8, 8)], sum_hbm.at[:, :, arr], store_sem.at[2 + arr]) for arr in range(2)]
    for cp in sums:
        cp.start()
    store_first()
    for mb in range(2):
        for arr in range(2):
            sent = tok.at[arr, mb, pl.ds(0, 7 if mb else 15)]
            pltpu.make_async_copy(sent, sent, tok_send.at[arr, mb]).wait()
    for cp in row_stores:
        cp.wait()
    pltpu.make_async_copy(act, act_hbm, store_sem.at[0]).wait()
    sent = act.at[:, :, pl.ds(0, 224), :]
    pltpu.make_async_copy(sent, sent, gather_sem.at[0]).wait()
    for cp in sums + firsts:
        cp.wait()


def exchange(x_loc, dy_loc, w_gate, w_up, w_down):
    d_loc, f_loc = w_gate.shape
    tiles = f_loc // LANES
    any_spec = pl.BlockSpec(memory_space=pl.ANY)
    f32, bf16 = jnp.float32, jnp.bfloat16
    return pl.pallas_call(
        functools.partial(exchange_kernel, tiles),
        out_shape=(jax.ShapeDtypeStruct((tiles, 3, 256, LANES), bf16),
                   jax.ShapeDtypeStruct((d_loc, 256), bf16),
                   jax.ShapeDtypeStruct((256, d_loc), bf16),
                   jax.ShapeDtypeStruct((8, 2, 2, 8, d_loc), f32),
                   *[jax.ShapeDtypeStruct((8, 4096), bf16)] * 2),
        in_specs=[any_spec] * 5,
        out_specs=(any_spec,) * 6,
        scratch_shapes=[
            pltpu.VMEM((2, 2, 8, 4096), bf16),
            pltpu.VMEM((2, 2, 16, 8, d_loc), bf16),
            pltpu.VMEM((2, 256, d_loc), bf16),
            pltpu.VMEM((d_loc, f_loc), bf16),
            pltpu.VMEM((d_loc, f_loc), bf16),
            pltpu.VMEM((f_loc, d_loc), bf16),
            pltpu.VMEM((SLOTS, 2, 3, 128, LANES), f32),
            pltpu.VMEM((2 * tiles, 3, 64, LANES), f32),
            pltpu.VMEM((SLOTS, 2, 3, 32, LANES), f32),
            pltpu.VMEM((2 * tiles, 3, 32, LANES), f32),
            pltpu.VMEM((SLOTS, 2, 3, 16, LANES), f32),
            pltpu.VMEM((2 * tiles, 3, 16, LANES), f32),
            pltpu.VMEM((tiles, 3, 256, LANES), bf16),
            pltpu.VMEM((2, 16, 2, 8, d_loc), f32),
            pltpu.VMEM((2, 8, 8, d_loc), f32),
            pltpu.VMEM((8, 2, 8, d_loc), bf16),
            pltpu.VMEM((2, 8, 4096), bf16),
            pltpu.VMEM((d_loc, 256), bf16),
            pltpu.SemaphoreType.DMA((5,)),
            pltpu.SemaphoreType.DMA((2, 2)),
            pltpu.SemaphoreType.DMA((2, 2)),
            pltpu.SemaphoreType.DMA((3, 4)),
            pltpu.SemaphoreType.DMA((3, SLOTS)),
            pltpu.SemaphoreType.DMA((3, LATE_SLOTS)),
            pltpu.SemaphoreType.DMA((1,)),
            pltpu.SemaphoreType.DMA((2, 2, LEAD)),
            pltpu.SemaphoreType.DMA((2, 2)),
            pltpu.SemaphoreType.DMA((7,)),
            pltpu.SemaphoreType.DMA((2,)),
            pltpu.SemaphoreType.DMA((2,)),
        ],
        compiler_params=pltpu.CompilerParams(collective_id=0, has_side_effects=True, vmem_limit_bytes=60 * 2**20),
        cost_estimate=pl.CostEstimate(flops=9 * 10**9, bytes_accessed=28 * 10**6, transcendentals=0),
        name="exchange",
    )(x_loc, dy_loc, w_gate, w_up, w_down)


OUT_SLOTS = 3
WIDTH = 2 * LANES


def grads_kernel(tiles, xt_hbm, dy_hbm, act_hbm, dg_hbm, du_hbm, dd_hbm, xt, dy, act, gate, up, down, load_sem, out_sem):
    pairs = tiles // 2
    row_loads = [pltpu.make_async_copy(xt_hbm, xt, load_sem.at[10]), pltpu.make_async_copy(dy_hbm, dy, load_sem.at[11])]
    for cp in row_loads:
        cp.start()

    edges = [0, 1, 3] + list(range(7, pairs, 4)) + [pairs]

    def act_copy(k):
        last = tiles if edges[k + 1] == pairs else 2 * edges[k + 1]
        span = pl.ds(2 * edges[k], last - 2 * edges[k])
        return pltpu.make_async_copy(act_hbm.at[span], act.at[span], load_sem.at[k])

    for k in range(len(edges) - 1):
        act_copy(k).start()
    for cp in row_loads:
        cp.wait()

    def out_copies(i, slot, width):
        cols = pl.ds(pl.multiple_of(i * WIDTH, WIDTH), width)
        part = pl.ds(0, width)
        return [pltpu.make_async_copy(gate.at[slot, :, part], dg_hbm.at[:, cols], out_sem.at[0, slot]),
                pltpu.make_async_copy(up.at[slot, :, part], du_hbm.at[:, cols], out_sem.at[1, slot]),
                pltpu.make_async_copy(down.at[slot, part, :], dd_hbm.at[cols, :], out_sem.at[2, slot])]

    def step(i, n):
        slot = lax.rem(i, OUT_SLOTS)
        for k in range(len(edges) - 1):
            pl.when(i == edges[k])(act_copy(k).wait)

        def wait_old():
            for cp in out_copies(i - OUT_SLOTS, slot, WIDTH):
                cp.wait()

        pl.when(i >= OUT_SLOTS)(wait_old)

        def cols(kind):
            return jnp.concatenate([act[2 * i + k, kind] for k in range(n)], axis=1)

        part = slice(0, n * LANES)
        gate[slot, :, part] = dot_f32(xt[...], cols(1))
        up[slot, :, part] = dot_f32(xt[...], cols(2))
        down[slot, part, :] = lax.dot_general(cols(0), dy[...], TRANS_A, preferred_element_type=jnp.float32)
        for cp in out_copies(i, slot, n * LANES):
            cp.start()

    def body(i, carry):
        step(i, 2)
        return carry

    lax.fori_loop(0, pairs, body, 0)
    last = pairs
    if tiles % 2:
        step(pairs, 1)
        last = pairs + 1
    for i in range(last - OUT_SLOTS, last):
        for cp in out_copies(i, i % OUT_SLOTS, WIDTH if i < pairs else LANES):
            cp.wait()


def weight_grads(xt, dy_rows, act):
    tiles = act.shape[0]
    d_loc = xt.shape[0]
    f_loc = tiles * LANES
    any_spec = pl.BlockSpec(memory_space=pl.ANY)
    f32, bf16 = jnp.float32, jnp.bfloat16
    return pl.pallas_call(
        functools.partial(grads_kernel, tiles), in_specs=[any_spec] * 3, out_specs=[any_spec] * 3,
        out_shape=[jax.ShapeDtypeStruct((d_loc, f_loc), f32)] * 2 + [jax.ShapeDtypeStruct((f_loc, d_loc), f32)],
        scratch_shapes=[
            pltpu.VMEM((d_loc, 256), bf16),
            pltpu.VMEM((256, d_loc), bf16),
            pltpu.VMEM(act.shape, bf16),
            pltpu.VMEM((OUT_SLOTS, d_loc, WIDTH), f32),
            pltpu.VMEM((OUT_SLOTS, d_loc, WIDTH), f32),
            pltpu.VMEM((OUT_SLOTS, WIDTH, d_loc), f32),
            pltpu.SemaphoreType.DMA((12,)),
            pltpu.SemaphoreType.DMA((3, OUT_SLOTS)),
        ],
        compiler_params=pltpu.CompilerParams(vmem_limit_bytes=62 * 2**20),
        cost_estimate=pl.CostEstimate(flops=6 * 256 * d_loc * f_loc, bytes_accessed=44 * 10**6, transcendentals=0),
        name="weight_grads",
    )(xt, dy_rows, act)


def solution(mesh):
    row_spec = P(None, ("dp", "tp"), None)
    in_specs = (row_spec, P("dp", "tp"), P("dp", "tp"), P("tp", "dp"), row_spec)
    out_specs = (row_spec, row_spec, P("dp", "tp"), P("dp", "tp"), P("tp", "dp"))

    def local_step(x_loc, w_gate, w_up, w_down, dy_loc):
        act, xt, dy_rows, part, y_first, dx_first = exchange(x_loc, dy_loc, w_gate, w_up, w_down)
        part = lax.all_to_all(part.reshape(16, 2, 8, -1), ("dp", "tp"), split_axis=0, concat_axis=0, tiled=True)
        part = part.reshape(8, 2, 2, 8, -1)
        out = (part[:, 0] + part[:, 1]).transpose(1, 2, 0, 3).reshape(2, 8, 4096)
        y = jnp.stack([y_first, (x_loc[1].astype(jnp.float32) + out[0]).astype(jnp.bfloat16)])
        dx = jnp.stack([dx_first, (dy_loc[1].astype(jnp.float32) + out[1]).astype(jnp.bfloat16)])
        dg, du, dd = weight_grads(xt, dy_rows, act)
        return y, dx, dg, du, dd

    return jax.shard_map(local_step, mesh=mesh, in_specs=in_specs, out_specs=out_specs, check_vma=False)
```
